32 devices in a mesh: dp: 4 (over z), stage: 2 (over y), tp: 4 (over x, core).
Axes of the slice: x: 2, y: 2, z: 4, core: 2. Of those that a mesh axis runs over, the one named last changes fastest.
Arguments:
- act_in: bfloat16 [2, 128, 14, 14, 512], P('stage', ('dp', 'tp'))
- w_conv: bfloat16 [2, 3, 3, 512, 512], P('stage', None, None, None, 'tp')
- gamma_vec: float32 [2, 512], P('stage', 'tp')
- beta_vec: float32 [2, 512], P('stage', 'tp')
- z_grad: bfloat16 [2, 128, 14, 14, 512], P('stage', 'dp', None, None, 'tp')
Outputs:
- output 1: bfloat16 [2, 128, 14, 14, 512], P('stage', 'dp', None, None, 'tp')
- output 2: bfloat16 [2, 128, 14, 14, 512], P('stage', ('dp', 'tp'))
- output 3: float32 [2, 3, 3, 512, 512], P('stage', None, None, None, 'tp')
All inputs are finite; a program needn't handle non-finite values.
Results may differ from the reference program's by a relative error of at most 0.00522.
Values are sent between devices in bfloat16 or wider.
A program may use at most 1 GiB of HBM per device.

```python
import jax
import jax.numpy as jnp
from jax import lax

STAGES = 2
IMAGES = 128
IMG_SIDE = 14
CH_IN = 512
CH_OUT = 512


def put_at(stage_pos, values):
    widths = [(stage_pos, STAGES - 1 - stage_pos)] + [(0, 0)] * values.ndim
    return jnp.pad(values[None], widths)


def setup_inputs(seed: int = 0) -> dict:
    base_key = jax.random.key(seed)
    k_act, k_w, k_gam, k_beta, k_dz = jax.random.split(base_key, 5)
    act_vals = jax.random.normal(k_act, (IMAGES, IMG_SIDE, IMG_SIDE, CH_IN), jnp.float32)
    w_vals = jax.random.normal(k_w, (3, 3, CH_IN, CH_OUT), jnp.float32) * (9 * CH_IN) ** -0.5
    gamma_vals = 1.0 + 0.3 * jax.random.normal(k_gam, (CH_OUT,), jnp.float32)
    beta_vals = 0.5 * jax.random.normal(k_beta, (CH_OUT,), jnp.float32)
    dz_vals = jax.random.normal(k_dz, (IMAGES, IMG_SIDE, IMG_SIDE, CH_OUT), jnp.float32)
    return {
        'act_in': put_at(0, act_vals.astype(jnp.bfloat16)),
        'w_conv': put_at(1, w_vals.astype(jnp.bfloat16)),
        'gamma_vec': put_at(1, gamma_vals),
        'beta_vec': put_at(1, beta_vals),
        'z_grad': put_at(1, dz_vals.astype(jnp.bfloat16)),
    }


def conv_same(images, kernel):
    return lax.conv_general_dilated(images, kernel, (1, 1), 'SAME', dimension_numbers=('NHWC', 'HWIO', 'NHWC'))


def reference(act_in, w_conv, gamma_vec, beta_vec, z_grad):
    kernel = w_conv[1].astype(jnp.float32)
    gamma_row = gamma_vec[1]
    beta_row = beta_vec[1]

    def one_image(w_acc, img_pair):
        image_hwc, dz_hwc = img_pair
        image_f = image_hwc[None].astype(jnp.float32)
        pre_act, pull_back = jax.vjp(conv_same, image_f, kernel)
        affine = pre_act * gamma_row + beta_row
        z_img = jnp.maximum(affine, 0.0).astype(jnp.bfloat16)
        grad_pre = jnp.where(affine > 0, dz_hwc[None].astype(jnp.float32) * gamma_row, 0.0).astype(jnp.bfloat16)
        image_grad, kernel_grad = pull_back(grad_pre.astype(jnp.float32))
        return w_acc + kernel_grad, (z_img[0], image_grad[0].astype(jnp.bfloat16))

    w_init = jnp.zeros(kernel.shape, jnp.float32)
    w_sum, (z_all, dact_all) = lax.scan(one_image, w_init, (act_in[0], z_grad[1]))
    return put_at(1, z_all), put_at(0, dact_all), put_at(1, w_sum)
```

```python
import functools

import jax
import jax.numpy as jnp
from jax import lax
from jax.experimental import pallas as pl
from jax.experimental.pallas import tpu as pltpu
from jax.sharding import PartitionSpec as P

MESH = pl.DeviceIdType.MESH
F32 = jnp.float32
BF16 = jnp.bfloat16
PAD = 16


def remote(src, dst, send_sem, recv_sem, dev):
    return pltpu.make_async_remote_copy(src_ref=src, dst_ref=dst, send_sem=send_sem, recv_sem=recv_sem, device_id=dev, device_id_type=MESH)


def block_kernel(H, WD, CI, CO, n_chunk, x_ref, w_ref, gam_ref, bet_ref, dz_ref, z_ref, dx_ref, dw_ref,
                 xe, xo, ge, go, wall, dzb, zb, vec, acc, prx, pb, rb, mb, xt, relay, dxb, *sems):
    (s_xs, s_xr, s_xf, s_gs, s_gr, s_gl, s_gf, s_wl, s_ws, s_wr, s_vl, s_vs, s_vr, s_dl, s_ds, s_dr,
     s_zl, s_zs, s_zr, s_ps, s_pr, s_os, s_or, s_ms, s_mr, s_ts, s_tr, s_tl, s_dx) = sems
    R = WD * 8
    CW = 2 * CO
    zi = lax.axis_index("dp")
    st = lax.axis_index("stage")
    tp = lax.axis_index("tp")
    xi = tp // 2
    c = tp % 2
    y_dev = (zi, 1 - st, tp)
    x_dev = (zi, st, 2 * (1 - xi) + c)
    c_dev = (zi, st, 2 * xi + 1 - c)
    z_mate = jnp.where(zi == 1, 2, 1)
    z_out = jnp.where(zi < 2, 0, 3)
    z_in = jnp.where(zi < 2, 1, 2)
    inner = jnp.logical_or(zi == 1, zi == 2)
    mate_dev = (z_mate, st, tp)
    outer_dev = (z_out, st, tp)
    inner_dev = (z_in, st, tp)

    barrier = pltpu.get_barrier_semaphore()
    for dev in (y_dev, x_dev, c_dev):
        pl.semaphore_signal(barrier, inc=1, device_id=dev, device_id_type=MESH)

    @pl.when(inner)
    def _():
        for dev in (mate_dev, outer_dev):
            pl.semaphore_signal(barrier, inc=1, device_id=dev, device_id_type=MESH)
        pl.semaphore_wait(barrier, 5)

    @pl.when(jnp.logical_not(inner))
    def _():
        pl.semaphore_signal(barrier, inc=1, device_id=inner_dev, device_id_type=MESH)
        pl.semaphore_wait(barrier, 4)

    def zero_borders(buf):
        ch = buf.shape[-1]

        def rows(h, _):
            for s in range(2):
                buf[s, h, 0:PAD, :] = jnp.zeros((PAD, ch), BF16)
                buf[s, h, PAD + R:, :] = jnp.zeros((buf.shape[2] - PAD - R, ch), BF16)
            return 0

        lax.fori_loop(0, H + 2, rows, 0)

    def zero_planes(buf):
        for s in range(2):
            for h in (0, H + 1):
                buf[s, h] = jnp.zeros(buf.shape[2:], BF16)

    def odd_copy(even, odd, s, h):
        n = odd.shape[2]
        odd[s, h] = even[s, h, 8:8 + n, :]

    def tap_rows(even, odd, s, plane, shift, n):
        if shift == 0:
            return even[s, plane, PAD:PAD + n, :]
        start = PAD + 8 * shift - 8
        return odd[s, plane, start:start + n, :]

    @pl.when(st == 0)
    def _():
        def x_copy(h):
            return remote(x_ref.at[h], xe.at[xi, h + 1, pl.ds(PAD, R), :], s_xs.at[h], s_xr.at[xi, h], y_dev)

        lax.fori_loop(0, H, lambda h, _: (x_copy(h).start(), 0)[1], 0)
        zero_borders(ge)
        zero_planes(ge)
        zero_planes(go)

        def w_in(t, b):
            return remote(wall.at[b, t], wall.at[b, t], s_ws.at[0, t], s_wr.at[b, t], y_dev)

        def w_fwd(t, b, k, dev):
            return remote(wall.at[b, t], wall.at[b, t], s_ws.at[k, t], s_wr.at[b, t], dev)

        b_x = 2 * (1 - xi) + c

        def w_step(t, _):
            w_in(t, tp).wait_recv()
            w_fwd(t, tp, 0, c_dev).start()
            w_fwd(t, tp, 1, x_dev).start()
            return 0

        lax.fori_loop(0, 9, w_step, 0)

        def w_step2(t, _):
            w_in(t, b_x).wait_recv()
            w_fwd(t, b_x, 2, c_dev).start()
            return 0

        lax.fori_loop(0, 9, w_step2, 0)

        def w_step3(t, _):
            w_in(t, 2 * xi + 1 - c).wait_recv()
            w_in(t, 2 * (1 - xi) + 1 - c).wait_recv()
            return 0

        lax.fori_loop(0, 9, w_step3, 0)

        def g_in(j, b):
            return remote(ge.at[b, j + 1, pl.ds(PAD, R), :], ge.at[b, j + 1, pl.ds(PAD, R), :], s_gf.at[j], s_gr.at[b, j], y_dev)

        def relay_in(j):
            return remote(relay.at[j], relay.at[j], s_gf.at[j], s_gl.at[j], y_dev)

        def relay_out(j):
            return remote(relay.at[j], ge.at[xi, j + 1, pl.ds(PAD, R), :], s_gf.at[j], s_gr.at[xi, j], x_dev)

        def dx_out(h):
            return pltpu.make_async_copy(dxb.at[h], dx_ref.at[h], s_dx.at[h])

        def g_step(j, _):
            @pl.when(j < H)
            def _():
                relay_in(j).wait_recv()
                relay_out(j).start()
                g_in(j, xi).wait_recv()
                g_in(j, 1 - xi).wait_recv()
                for b in range(2):
                    odd_copy(ge, go, b, j + 1)

            @pl.when(j >= 1)
            def _():
                h = j - 1
                tot = jnp.zeros((R, CI), F32)
                for b in range(2):
                    for ky in range(3):
                        for kx in range(3):
                            t = 3 * ky + kx
                            lhs = tap_rows(ge, go, b, h + 2 - ky, 1 - kx, R)
                            rhs = jnp.concatenate([wall[2 * b, t], wall[2 * b + 1, t]], axis=1)
                            tot = tot + lax.dot_general(lhs, rhs, (((1,), (1,)), ((), ())), preferred_element_type=F32)
                dxb[h] = tot.astype(BF16)
                dx_out(h).start()

            return 0

        lax.fori_loop(0, H + 1, g_step, 0)

        def drain(h, _):
            x_copy(h).wait_send()
            relay_out(h).wait_send()
            dx_out(h).wait()
            return 0

        lax.fori_loop(0, H, drain, 0)

        def drain_w(t, _):
            w_fwd(t, tp, 0, c_dev).wait_send()
            w_fwd(t, tp, 1, x_dev).wait_send()
            w_fwd(t, b_x, 2, c_dev).wait_send()
            return 0

        lax.fori_loop(0, 9, drain_w, 0)

    @pl.when(st == 1)
    def _():
        w_loc = pltpu.make_async_copy(w_ref, wall.at[c], s_wl)
        w_core = remote(w_ref, wall.at[c], s_vs.at[2], s_vr.at[2], c_dev)
        vecs_l = [pltpu.make_async_copy(r, vec.at[k, c], s_vl.at[k]) for k, r in enumerate((gam_ref, bet_ref))]
        vecs_r = [remote(r, vec.at[k, c], s_vs.at[k], s_vr.at[k], c_dev) for k, r in enumerate((gam_ref, bet_ref))]
        dz_l = [pltpu.make_async_copy(dz_ref.at[:, :, 2 * s + c], dzb.at[s, c], s_dl.at[s]) for s in range(2)]
        dz_r = [remote(dz_ref.at[:, :, 2 * s + 1 - c], dzb.at[s, c], s_ds.at[s], s_dr.at[s], c_dev) for s in range(2)]

        def w_y(t):
            return remote(w_ref.at[t], wall.at[tp, t], s_ws.at[0, t], s_wr.at[tp, t], y_dev)

        w_loc.start()
        w_core.start()
        for k in range(2):
            vecs_l[k].start()
            vecs_r[k].start()
            dz_l[k].start()
            dz_r[k].start()
        lax.fori_loop(0, 9, lambda t, _: (w_y(t).start(), 0)[1], 0)

        zero_borders(xe)
        zero_borders(ge)
        for buf in (xe, xo, ge, go):
            zero_planes(buf)

        def zero_acc(t, _):
            for k in range(2):
                acc[k, t] = jnp.zeros((CI, CO), F32)
            return 0

        lax.fori_loop(0, 9, zero_acc, 0)
        for k in range(2):
            vecs_l[k].wait()
            vecs_r[k].wait_recv()
            dz_l[k].wait()
            dz_r[k].wait_recv()
        w_loc.wait()
        w_core.wait_recv()

        def x_in(j, s):
            view = xe.at[s, j + 1, pl.ds(PAD, R), :]
            return remote(view, view, s_xf.at[j], s_xr.at[s, j], y_dev)

        def x_fwd(j):
            view = xe.at[xi, j + 1, pl.ds(PAD, R), :]
            return remote(view, view, s_xf.at[j], s_xr.at[xi, j], x_dev)

        def g_own(h):
            return remote(ge.at[xi, h + 1, pl.ds(PAD, R), :], ge.at[xi, h + 1, pl.ds(PAD, R), :], s_gs.at[0, h], s_gr.at[xi, h], y_dev)

        def g_other(h):
            return remote(ge.at[1 - xi, h + 1, pl.ds(PAD, R), :], relay.at[h], s_gs.at[1, h], s_gl.at[h], y_dev)

        def step(j, _):
            @pl.when(j < H)
            def _():
                x_in(j, xi).wait_recv()
                x_fwd(j).start()
                x_in(j, 1 - xi).wait_recv()
                for s in range(2):
                    odd_copy(xe, xo, s, j + 1)

            @pl.when(jnp.logical_and(j >= 1, j < H + 1))
            def _():
                h = j - 1
                pre = jnp.zeros((2 * R, CW), F32)
                for ky in range(3):
                    for kx in range(3):
                        t = 3 * ky + kx
                        lhs = jnp.concatenate([tap_rows(xe, xo, s, h + ky, kx - 1, R) for s in range(2)], axis=0)
                        rhs = jnp.concatenate([wall[0, t], wall[1, t]], axis=1)
                        pre = pre + jnp.dot(lhs, rhs, preferred_element_type=F32)
                for k in range(2):
                    gam = vec[0, k]
                    bet = vec[1, k]
                    for s in range(2):
                        y = pre[s * R:(s + 1) * R, k * CO:(k + 1) * CO] * gam + bet
                        zb[s, k, h] = jnp.maximum(y, 0.0).reshape(WD, 8, CO).astype(BF16)
                        dzr = dzb[s, k, h].astype(F32).reshape(R, CO)
                        ge[s, h + 1, PAD:PAD + R, k * CO:(k + 1) * CO] = jnp.where(y > 0, dzr * gam, 0.0).astype(BF16)
                g_own(h).start()
                g_other(h).start()
                for s in range(2):
                    odd_copy(ge, go, s, h + 1)

            @pl.when(j >= 2)
            def _():
                q = j - 2
                rows = jnp.concatenate([xe[s, q + 1, PAD:PAD + 128, :] for s in range(2)], axis=0)
                xt[...] = rows.T
                for ky in range(3):
                    for kx in range(3):
                        t = 3 * ky + kx
                        rhs = jnp.concatenate([tap_rows(ge, go, s, q + 2 - ky, 1 - kx, 128) for s in range(2)], axis=0)
                        part = jnp.dot(xt[...], rhs, preferred_element_type=F32)
                        for k in range(2):
                            acc[k, t] += part[:, k * CO:(k + 1) * CO]

            return 0

        lax.fori_loop(0, H + 2, step, 0)

        def pair(t):
            return remote(acc.at[1 - c, t], prx.at[t], s_ps.at[t], s_pr.at[t], c_dev)

        lax.fori_loop(0, 9, lambda t, _: (pair(t).start(), 0)[1], 0)
        z_l = [pltpu.make_async_copy(zb.at[s, c], z_ref.at[:, :, 2 * s + c], s_zl.at[s]) for s in range(2)]
        z_r = [remote(zb.at[s, 1 - c], z_ref.at[:, :, 2 * s + c], s_zs.at[s], s_zr.at[s], c_dev) for s in range(2)]
        z_w = [remote(zb.at[s, 1 - c], z_ref.at[:, :, 2 * s + 1 - c], s_zs.at[s], s_zr.at[s], c_dev) for s in range(2)]
        for s in range(2):
            z_l[s].start()
            z_r[s].start()

        half = CI // 2

        def own_part(k):
            t = k // 2
            q = pl.multiple_of((k % 2) * half, half)

            @pl.when(k % 2 == 0)
            def _():
                pair(t).wait_recv()

            return acc[c, t, pl.ds(q, half), :] + prx[t, pl.ds(q, half), :]

        def dw_view(k):
            return dw_ref.at[k // 2, pl.ds(pl.multiple_of((k % 2) * half, half), half), :]

        def to_inner(k):
            return remote(pb.at[k], rb.at[k], s_os.at[k], s_or.at[k], inner_dev)

        def from_outer(k):
            return remote(pb.at[k], rb.at[k], s_os.at[k], s_or.at[k], outer_dev)

        def to_mate(k):
            return remote(pb.at[k], mb.at[k], s_ms.at[k], s_mr.at[k], mate_dev)

        def to_outer(k):
            return remote(rb.at[k], dw_view(k), s_ts.at[k], s_tr.at[k], outer_dev)

        def from_inner(k):
            return remote(rb.at[k], dw_view(k), s_ts.at[k], s_tr.at[k], inner_dev)

        def own_out(k):
            return pltpu.make_async_copy(rb.at[k], dw_view(k), s_tl.at[k])

        @pl.when(jnp.logical_not(inner))
        def _():
            def send(k, _):
                pb[k] = own_part(k)
                to_inner(k).start()
                return 0

            lax.fori_loop(0, n_chunk, send, 0)

            def take(k, _):
                from_inner(k).wait_recv()
                to_inner(k).wait_send()
                return 0

            lax.fori_loop(0, n_chunk, take, 0)

        @pl.when(inner)
        def _():
            LAG = 2

            def both(k, _):
                @pl.when(k < n_chunk)
                def _():
                    part = own_part(k)
                    from_outer(k).wait_recv()
                    pb[k] = part + rb[k]
                    to_mate(k).start()

                @pl.when(k >= LAG)
                def _():
                    m = k - LAG
                    to_mate(m).wait_recv()
                    rb[m] = pb[m] + mb[m]
                    to_outer(m).start()
                    own_out(m).start()

                return 0

            lax.fori_loop(0, n_chunk + LAG, both, 0)

            def done(k, _):
                to_mate(k).wait_send()
                to_outer(k).wait_send()
                own_out(k).wait()
                return 0

            lax.fori_loop(0, n_chunk, done, 0)

        def drain(h, _):
            x_fwd(h).wait_send()
            g_own(h).wait_send()
            g_other(h).wait_send()
            return 0

        lax.fori_loop(0, H, drain, 0)

        def drain_w(t, _):
            w_y(t).wait_send()
            pair(t).wait_send()
            return 0

        lax.fori_loop(0, 9, drain_w, 0)
        w_core.wait_send()
        for k in range(2):
            vecs_r[k].wait_send()
            dz_r[k].wait_send()
            z_l[k].wait()
            z_r[k].wait_send()
            z_w[k].wait_recv()


def solution(mesh):
    act_spec = P('stage', ('dp', 'tp'))
    w_spec = P('stage', None, None, None, 'tp')
    vec_spec = P('stage', 'tp')
    chan_spec = P('stage', 'dp', None, None, 'tp')

    def device_step(act_in, w_conv, gamma_vec, beta_vec, z_grad):
        on_conv = lax.axis_index('stage') == 1
        N, H, WD, CI = act_in.shape[1:]
        CO = w_conv.shape[-1]
        R = WD * N
        RP = 128 + 2 * PAD
        n_chunk = 18
        x = act_in[0].transpose(1, 2, 0, 3).reshape(H, R, CI)
        w = w_conv[0].reshape(9, CI, CO)
        dz = z_grad[0].transpose(1, 2, 0, 3).reshape(H, WD, 4, N, CO)
        any_spec = pl.BlockSpec(memory_space=pl.ANY)
        dma = pltpu.SemaphoreType.DMA
        z, dx, dw = pl.pallas_call(
            functools.partial(block_kernel, H, WD, CI, CO, n_chunk),
            out_shape=(
                jax.ShapeDtypeStruct((H, WD, 4, N, CO), BF16),
                jax.ShapeDtypeStruct((H, R, CI), BF16),
                jax.ShapeDtypeStruct((9, CI, CO), F32),
            ),
            in_specs=[any_spec] * 5,
            out_specs=(any_spec,) * 3,
            scratch_shapes=[
                pltpu.VMEM((2, H + 2, RP, CI), BF16),
                pltpu.VMEM((2, H + 2, RP - 16, CI), BF16),
                pltpu.VMEM((2, H + 2, RP, 2 * CO), BF16),
                pltpu.VMEM((2, H + 2, RP - 16, 2 * CO), BF16),
                pltpu.VMEM((4, 9, CI, CO), BF16),
                pltpu.VMEM((2, 2, H, WD, N, CO), BF16),
                pltpu.VMEM((2, 2, H, WD, N, CO), BF16),
                pltpu.VMEM((2, 2, 1, CO), F32),
                pltpu.VMEM((2, 9, CI, CO), F32),
                pltpu.VMEM((9, CI, CO), F32),
                pltpu.VMEM((n_chunk, CI // 2, CO), F32),
                pltpu.VMEM((n_chunk, CI // 2, CO), F32),
                pltpu.VMEM((n_chunk, CI // 2, CO), F32),
                pltpu.VMEM((CI, 256), BF16),
                pltpu.VMEM((H, R, 2 * CO), BF16),
                pltpu.VMEM((H, R, CI), BF16),
                dma((H,)), dma((2, H)), dma((H,)), dma((2, H)), dma((2, H)), dma((H,)), dma((H,)),
                dma, dma((3, 9)), dma((4, 9)), dma((2,)), dma((3,)), dma((3,)), dma((2,)), dma((2,)), dma((2,)),
                dma((2,)), dma((2,)), dma((2,)), dma((9,)), dma((9,)),
                dma((n_chunk,)), dma((n_chunk,)), dma((n_chunk,)), dma((n_chunk,)), dma((n_chunk,)), dma((n_chunk,)), dma((n_chunk,)), dma((H,)),
            ],
            compiler_params=pltpu.CompilerParams(collective_id=0, has_side_effects=True, vmem_limit_bytes=64 * 1024 * 1024 - 65536),
        )(x, w, gamma_vec, beta_vec, dz)
        z_full = z.reshape(H, WD, 4 * N, CO).transpose(2, 0, 1, 3)
        dx_full = dx.reshape(H, WD, N, CI).transpose(2, 0, 1, 3)
        dw_full = dw.reshape(3, 3, CI, CO)
        z_keep = jnp.where(on_conv, z_full, jnp.zeros_like(z_full))
        dx_keep = jnp.where(on_conv, jnp.zeros_like(dx_full), dx_full)
        w_keep = jnp.where(on_conv, dw_full, jnp.zeros_like(dw_full))
        return z_keep[None], dx_keep[None], w_keep[None]

    return jax.shard_map(device_step, mesh=mesh, in_specs=(act_spec, w_spec, vec_spec, vec_spec, chan_spec), out_specs=(chan_spec, act_spec, w_spec), check_vma=False)
```

```python
import functools

import jax
import jax.numpy as jnp
from jax import lax
from jax.experimental import pallas as pl
from jax.experimental.pallas import tpu as pltpu
from jax.sharding import PartitionSpec as P

MESH = pl.DeviceIdType.MESH
F32 = jnp.float32
BF16 = jnp.bfloat16
PAD = 16
AHEAD = 2


def remote(src, dst, send_sem, recv_sem, dev):
    return pltpu.make_async_remote_copy(src_ref=src, dst_ref=dst, send_sem=send_sem, recv_sem=recv_sem, device_id=dev, device_id_type=MESH)


def block_kernel(H, WD, CI, CO, n_chunk, x_ref, w_ref, gam_ref, bet_ref, dz_ref, z_ref, dx_ref, dw_ref,
                 xe, xo, ge, go, wall, dzb, zb, vec, acc, prx, pb, rb, mb, xt, relay, dxb, *sems):
    (s_xs, s_xr, s_xf, s_gs, s_gr, s_gl, s_gf, s_wl, s_ws, s_wr, s_vl, s_vs, s_vr, s_dl, s_ds, s_dr,
     s_zl, s_zs, s_zr, s_ps, s_pr, s_os, s_or, s_ms, s_mr, s_ts, s_tr, s_tl, s_dx) = sems
    R = WD * 8
    CW = 2 * CO
    zi = lax.axis_index("dp")
    st = lax.axis_index("stage")
    tp = lax.axis_index("tp")
    xi = tp // 2
    c = tp % 2
    y_dev = (zi, 1 - st, tp)
    x_dev = (zi, st, 2 * (1 - xi) + c)
    c_dev = (zi, st, 2 * xi + 1 - c)
    z_mate = jnp.where(zi == 1, 2, 1)
    z_out = jnp.where(zi < 2, 0, 3)
    z_in = jnp.where(zi < 2, 1, 2)
    inner = jnp.logical_or(zi == 1, zi == 2)
    mate_dev = (z_mate, st, tp)
    outer_dev = (z_out, st, tp)
    inner_dev = (z_in, st, tp)

    barrier = pltpu.get_barrier_semaphore()
    for dev in (y_dev, x_dev, c_dev):
        pl.semaphore_signal(barrier, inc=1, device_id=dev, device_id_type=MESH)

    @pl.when(inner)
    def _():
        for dev in (mate_dev, outer_dev):
            pl.semaphore_signal(barrier, inc=1, device_id=dev, device_id_type=MESH)
        pl.semaphore_wait(barrier, 5)

    @pl.when(jnp.logical_not(inner))
    def _():
        pl.semaphore_signal(barrier, inc=1, device_id=inner_dev, device_id_type=MESH)
        pl.semaphore_wait(barrier, 4)

    def zero_borders(buf):
        ch = buf.shape[-1]

        def rows(h, _):
            for s in range(2):
                buf[s, h, 0:PAD, :] = jnp.zeros((PAD, ch), BF16)
                buf[s, h, PAD + R:, :] = jnp.zeros((buf.shape[2] - PAD - R, ch), BF16)
            return 0

        lax.fori_loop(0, H + 2, rows, 0)

    def zero_planes(buf):
        for s in range(2):
            for h in (0, H + 1):
                buf[s, h] = jnp.zeros(buf.shape[2:], BF16)

    def odd_copy(even, odd, s, h):
        n = odd.shape[2]
        odd[s, h] = even[s, h, 8:8 + n, :]

    def tap_rows(even, odd, s, plane, shift, n):
        if shift == 0:
            return even[s, plane, PAD:PAD + n, :]
        start = PAD + 8 * shift - 8
        return odd[s, plane, start:start + n, :]

    @pl.when(st == 0)
    def _():
        def x_copy(h):
            return remote(x_ref.at[h], xe.at[xi, h + 1, pl.ds(PAD, R), :], s_xs.at[h], s_xr.at[xi, h], y_dev)

        lax.fori_loop(0, H, lambda h, _: (x_copy(h).start(), 0)[1], 0)
        zero_borders(ge)
        zero_planes(ge)
        zero_planes(go)

        def w_in(t, b):
            return remote(wall.at[b, t], wall.at[b, t], s_ws.at[0, t], s_wr.at[b, t], y_dev)

        def w_fwd(t, b, k, dev):
            return remote(wall.at[b, t], wall.at[b, t], s_ws.at[k, t], s_wr.at[b, t], dev)

        b_x = 2 * (1 - xi) + c

        def w_step(t, _):
            w_in(t, tp).wait_recv()
            w_fwd(t, tp, 0, c_dev).start()
            w_fwd(t, tp, 1, x_dev).start()
            return 0

        lax.fori_loop(0, 9, w_step, 0)

        def w_step2(t, _):
            w_in(t, b_x).wait_recv()
            w_fwd(t, b_x, 2, c_dev).start()
            return 0

        lax.fori_loop(0, 9, w_step2, 0)

        def w_step3(t, _):
            w_in(t, 2 * xi + 1 - c).wait_recv()
            w_in(t, 2 * (1 - xi) + 1 - c).wait_recv()
            return 0

        lax.fori_loop(0, 9, w_step3, 0)

        def g_in(j, b):
            return remote(ge.at[b, j + 1, pl.ds(PAD, R), :], ge.at[b, j + 1, pl.ds(PAD, R), :], s_gf.at[j], s_gr.at[b, j], y_dev)

        def relay_in(j):
            return remote(relay.at[j], relay.at[j], s_gf.at[j], s_gl.at[j], y_dev)

        def relay_out(j):
            return remote(relay.at[j], ge.at[xi, j + 1, pl.ds(PAD, R), :], s_gf.at[j], s_gr.at[xi, j], x_dev)

        def dx_out(h):
            return pltpu.make_async_copy(dxb.at[h], dx_ref.at[h], s_dx.at[h])

        def g_relay(j):
            relay_in(j).wait_recv()
            relay_out(j).start()

        lax.fori_loop(0, AHEAD, lambda j, _: (g_relay(j), 0)[1], 0)

        def g_step(j, _):
            @pl.when(j + AHEAD < H)
            def _():
                g_relay(j + AHEAD)

            @pl.when(j < H)
            def _():
                g_in(j, xi).wait_recv()
                g_in(j, 1 - xi).wait_recv()
                for b in range(2):
                    odd_copy(ge, go, b, j + 1)

            @pl.when(j >= 1)
            def _():
                h = j - 1
                tot = jnp.zeros((R, CI), F32)
                for b in range(2):
                    for ky in range(3):
                        for kx in range(3):
                            t = 3 * ky + kx
                            lhs = tap_rows(ge, go, b, h + 2 - ky, 1 - kx, R)
                            rhs = jnp.concatenate([wall[2 * b, t], wall[2 * b + 1, t]], axis=1)
                            tot = tot + lax.dot_general(lhs, rhs, (((1,), (1,)), ((), ())), preferred_element_type=F32)
                dxb[h] = tot.astype(BF16)
                dx_out(h).start()

            return 0

        lax.fori_loop(0, H + 1, g_step, 0)

        def drain(h, _):
            x_copy(h).wait_send()
            relay_out(h).wait_send()
            dx_out(h).wait()
            return 0

        lax.fori_loop(0, H, drain, 0)

        def drain_w(t, _):
            w_fwd(t, tp, 0, c_dev).wait_send()
            w_fwd(t, tp, 1, x_dev).wait_send()
            w_fwd(t, b_x, 2, c_dev).wait_send()
            return 0

        lax.fori_loop(0, 9, drain_w, 0)

    @pl.when(st == 1)
    def _():
        w_loc = pltpu.make_async_copy(w_ref, wall.at[c], s_wl)
        w_core = remote(w_ref, wall.at[c], s_vs.at[2], s_vr.at[2], c_dev)
        vecs_l = [pltpu.make_async_copy(r, vec.at[k, c], s_vl.at[k]) for k, r in enumerate((gam_ref, bet_ref))]
        vecs_r = [remote(r, vec.at[k, c], s_vs.at[k], s_vr.at[k], c_dev) for k, r in enumerate((gam_ref, bet_ref))]
        dz_l = [pltpu.make_async_copy(dz_ref.at[:, :, 2 * s + c], dzb.at[s, c], s_dl.at[s]) for s in range(2)]
        dz_r = [remote(dz_ref.at[:, :, 2 * s + 1 - c], dzb.at[s, c], s_ds.at[s], s_dr.at[s], c_dev) for s in range(2)]

        def w_y(t):
            return remote(w_ref.at[t], wall.at[tp, t], s_ws.at[0, t], s_wr.at[tp, t], y_dev)

        w_loc.start()
        w_core.start()
        for k in range(2):
            vecs_l[k].start()
            vecs_r[k].start()
            dz_l[k].start()
            dz_r[k].start()
        lax.fori_loop(0, 9, lambda t, _: (w_y(t).start(), 0)[1], 0)

        zero_borders(xe)
        zero_borders(ge)
        for buf in (xe, xo, ge, go):
            zero_planes(buf)

        def zero_acc(t, _):
            for k in range(2):
                acc[k, t] = jnp.zeros((CI, CO), F32)
            return 0

        lax.fori_loop(0, 9, zero_acc, 0)
        for k in range(2):
            vecs_l[k].wait()
            vecs_r[k].wait_recv()
            dz_l[k].wait()
            dz_r[k].wait_recv()
        w_loc.wait()
        w_core.wait_recv()

        def x_in(j, s):
            view = xe.at[s, j + 1, pl.ds(PAD, R), :]
            return remote(view, view, s_xf.at[j], s_xr.at[s, j], y_dev)

        def x_fwd(j):
            view = xe.at[xi, j + 1, pl.ds(PAD, R), :]
            return remote(view, view, s_xf.at[j], s_xr.at[xi, j], x_dev)

        def g_own(h):
            return remote(ge.at[xi, h + 1, pl.ds(PAD, R), :], ge.at[xi, h + 1, pl.ds(PAD, R), :], s_gs.at[0, h], s_gr.at[xi, h], y_dev)

        def g_other(h):
            return remote(ge.at[1 - xi, h + 1, pl.ds(PAD, R), :], relay.at[h], s_gs.at[1, h], s_gl.at[h], y_dev)

        def x_relay(j):
            x_in(j, xi).wait_recv()
            x_fwd(j).start()

        lax.fori_loop(0, AHEAD, lambda j, _: (x_relay(j), 0)[1], 0)

        def step(j, _):
            @pl.when(j + AHEAD < H)
            def _():
                x_relay(j + AHEAD)

            @pl.when(j < H)
            def _():
                x_in(j, 1 - xi).wait_recv()
                for s in range(2):
                    odd_copy(xe, xo, s, j + 1)

            @pl.when(jnp.logical_and(j >= 1, j < H + 1))
            def _():
                h = j - 1
                pre = jnp.zeros((2 * R, CW), F32)
                for ky in range(3):
                    for kx in range(3):
                        t = 3 * ky + kx
                        lhs = jnp.concatenate([tap_rows(xe, xo, s, h + ky, kx - 1, R) for s in range(2)], axis=0)
                        rhs = jnp.concatenate([wall[0, t], wall[1, t]], axis=1)
                        pre = pre + jnp.dot(lhs, rhs, preferred_element_type=F32)
                for k in range(2):
                    gam = vec[0, k]
                    bet = vec[1, k]
                    for s in range(2):
                        y = pre[s * R:(s + 1) * R, k * CO:(k + 1) * CO] * gam + bet
                        zb[s, k, h] = jnp.maximum(y, 0.0).reshape(WD, 8, CO).astype(BF16)
                        dzr = dzb[s, k, h].astype(F32).reshape(R, CO)
                        ge[s, h + 1, PAD:PAD + R, k * CO:(k + 1) * CO] = jnp.where(y > 0, dzr * gam, 0.0).astype(BF16)
                g_own(h).start()
                g_other(h).start()
                for s in range(2):
                    odd_copy(ge, go, s, h + 1)

            @pl.when(j >= 2)
            def _():
                q = j - 2
                rows = jnp.concatenate([xe[s, q + 1, PAD:PAD + 128, :] for s in range(2)], axis=0)
                xt[...] = rows.T
                for ky in range(3):
                    for kx in range(3):
                        t = 3 * ky + kx
                        rhs = jnp.concatenate([tap_rows(ge, go, s, q + 2 - ky, 1 - kx, 128) for s in range(2)], axis=0)
                        part = jnp.dot(xt[...], rhs, preferred_element_type=F32)
                        for k in range(2):
                            acc[k, t] += part[:, k * CO:(k + 1) * CO]

            return 0

        lax.fori_loop(0, H + 2, step, 0)

        def pair(t):
            return remote(acc.at[1 - c, t], prx.at[t], s_ps.at[t], s_pr.at[t], c_dev)

        lax.fori_loop(0, 9, lambda t, _: (pair(t).start(), 0)[1], 0)
        z_l = [pltpu.make_async_copy(zb.at[s, c], z_ref.at[:, :, 2 * s + c], s_zl.at[s]) for s in range(2)]
        z_r = [remote(zb.at[s, 1 - c], z_ref.at[:, :, 2 * s + c], s_zs.at[s], s_zr.at[s], c_dev) for s in range(2)]
        z_w = [remote(zb.at[s, 1 - c], z_ref.at[:, :, 2 * s + 1 - c], s_zs.at[s], s_zr.at[s], c_dev) for s in range(2)]
        for s in range(2):
            z_l[s].start()
            z_r[s].start()

        half = CI // 2

        def own_part(k):
            t = k // 2
            q = pl.multiple_of((k % 2) * half, half)

            @pl.when(k % 2 == 0)
            def _():
                pair(t).wait_recv()

            return acc[c, t, pl.ds(q, half), :] + prx[t, pl.ds(q, half), :]

        def dw_view(k):
            return dw_ref.at[k // 2, pl.ds(pl.multiple_of((k % 2) * half, half), half), :]

        def to_inner(k):
            return remote(pb.at[k], rb.at[k], s_os.at[k], s_or.at[k], inner_dev)

        def from_outer(k):
            return remote(pb.at[k], rb.at[k], s_os.at[k], s_or.at[k], outer_dev)

        def to_mate(k):
            return remote(pb.at[k], mb.at[k], s_ms.at[k], s_mr.at[k], mate_dev)

        def to_outer(k):
            return remote(rb.at[k], dw_view(k), s_ts.at[k], s_tr.at[k], outer_dev)

        def from_inner(k):
            return remote(rb.at[k], dw_view(k), s_ts.at[k], s_tr.at[k], inner_dev)

        def own_out(k):
            return pltpu.make_async_copy(rb.at[k], dw_view(k), s_tl.at[k])

        @pl.when(jnp.logical_not(inner))
        def _():
            def send(k, _):
                pb[k] = own_part(k)
                to_inner(k).start()
                return 0

            lax.fori_loop(0, n_chunk, send, 0)

            def take(k, _):
                from_inner(k).wait_recv()
                to_inner(k).wait_send()
                return 0

            lax.fori_loop(0, n_chunk, take, 0)

        @pl.when(inner)
        def _():
            LAG = 2

            def both(k, _):
                @pl.when(k < n_chunk)
                def _():
                    part = own_part(k)
                    from_outer(k).wait_recv()
                    pb[k] = part + rb[k]
                    to_mate(k).start()

                @pl.when(k >= LAG)
                def _():
                    m = k - LAG
                    to_mate(m).wait_recv()
                    rb[m] = pb[m] + mb[m]
                    to_outer(m).start()
                    own_out(m).start()

                return 0

            lax.fori_loop(0, n_chunk + LAG, both, 0)

            def done(k, _):
                to_mate(k).wait_send()
                to_outer(k).wait_send()
                own_out(k).wait()
                return 0

            lax.fori_loop(0, n_chunk, done, 0)

        def drain(h, _):
            x_fwd(h).wait_send()
            g_own(h).wait_send()
            g_other(h).wait_send()
            return 0

        lax.fori_loop(0, H, drain, 0)

        def drain_w(t, _):
            w_y(t).wait_send()
            pair(t).wait_send()
            return 0

        lax.fori_loop(0, 9, drain_w, 0)
        w_core.wait_send()
        for k in range(2):
            vecs_r[k].wait_send()
            dz_r[k].wait_send()
            z_l[k].wait()
            z_r[k].wait_send()
            z_w[k].wait_recv()


def solution(mesh):
    act_spec = P('stage', ('dp', 'tp'))
    w_spec = P('stage', None, None, None, 'tp')
    vec_spec = P('stage', 'tp')
    chan_spec = P('stage', 'dp', None, None, 'tp')

    def device_step(act_in, w_conv, gamma_vec, beta_vec, z_grad):
        on_conv = lax.axis_index('stage') == 1
        N, H, WD, CI = act_in.shape[1:]
        CO = w_conv.shape[-1]
        R = WD * N
        RP = 128 + 2 * PAD
        n_chunk = 18
        x = act_in[0].transpose(1, 2, 0, 3).reshape(H, R, CI)
        w = w_conv[0].reshape(9, CI, CO)
        dz = z_grad[0].transpose(1, 2, 0, 3).reshape(H, WD, 4, N, CO)
        any_spec = pl.BlockSpec(memory_space=pl.ANY)
        dma = pltpu.SemaphoreType.DMA
        z, dx, dw = pl.pallas_call(
            functools.partial(block_kernel, H, WD, CI, CO, n_chunk),
            out_shape=(
                jax.ShapeDtypeStruct((H, WD, 4, N, CO), BF16),
                jax.ShapeDtypeStruct((H, R, CI), BF16),
                jax.ShapeDtypeStruct((9, CI, CO), F32),
            ),
            in_specs=[any_spec] * 5,
            out_specs=(any_spec,) * 3,
            scratch_shapes=[
                pltpu.VMEM((2, H + 2, RP, CI), BF16),
                pltpu.VMEM((2, H + 2, RP - 16, CI), BF16),
                pltpu.VMEM((2, H + 2, RP, 2 * CO), BF16),
                pltpu.VMEM((2, H + 2, RP - 16, 2 * CO), BF16),
                pltpu.VMEM((4, 9, CI, CO), BF16),
                pltpu.VMEM((2, 2, H, WD, N, CO), BF16),
                pltpu.VMEM((2, 2, H, WD, N, CO), BF16),
                pltpu.VMEM((2, 2, 1, CO), F32),
                pltpu.VMEM((2, 9, CI, CO), F32),
                pltpu.VMEM((9, CI, CO), F32),
                pltpu.VMEM((n_chunk, CI // 2, CO), F32),
                pltpu.VMEM((n_chunk, CI // 2, CO), F32),
                pltpu.VMEM((n_chunk, CI // 2, CO), F32),
                pltpu.VMEM((CI, 256), BF16),
                pltpu.VMEM((H, R, 2 * CO), BF16),
                pltpu.VMEM((H, R, CI), BF16),
                dma((H,)), dma((2, H)), dma((H,)), dma((2, H)), dma((2, H)), dma((H,)), dma((H,)),
                dma, dma((3, 9)), dma((4, 9)), dma((2,)), dma((3,)), dma((3,)), dma((2,)), dma((2,)), dma((2,)),
                dma((2,)), dma((2,)), dma((2,)), dma((9,)), dma((9,)),
                dma((n_chunk,)), dma((n_chunk,)), dma((n_chunk,)), dma((n_chunk,)), dma((n_chunk,)), dma((n_chunk,)), dma((n_chunk,)), dma((H,)),
            ],
            compiler_params=pltpu.CompilerParams(collective_id=0, has_side_effects=True, vmem_limit_bytes=64 * 1024 * 1024 - 65536),
        )(x, w, gamma_vec, beta_vec, dz)
        z_full = z.reshape(H, WD, 4 * N, CO).transpose(2, 0, 1, 3)
        dx_full = dx.reshape(H, WD, N, CI).transpose(2, 0, 1, 3)
        dw_full = dw.reshape(3, 3, CI, CO)
        z_keep = jnp.where(on_conv, z_full, jnp.zeros_like(z_full))
        dx_keep = jnp.where(on_conv, jnp.zeros_like(dx_full), dx_full)
        w_keep = jnp.where(on_conv, dw_full, jnp.zeros_like(dw_full))
        return z_keep[None], dx_keep[None], w_keep[None]

    return jax.shard_map(device_step, mesh=mesh, in_specs=(act_spec, w_spec, vec_spec, vec_spec, chan_spec), out_specs=(chan_spec, act_spec, w_spec), check_vma=False)
```

```python
import functools

import jax
import jax.numpy as jnp
from jax import lax
from jax.experimental import pallas as pl
from jax.experimental.pallas import tpu as pltpu
from jax.sharding import PartitionSpec as P

MESH = pl.DeviceIdType.MESH
F32 = jnp.float32
BF16 = jnp.bfloat16
PAD = 16
AHEAD = 2


def remote(src, dst, send_sem, recv_sem, dev):
    return pltpu.make_async_remote_copy(src_ref=src, dst_ref=dst, send_sem=send_sem, recv_sem=recv_sem, device_id=dev, device_id_type=MESH)


def block_kernel(H, WD, CI, CO, n_chunk, x_ref, w_ref, gam_ref, bet_ref, dz_ref, z_ref, dx_ref, dw_ref,
                 xe, xo, ge, go, wall, dzb, zb, vec, acc, prx, pb, rb, mb, xt, relay, *sems):
    (s_xs, s_xr, s_xf, s_gs, s_gr, s_gl, s_gf, s_wl, s_ws, s_wr, s_vl, s_vs, s_vr, s_dl, s_ds, s_dr,
     s_zs, s_zr, s_ps, s_pr, s_os, s_or, s_ms, s_mr, s_ts, s_tr) = sems
    R = WD * 8
    CW = 2 * CO
    zi = lax.axis_index("dp")
    st = lax.axis_index("stage")
    tp = lax.axis_index("tp")
    xi = tp // 2
    c = tp % 2
    y_dev = (zi, 1 - st, tp)
    x_dev = (zi, st, 2 * (1 - xi) + c)
    c_dev = (zi, st, 2 * xi + 1 - c)
    z_mate = jnp.where(zi == 1, 2, 1)
    z_out = jnp.where(zi < 2, 0, 3)
    z_in = jnp.where(zi < 2, 1, 2)
    inner = jnp.logical_or(zi == 1, zi == 2)
    mate_dev = (z_mate, st, tp)
    outer_dev = (z_out, st, tp)
    inner_dev = (z_in, st, tp)

    barrier = pltpu.get_barrier_semaphore()
    for dev in (y_dev, x_dev, c_dev):
        pl.semaphore_signal(barrier, inc=1, device_id=dev, device_id_type=MESH)

    @pl.when(inner)
    def _():
        for dev in (mate_dev, outer_dev):
            pl.semaphore_signal(barrier, inc=1, device_id=dev, device_id_type=MESH)
        pl.semaphore_wait(barrier, 5)

    @pl.when(jnp.logical_not(inner))
    def _():
        pl.semaphore_signal(barrier, inc=1, device_id=inner_dev, device_id_type=MESH)
        pl.semaphore_wait(barrier, 4)

    def zero_borders(buf):
        ch = buf.shape[-1]

        def rows(h, _):
            for s in range(2):
                buf[s, h, 0:PAD, :] = jnp.zeros((PAD, ch), BF16)
                buf[s, h, PAD + R:, :] = jnp.zeros((buf.shape[2] - PAD - R, ch), BF16)
            return 0

        lax.fori_loop(0, H + 2, rows, 0)

    def zero_planes(buf):
        for s in range(2):
            for h in (0, H + 1):
                buf[s, h] = jnp.zeros(buf.shape[2:], BF16)

    def odd_copy(even, odd, s, h):
        n = odd.shape[2]
        odd[s, h] = even[s, h, 8:8 + n, :]

    def tap_rows(even, odd, s, plane, shift, n):
        if shift == 0:
            return even[s, plane, PAD:PAD + n, :]
        start = PAD + 8 * shift - 8
        return odd[s, plane, start:start + n, :]

    @pl.when(st == 0)
    def _():
        def x_copy(h):
            return remote(x_ref.at[h], xe.at[xi, h + 1, pl.ds(PAD, R), :], s_xs.at[h], s_xr.at[xi, h], y_dev)

        lax.fori_loop(0, H, lambda h, _: (x_copy(h).start(), 0)[1], 0)
        zero_borders(ge)
        zero_planes(ge)
        zero_planes(go)

        def zero_out(h, _):
            z_ref[h] = jnp.zeros(z_ref.shape[1:], BF16)
            return 0

        lax.fori_loop(0, H, zero_out, 0)

        def zero_dw(t, _):
            dw_ref[t] = jnp.zeros((CI, CO), F32)
            return 0

        lax.fori_loop(0, 9, zero_dw, 0)

        def w_in(t, b):
            return remote(wall.at[b, t], wall.at[b, t], s_ws.at[0, t], s_wr.at[b, t], y_dev)

        def w_fwd(t, b, k, dev):
            return remote(wall.at[b, t], wall.at[b, t], s_ws.at[k, t], s_wr.at[b, t], dev)

        b_x = 2 * (1 - xi) + c

        def w_step(t, _):
            w_in(t, tp).wait_recv()
            w_fwd(t, tp, 0, c_dev).start()
            w_fwd(t, tp, 1, x_dev).start()
            return 0

        lax.fori_loop(0, 9, w_step, 0)

        def w_step2(t, _):
            w_in(t, b_x).wait_recv()
            w_fwd(t, b_x, 2, c_dev).start()
            return 0

        lax.fori_loop(0, 9, w_step2, 0)

        def w_step3(t, _):
            w_in(t, 2 * xi + 1 - c).wait_recv()
            w_in(t, 2 * (1 - xi) + 1 - c).wait_recv()
            return 0

        lax.fori_loop(0, 9, w_step3, 0)

        def g_in(j, b):
            return remote(ge.at[b, j + 1, pl.ds(PAD, R), :], ge.at[b, j + 1, pl.ds(PAD, R), :], s_gf.at[j], s_gr.at[b, j], y_dev)

        def relay_in(j):
            return remote(relay.at[j], relay.at[j], s_gf.at[j], s_gl.at[j], y_dev)

        def relay_out(j):
            return remote(relay.at[j], ge.at[xi, j + 1, pl.ds(PAD, R), :], s_gf.at[j], s_gr.at[xi, j], x_dev)

        def g_relay(j):
            relay_in(j).wait_recv()
            relay_out(j).start()

        lax.fori_loop(0, AHEAD, lambda j, _: (g_relay(j), 0)[1], 0)

        def g_step(j, _):
            @pl.when(j + AHEAD < H)
            def _():
                g_relay(j + AHEAD)

            @pl.when(j < H)
            def _():
                g_in(j, xi).wait_recv()
                g_in(j, 1 - xi).wait_recv()
                for b in range(2):
                    odd_copy(ge, go, b, j + 1)

            @pl.when(j >= 1)
            def _():
                h = j - 1
                tot = jnp.zeros((R, CI), F32)
                for b in range(2):
                    for ky in range(3):
                        for kx in range(3):
                            t = 3 * ky + kx
                            lhs = tap_rows(ge, go, b, h + 2 - ky, 1 - kx, R)
                            rhs = jnp.concatenate([wall[2 * b, t], wall[2 * b + 1, t]], axis=1)
                            tot = tot + lax.dot_general(lhs, rhs, (((1,), (1,)), ((), ())), preferred_element_type=F32)
                dx_ref[h] = tot.astype(BF16)

            return 0

        lax.fori_loop(0, H + 1, g_step, 0)

        def drain(h, _):
            x_copy(h).wait_send()
            relay_out(h).wait_send()
            return 0

        lax.fori_loop(0, H, drain, 0)

        def drain_w(t, _):
            w_fwd(t, tp, 0, c_dev).wait_send()
            w_fwd(t, tp, 1, x_dev).wait_send()
            w_fwd(t, b_x, 2, c_dev).wait_send()
            return 0

        lax.fori_loop(0, 9, drain_w, 0)

    @pl.when(st == 1)
    def _():
        w_loc = pltpu.make_async_copy(w_ref, wall.at[c], s_wl)
        w_core = remote(w_ref, wall.at[c], s_vs.at[2], s_vr.at[2], c_dev)
        vecs_l = [pltpu.make_async_copy(r, vec.at[k, c], s_vl.at[k]) for k, r in enumerate((gam_ref, bet_ref))]
        vecs_r = [remote(r, vec.at[k, c], s_vs.at[k], s_vr.at[k], c_dev) for k, r in enumerate((gam_ref, bet_ref))]
        dz_l = [pltpu.make_async_copy(dz_ref.at[:, :, 2 * s + c], dzb.at[s, c], s_dl.at[s]) for s in range(2)]
        dz_r = [remote(dz_ref.at[:, :, 2 * s + 1 - c], dzb.at[s, c], s_ds.at[s], s_dr.at[s], c_dev) for s in range(2)]

        def w_y(t):
            return remote(w_ref.at[t], wall.at[tp, t], s_ws.at[0, t], s_wr.at[tp, t], y_dev)

        w_loc.start()
        w_core.start()
        for k in range(2):
            vecs_l[k].start()
            vecs_r[k].start()
            dz_l[k].start()
            dz_r[k].start()
        lax.fori_loop(0, 9, lambda t, _: (w_y(t).start(), 0)[1], 0)

        zero_borders(xe)
        zero_borders(ge)
        for buf in (xe, xo, ge, go):
            zero_planes(buf)

        def zero_acc(t, _):
            for k in range(2):
                acc[k, t] = jnp.zeros((CI, CO), F32)
            return 0

        lax.fori_loop(0, 9, zero_acc, 0)

        def zero_dx(h, _):
            dx_ref[h] = jnp.zeros((R, CI), BF16)
            return 0

        lax.fori_loop(0, H, zero_dx, 0)
        for k in range(2):
            vecs_l[k].wait()
            vecs_r[k].wait_recv()
            dz_l[k].wait()
            dz_r[k].wait_recv()
        w_loc.wait()
        w_core.wait_recv()

        def x_in(j, s):
            view = xe.at[s, j + 1, pl.ds(PAD, R), :]
            return remote(view, view, s_xf.at[j], s_xr.at[s, j], y_dev)

        def x_fwd(j):
            view = xe.at[xi, j + 1, pl.ds(PAD, R), :]
            return remote(view, view, s_xf.at[j], s_xr.at[xi, j], x_dev)

        def g_own(h):
            return remote(ge.at[xi, h + 1, pl.ds(PAD, R), :], ge.at[xi, h + 1, pl.ds(PAD, R), :], s_gs.at[0, h], s_gr.at[xi, h], y_dev)

        def g_other(h):
            return remote(ge.at[1 - xi, h + 1, pl.ds(PAD, R), :], relay.at[h], s_gs.at[1, h], s_gl.at[h], y_dev)

        def x_relay(j):
            x_in(j, xi).wait_recv()
            x_fwd(j).start()

        lax.fori_loop(0, AHEAD, lambda j, _: (x_relay(j), 0)[1], 0)

        def step(j, _):
            @pl.when(j + AHEAD < H)
            def _():
                x_relay(j + AHEAD)

            @pl.when(j < H)
            def _():
                x_in(j, 1 - xi).wait_recv()
                for s in range(2):
                    odd_copy(xe, xo, s, j + 1)

            @pl.when(jnp.logical_and(j >= 1, j < H + 1))
            def _():
                h = j - 1
                pre = jnp.zeros((2 * R, CW), F32)
                for ky in range(3):
                    for kx in range(3):
                        t = 3 * ky + kx
                        lhs = jnp.concatenate([tap_rows(xe, xo, s, h + ky, kx - 1, R) for s in range(2)], axis=0)
                        rhs = jnp.concatenate([wall[0, t], wall[1, t]], axis=1)
                        pre = pre + jnp.dot(lhs, rhs, preferred_element_type=F32)
                for k in range(2):
                    gam = vec[0, k]
                    bet = vec[1, k]
                    for s in range(2):
                        y = pre[s * R:(s + 1) * R, k * CO:(k + 1) * CO] * gam + bet
                        zb[s, k, h] = jnp.maximum(y, 0.0).reshape(WD, 8, CO).astype(BF16)
                        dzr = dzb[s, k, h].astype(F32).reshape(R, CO)
                        ge[s, h + 1, PAD:PAD + R, k * CO:(k + 1) * CO] = jnp.where(y > 0, dzr * gam, 0.0).astype(BF16)
                g_own(h).start()
                g_other(h).start()
                for s in range(2):
                    odd_copy(ge, go, s, h + 1)
                    z_ref[h, :, 2 * s + c] = zb[s, c, h]

            @pl.when(j >= 2)
            def _():
                q = j - 2
                rows = jnp.concatenate([xe[s, q + 1, PAD:PAD + 128, :] for s in range(2)], axis=0)
                xt[...] = rows.T
                for ky in range(3):
                    for kx in range(3):
                        t = 3 * ky + kx
                        rhs = jnp.concatenate([tap_rows(ge, go, s, q + 2 - ky, 1 - kx, 128) for s in range(2)], axis=0)
                        part = jnp.dot(xt[...], rhs, preferred_element_type=F32)
                        for k in range(2):
                            acc[k, t] += part[:, k * CO:(k + 1) * CO]

            return 0

        lax.fori_loop(0, H + 2, step, 0)

        def pair(t):
            return remote(acc.at[1 - c, t], prx.at[t], s_ps.at[t], s_pr.at[t], c_dev)

        lax.fori_loop(0, 9, lambda t, _: (pair(t).start(), 0)[1], 0)
        z_r = [remote(zb.at[s, 1 - c], z_ref.at[:, :, 2 * s + c], s_zs.at[s], s_zr.at[s], c_dev) for s in range(2)]
        z_w = [remote(zb.at[s, 1 - c], z_ref.at[:, :, 2 * s + 1 - c], s_zs.at[s], s_zr.at[s], c_dev) for s in range(2)]
        for s in range(2):
            z_r[s].start()

        half = CI // 2

        def own_part(k):
            t = k // 2
            q = pl.multiple_of((k % 2) * half, half)

            @pl.when(k % 2 == 0)
            def _():
                pair(t).wait_recv()

            return acc[c, t, pl.ds(q, half), :] + prx[t, pl.ds(q, half), :]

        def dw_view(k):
            return dw_ref.at[k // 2, pl.ds(pl.multiple_of((k % 2) * half, half), half), :]

        def to_inner(k):
            return remote(pb.at[k], rb.at[k], s_os.at[k], s_or.at[k], inner_dev)

        def from_outer(k):
            return remote(pb.at[k], rb.at[k], s_os.at[k], s_or.at[k], outer_dev)

        def to_mate(k):
            return remote(pb.at[k], mb.at[k], s_ms.at[k], s_mr.at[k], mate_dev)

        def to_outer(k):
            return remote(dw_view(k), dw_view(k), s_ts.at[k], s_tr.at[k], outer_dev)

        def from_inner(k):
            return remote(dw_view(k), dw_view(k), s_ts.at[k], s_tr.at[k], inner_dev)

        @pl.when(jnp.logical_not(inner))
        def _():
            def send(k, _):
                pb[k] = own_part(k)
                to_inner(k).start()
                return 0

            lax.fori_loop(0, n_chunk, send, 0)

            def take(k, _):
                from_inner(k).wait_recv()
                to_inner(k).wait_send()
                return 0

            lax.fori_loop(0, n_chunk, take, 0)

        @pl.when(inner)
        def _():
            LAG = 2

            def both(k, _):
                @pl.when(k < n_chunk)
                def _():
                    part = own_part(k)
                    from_outer(k).wait_recv()
                    pb[k] = part + rb[k]
                    to_mate(k).start()

                @pl.when(k >= LAG)
                def _():
                    m = k - LAG
                    to_mate(m).wait_recv()
                    dw_ref[m // 2, pl.ds(pl.multiple_of((m % 2) * half, half), half), :] = pb[m] + mb[m]
                    to_outer(m).start()

                return 0

            lax.fori_loop(0, n_chunk + LAG, both, 0)

            def done(k, _):
                to_mate(k).wait_send()
                to_outer(k).wait_send()
                return 0

            lax.fori_loop(0, n_chunk, done, 0)

        def drain(h, _):
            x_fwd(h).wait_send()
            g_own(h).wait_send()
            g_other(h).wait_send()
            return 0

        lax.fori_loop(0, H, drain, 0)

        def drain_w(t, _):
            w_y(t).wait_send()
            pair(t).wait_send()
            return 0

        lax.fori_loop(0, 9, drain_w, 0)
        w_core.wait_send()
        for k in range(2):
            vecs_r[k].wait_send()
            dz_r[k].wait_send()
            z_r[k].wait_send()
            z_w[k].wait_recv()


def out_kernel(*refs):
    srcs, dsts, sem = refs[:3], refs[3:6], refs[6]
    copies = [pltpu.make_async_copy(a, b, sem.at[i]) for i, (a, b) in enumerate(zip(srcs, dsts))]
    for cp in copies:
        cp.start()
    for cp in copies:
        cp.wait()


def write_out(*arrays):
    return pl.pallas_call(
        out_kernel,
        out_shape=tuple(jax.ShapeDtypeStruct(a.shape, a.dtype) for a in arrays),
        in_specs=[pl.BlockSpec(memory_space=pltpu.VMEM)] * 3,
        out_specs=(pl.BlockSpec(memory_space=pl.ANY),) * 3,
        scratch_shapes=[pltpu.SemaphoreType.DMA((3,))],
        compiler_params=pltpu.CompilerParams(vmem_limit_bytes=16 * 1024 * 1024),
    )(*arrays)


def solution(mesh):
    act_spec = P('stage', ('dp', 'tp'))
    w_spec = P('stage', None, None, None, 'tp')
    vec_spec = P('stage', 'tp')
    chan_spec = P('stage', 'dp', None, None, 'tp')

    def device_step(act_in, w_conv, gamma_vec, beta_vec, z_grad):
        N, H, WD, CI = act_in.shape[1:]
        CO = w_conv.shape[-1]
        R = WD * N
        RP = 128 + 2 * PAD
        n_chunk = 18
        x = act_in[0].transpose(1, 2, 0, 3).reshape(H, R, CI)
        w = w_conv[0].reshape(9, CI, CO)
        dz = z_grad[0].transpose(1, 2, 0, 3).reshape(H, WD, 4, N, CO)
        dma = pltpu.SemaphoreType.DMA
        z, dx, dw = pl.pallas_call(
            functools.partial(block_kernel, H, WD, CI, CO, n_chunk),
            out_shape=(
                jax.ShapeDtypeStruct((H, WD, 4, N, CO), BF16),
                jax.ShapeDtypeStruct((H, R, CI), BF16),
                jax.ShapeDtypeStruct((9, CI, CO), F32),
            ),
            in_specs=[pl.BlockSpec(memory_space=pltpu.HBM)] * 5,
            out_specs=(pl.BlockSpec(memory_space=pltpu.VMEM),) * 3,
            scratch_shapes=[
                pltpu.VMEM((2, H + 2, RP, CI), BF16),
                pltpu.VMEM((2, H + 2, RP - 16, CI), BF16),
                pltpu.VMEM((2, H + 2, RP, 2 * CO), BF16),
                pltpu.VMEM((2, H + 2, RP - 16, 2 * CO), BF16),
                pltpu.VMEM((4, 9, CI, CO), BF16),
                pltpu.VMEM((2, 2, H, WD, N, CO), BF16),
                pltpu.VMEM((2, 2, H, WD, N, CO), BF16),
                pltpu.VMEM((2, 2, 1, CO), F32),
                pltpu.VMEM((2, 9, CI, CO), F32),
                pltpu.VMEM((9, CI, CO), F32),
                pltpu.VMEM((n_chunk, CI // 2, CO), F32),
                pltpu.VMEM((n_chunk, CI // 2, CO), F32),
                pltpu.VMEM((n_chunk, CI // 2, CO), F32),
                pltpu.VMEM((CI, 256), BF16),
                pltpu.VMEM((H, R, 2 * CO), BF16),
                dma((H,)), dma((2, H)), dma((H,)), dma((2, H)), dma((2, H)), dma((H,)), dma((H,)),
                dma, dma((3, 9)), dma((4, 9)), dma((2,)), dma((3,)), dma((3,)), dma((2,)), dma((2,)), dma((2,)),
                dma((2,)), dma((2,)), dma((9,)), dma((9,)),
                dma((n_chunk,)), dma((n_chunk,)), dma((n_chunk,)), dma((n_chunk,)), dma((n_chunk,)), dma((n_chunk,)),
            ],
            compiler_params=pltpu.CompilerParams(collective_id=0, has_side_effects=True, vmem_limit_bytes=46 * 1024 * 1024),
        )(*[pltpu.with_memory_space_constraint(a, pltpu.HBM) for a in (x, w, gamma_vec, beta_vec, dz)])
        z, dx, dw = write_out(z, dx, dw)
        z_full = z.reshape(H, WD, 4 * N, CO).transpose(2, 0, 1, 3)
        dx_full = dx.reshape(H, WD, N, CI).transpose(2, 0, 1, 3)
        dw_full = dw.reshape(3, 3, CI, CO)
        return z_full[None], dx_full[None], dw_full[None]

    return jax.shard_map(device_step, mesh=mesh, in_specs=(act_spec, w_spec, vec_spec, vec_spec, chan_spec), out_specs=(chan_spec, act_spec, w_spec), check_vma=False)
```

```python
import functools

import jax
import jax.numpy as jnp
from jax import lax
from jax.experimental import pallas as pl
from jax.experimental.pallas import tpu as pltpu
from jax.sharding import PartitionSpec as P

MESH = pl.DeviceIdType.MESH
F32 = jnp.float32
BF16 = jnp.bfloat16
PAD = 16
AHEAD = 2
LAG = 2
N_B = 5


def remote(src, dst, send_sem, recv_sem, dev):
    return pltpu.make_async_remote_copy(src_ref=src, dst_ref=dst, send_sem=send_sem, recv_sem=recv_sem, device_id=dev, device_id_type=MESH)


def block_kernel(H, WD, CI, CO, n_chunk, x_ref, w_ref, gam_ref, bet_ref, dz_ref, z_ref, dx_ref, dw_ref,
                 xe, xo, ge, go, wall, dzb, zb, vec, acc, prx, pb, rb, mb, xt, relay, *sems):
    (s_xs, s_xr, s_xf, s_gs, s_gr, s_gl, s_gf, s_wl, s_ws, s_wr, s_vl, s_vs, s_vr, s_dl, s_ds, s_dr,
     s_zs, s_zr, s_ps, s_pr, s_os, s_or, s_ms, s_mr, s_ts, s_tr,
     s_bs, s_br, s_us, s_ur) = sems
    R = WD * 8
    half = CI // 2
    n_a = n_chunk - N_B
    CW = 2 * CO
    zi = lax.axis_index("dp")
    st = lax.axis_index("stage")
    tp = lax.axis_index("tp")
    xi = tp // 2
    c = tp % 2
    y_dev = (zi, 1 - st, tp)
    x_dev = (zi, st, 2 * (1 - xi) + c)
    c_dev = (zi, st, 2 * xi + 1 - c)
    z_mate = jnp.where(zi == 1, 2, 1)
    z_out = jnp.where(zi < 2, 0, 3)
    z_in = jnp.where(zi < 2, 1, 2)
    inner = jnp.logical_or(zi == 1, zi == 2)
    mate_dev = (z_mate, st, tp)
    outer_dev = (z_out, st, tp)
    inner_dev = (z_in, st, tp)

    barrier = pltpu.get_barrier_semaphore()
    for dev in (y_dev, x_dev, c_dev):
        pl.semaphore_signal(barrier, inc=1, device_id=dev, device_id_type=MESH)

    @pl.when(inner)
    def _():
        for dev in (mate_dev, outer_dev):
            pl.semaphore_signal(barrier, inc=1, device_id=dev, device_id_type=MESH)
        pl.semaphore_wait(barrier, 5)

    @pl.when(jnp.logical_not(inner))
    def _():
        pl.semaphore_signal(barrier, inc=1, device_id=inner_dev, device_id_type=MESH)
        pl.semaphore_wait(barrier, 4)

    def zero_borders(buf):
        ch = buf.shape[-1]

        def rows(h, _):
            for s in range(2):
                buf[s, h, 0:PAD, :] = jnp.zeros((PAD, ch), BF16)
                buf[s, h, PAD + R:, :] = jnp.zeros((buf.shape[2] - PAD - R, ch), BF16)
            return 0

        lax.fori_loop(0, H + 2, rows, 0)

    def zero_planes(buf):
        for s in range(2):
            for h in (0, H + 1):
                buf[s, h] = jnp.zeros(buf.shape[2:], BF16)

    def odd_copy(even, odd, s, h):
        n = odd.shape[2]
        odd[s, h] = even[s, h, 8:8 + n, :]

    def tap_rows(even, odd, s, plane, shift, n):
        if shift == 0:
            return even[s, plane, PAD:PAD + n, :]
        start = PAD + 8 * shift - 8
        return odd[s, plane, start:start + n, :]

    def dw_view(k):
        return dw_ref.at[k // 2, pl.ds(pl.multiple_of((k % 2) * half, half), half), :]

    def part_up(k):
        return remote(pb.at[k], pb.at[k], s_os.at[k], s_or.at[k], y_dev)

    def to_mate(k):
        return remote(pb.at[k], mb.at[k], s_ms.at[k], s_mr.at[k], mate_dev)

    def total_down(src, k):
        return remote(src.at[k], dw_view(k), s_ts.at[k], s_tr.at[k], y_dev)

    @pl.when(st == 0)
    def _():
        def x_copy(h):
            return remote(x_ref.at[h], xe.at[xi, h + 1, pl.ds(PAD, R), :], s_xs.at[h], s_xr.at[xi, h], y_dev)

        lax.fori_loop(0, H, lambda h, _: (x_copy(h).start(), 0)[1], 0)
        zero_borders(ge)
        zero_planes(ge)
        zero_planes(go)

        def zero_out(h, _):
            z_ref[h] = jnp.zeros(z_ref.shape[1:], BF16)
            return 0

        lax.fori_loop(0, H, zero_out, 0)

        def zero_dw(t, _):
            dw_ref[t] = jnp.zeros((CI, CO), F32)
            return 0

        lax.fori_loop(0, 9, zero_dw, 0)

        def w_in(t, b):
            return remote(wall.at[b, t], wall.at[b, t], s_ws.at[0, t], s_wr.at[b, t], y_dev)

        def w_fwd(t, b, k, dev):
            return remote(wall.at[b, t], wall.at[b, t], s_ws.at[k, t], s_wr.at[b, t], dev)

        b_x = 2 * (1 - xi) + c

        def w_step(t, _):
            w_in(t, tp).wait_recv()
            w_fwd(t, tp, 0, c_dev).start()
            w_fwd(t, tp, 1, x_dev).start()
            return 0

        lax.fori_loop(0, 9, w_step, 0)

        def w_step2(t, _):
            w_in(t, b_x).wait_recv()
            w_fwd(t, b_x, 2, c_dev).start()
            return 0

        lax.fori_loop(0, 9, w_step2, 0)

        def w_step3(t, _):
            w_in(t, 2 * xi + 1 - c).wait_recv()
            w_in(t, 2 * (1 - xi) + 1 - c).wait_recv()
            return 0

        lax.fori_loop(0, 9, w_step3, 0)

        def g_in(j, b):
            return remote(ge.at[b, j + 1, pl.ds(PAD, R), :], ge.at[b, j + 1, pl.ds(PAD, R), :], s_gf.at[j], s_gr.at[b, j], y_dev)

        def relay_in(j):
            return remote(relay.at[j], relay.at[j], s_gf.at[j], s_gl.at[j], y_dev)

        def relay_out(j):
            return remote(relay.at[j], ge.at[xi, j + 1, pl.ds(PAD, R), :], s_gf.at[j], s_gr.at[xi, j], x_dev)

        def g_relay(j):
            relay_in(j).wait_recv()
            relay_out(j).start()

        lax.fori_loop(0, AHEAD, lambda j, _: (g_relay(j), 0)[1], 0)

        def g_step(j, _):
            @pl.when(j + AHEAD < H)
            def _():
                g_relay(j + AHEAD)

            @pl.when(j < H)
            def _():
                g_in(j, xi).wait_recv()
                g_in(j, 1 - xi).wait_recv()
                for b in range(2):
                    odd_copy(ge, go, b, j + 1)

            @pl.when(j >= 1)
            def _():
                h = j - 1
                tot = jnp.zeros((R, CI), F32)
                for b in range(2):
                    for ky in range(3):
                        for kx in range(3):
                            t = 3 * ky + kx
                            lhs = tap_rows(ge, go, b, h + 2 - ky, 1 - kx, R)
                            rhs = jnp.concatenate([wall[2 * b, t], wall[2 * b + 1, t]], axis=1)
                            tot = tot + lax.dot_general(lhs, rhs, (((1,), (1,)), ((), ())), preferred_element_type=F32)
                dx_ref[h] = tot.astype(BF16)

            return 0

        lax.fori_loop(0, H + 1, g_step, 0)

        def b_to_inner(k, dev):
            return remote(pb.at[k], rb.at[k], s_bs.at[k], s_br.at[k], dev)

        def b_to_outer(k, dev):
            return remote(rb.at[k], mb.at[k], s_us.at[k], s_ur.at[k], dev)

        @pl.when(jnp.logical_not(inner))
        def _():
            def up(k, _):
                part_up(k).wait_recv()
                b_to_inner(k, inner_dev).start()
                return 0

            lax.fori_loop(n_a, n_chunk, up, 0)

            def down(k, _):
                b_to_outer(k, inner_dev).wait_recv()
                total_down(mb, k).start()
                return 0

            lax.fori_loop(n_a, n_chunk, down, 0)

            def done(k, _):
                b_to_inner(k, inner_dev).wait_send()
                total_down(mb, k).wait_send()
                return 0

            lax.fori_loop(n_a, n_chunk, done, 0)

        @pl.when(inner)
        def _():
            def both(k, _):
                @pl.when(k < n_chunk)
                def _():
                    part_up(k).wait_recv()
                    b_to_inner(k, outer_dev).wait_recv()
                    pb[k] = pb[k] + rb[k]
                    to_mate(k).start()

                @pl.when(k >= n_a + LAG)
                def _():
                    m = k - LAG
                    to_mate(m).wait_recv()
                    rb[m] = pb[m] + mb[m]
                    b_to_outer(m, outer_dev).start()
                    total_down(rb, m).start()

                return 0

            lax.fori_loop(n_a, n_chunk + LAG, both, 0)

            def done(k, _):
                to_mate(k).wait_send()
                b_to_outer(k, outer_dev).wait_send()
                total_down(rb, k).wait_send()
                return 0

            lax.fori_loop(n_a, n_chunk, done, 0)

        def drain(h, _):
            x_copy(h).wait_send()
            relay_out(h).wait_send()
            return 0

        lax.fori_loop(0, H, drain, 0)

        def drain_w(t, _):
            w_fwd(t, tp, 0, c_dev).wait_send()
            w_fwd(t, tp, 1, x_dev).wait_send()
            w_fwd(t, b_x, 2, c_dev).wait_send()
            return 0

        lax.fori_loop(0, 9, drain_w, 0)

    @pl.when(st == 1)
    def _():
        w_loc = pltpu.make_async_copy(w_ref, wall.at[c], s_wl)
        w_core = remote(w_ref, wall.at[c], s_vs.at[2], s_vr.at[2], c_dev)
        vecs_l = [pltpu.make_async_copy(r, vec.at[k, c], s_vl.at[k]) for k, r in enumerate((gam_ref, bet_ref))]
        vecs_r = [remote(r, vec.at[k, c], s_vs.at[k], s_vr.at[k], c_dev) for k, r in enumerate((gam_ref, bet_ref))]
        dz_l = [pltpu.make_async_copy(dz_ref.at[:, :, 2 * s + c], dzb.at[s, c], s_dl.at[s]) for s in range(2)]
        dz_r = [remote(dz_ref.at[:, :, 2 * s + 1 - c], dzb.at[s, c], s_ds.at[s], s_dr.at[s], c_dev) for s in range(2)]

        def w_y(t):
            return remote(w_ref.at[t], wall.at[tp, t], s_ws.at[0, t], s_wr.at[tp, t], y_dev)

        w_loc.start()
        w_core.start()
        for k in range(2):
            vecs_l[k].start()
            vecs_r[k].start()
            dz_l[k].start()
            dz_r[k].start()
        lax.fori_loop(0, 9, lambda t, _: (w_y(t).start(), 0)[1], 0)

        zero_borders(xe)
        zero_borders(ge)
        for buf in (xe, xo, ge, go):
            zero_planes(buf)

        def zero_acc(t, _):
            for k in range(2):
                acc[k, t] = jnp.zeros((CI, CO), F32)
            return 0

        lax.fori_loop(0, 9, zero_acc, 0)

        def zero_dx(h, _):
            dx_ref[h] = jnp.zeros((R, CI), BF16)
            return 0

        lax.fori_loop(0, H, zero_dx, 0)
        for k in range(2):
            vecs_l[k].wait()
            vecs_r[k].wait_recv()
            dz_l[k].wait()
            dz_r[k].wait_recv()
        w_loc.wait()
        w_core.wait_recv()

        def x_in(j, s):
            view = xe.at[s, j + 1, pl.ds(PAD, R), :]
            return remote(view, view, s_xf.at[j], s_xr.at[s, j], y_dev)

        def x_fwd(j):
            view = xe.at[xi, j + 1, pl.ds(PAD, R), :]
            return remote(view, view, s_xf.at[j], s_xr.at[xi, j], x_dev)

        def g_own(h):
            return remote(ge.at[xi, h + 1, pl.ds(PAD, R), :], ge.at[xi, h + 1, pl.ds(PAD, R), :], s_gs.at[0, h], s_gr.at[xi, h], y_dev)

        def g_other(h):
            return remote(ge.at[1 - xi, h + 1, pl.ds(PAD, R), :], relay.at[h], s_gs.at[1, h], s_gl.at[h], y_dev)

        def x_relay(j):
            x_in(j, xi).wait_recv()
            x_fwd(j).start()

        lax.fori_loop(0, AHEAD, lambda j, _: (x_relay(j), 0)[1], 0)

        def step(j, _):
            @pl.when(j + AHEAD < H)
            def _():
                x_relay(j + AHEAD)

            @pl.when(j < H)
            def _():
                x_in(j, 1 - xi).wait_recv()
                for s in range(2):
                    odd_copy(xe, xo, s, j + 1)

            @pl.when(jnp.logical_and(j >= 1, j < H + 1))
            def _():
                h = j - 1
                pre = jnp.zeros((2 * R, CW), F32)
                for ky in range(3):
                    for kx in range(3):
                        t = 3 * ky + kx
                        lhs = jnp.concatenate([tap_rows(xe, xo, s, h + ky, kx - 1, R) for s in range(2)], axis=0)
                        rhs = jnp.concatenate([wall[0, t], wall[1, t]], axis=1)
                        pre = pre + jnp.dot(lhs, rhs, preferred_element_type=F32)
                for k in range(2):
                    gam = vec[0, k]
                    bet = vec[1, k]
                    for s in range(2):
                        y = pre[s * R:(s + 1) * R, k * CO:(k + 1) * CO] * gam + bet
                        zb[s, k, h] = jnp.maximum(y, 0.0).reshape(WD, 8, CO).astype(BF16)
                        dzr = dzb[s, k, h].astype(F32).reshape(R, CO)
                        ge[s, h + 1, PAD:PAD + R, k * CO:(k + 1) * CO] = jnp.where(y > 0, dzr * gam, 0.0).astype(BF16)
                g_own(h).start()
                g_other(h).start()
                for s in range(2):
                    odd_copy(ge, go, s, h + 1)
                    z_ref[h, :, 2 * s + c] = zb[s, c, h]

            @pl.when(j >= 2)
            def _():
                q = j - 2
                rows = jnp.concatenate([xe[s, q + 1, PAD:PAD + 128, :] for s in range(2)], axis=0)
                xt[...] = rows.T
                for ky in range(3):
                    for kx in range(3):
                        t = 3 * ky + kx
                        rhs = jnp.concatenate([tap_rows(ge, go, s, q + 2 - ky, 1 - kx, 128) for s in range(2)], axis=0)
                        part = jnp.dot(xt[...], rhs, preferred_element_type=F32)
                        for k in range(2):
                            acc[k, t] += part[:, k * CO:(k + 1) * CO]

            return 0

        lax.fori_loop(0, H + 2, step, 0)

        def pair(t):
            return remote(acc.at[1 - c, t], prx.at[t], s_ps.at[t], s_pr.at[t], c_dev)

        lax.fori_loop(0, 9, lambda i, _: (pair((i + n_a // 2) % 9).start(), 0)[1], 0)
        z_r = [remote(zb.at[s, 1 - c], z_ref.at[:, :, 2 * s + c], s_zs.at[s], s_zr.at[s], c_dev) for s in range(2)]
        z_w = [remote(zb.at[s, 1 - c], z_ref.at[:, :, 2 * s + 1 - c], s_zs.at[s], s_zr.at[s], c_dev) for s in range(2)]
        for s in range(2):
            z_r[s].start()

        def own_part(k, fresh):
            t = k // 2
            q = pl.multiple_of((k % 2) * half, half)

            @pl.when(fresh)
            def _():
                pair(t).wait_recv()

            return acc[c, t, pl.ds(q, half), :] + prx[t, pl.ds(q, half), :]

        def part_a(k):
            return own_part(k, jnp.logical_and(k % 2 == 0, k // 2 < n_a // 2))

        def send_b(k, _):
            pb[k] = own_part(k, jnp.logical_or(k % 2 == 0, k == n_a))
            part_up(k).start()
            return 0

        lax.fori_loop(n_a, n_chunk, send_b, 0)

        def to_inner(k):
            return remote(pb.at[k], rb.at[k], s_os.at[k], s_or.at[k], inner_dev)

        def from_outer(k):
            return remote(pb.at[k], rb.at[k], s_os.at[k], s_or.at[k], outer_dev)

        def to_outer(k):
            return remote(dw_view(k), dw_view(k), s_ts.at[k], s_tr.at[k], outer_dev)

        def from_inner(k):
            return remote(dw_view(k), dw_view(k), s_ts.at[k], s_tr.at[k], inner_dev)

        @pl.when(jnp.logical_not(inner))
        def _():
            def send(k, _):
                pb[k] = part_a(k)
                to_inner(k).start()
                return 0

            lax.fori_loop(0, n_a, send, 0)

            def take(k, _):
                from_inner(k).wait_recv()
                to_inner(k).wait_send()
                return 0

            lax.fori_loop(0, n_a, take, 0)

        @pl.when(inner)
        def _():
            def both(k, _):
                @pl.when(k < n_a)
                def _():
                    part = part_a(k)
                    from_outer(k).wait_recv()
                    pb[k] = part + rb[k]
                    to_mate(k).start()

                @pl.when(k >= LAG)
                def _():
                    m = k - LAG
                    to_mate(m).wait_recv()
                    dw_ref[m // 2, pl.ds(pl.multiple_of((m % 2) * half, half), half), :] = pb[m] + mb[m]
                    to_outer(m).start()

                return 0

            lax.fori_loop(0, n_a + LAG, both, 0)

            def done(k, _):
                to_mate(k).wait_send()
                to_outer(k).wait_send()
                return 0

            lax.fori_loop(0, n_a, done, 0)

        def done_b(k, _):
            total_down(rb, k).wait_recv()
            part_up(k).wait_send()
            return 0

        lax.fori_loop(n_a, n_chunk, done_b, 0)

        def drain(h, _):
            x_fwd(h).wait_send()
            g_own(h).wait_send()
            g_other(h).wait_send()
            return 0

        lax.fori_loop(0, H, drain, 0)

        def drain_w(t, _):
            w_y(t).wait_send()
            pair(t).wait_send()
            return 0

        lax.fori_loop(0, 9, drain_w, 0)
        w_core.wait_send()
        for k in range(2):
            vecs_r[k].wait_send()
            dz_r[k].wait_send()
            z_r[k].wait_send()
            z_w[k].wait_recv()


def out_kernel(*refs):
    srcs, dsts, sem = refs[:3], refs[3:6], refs[6]
    copies = [pltpu.make_async_copy(a, b, sem.at[i]) for i, (a, b) in enumerate(zip(srcs, dsts))]
    for cp in copies:
        cp.start()
    for cp in copies:
        cp.wait()


def write_out(*arrays):
    return pl.pallas_call(
        out_kernel,
        out_shape=tuple(jax.ShapeDtypeStruct(a.shape, a.dtype) for a in arrays),
        in_specs=[pl.BlockSpec(memory_space=pltpu.VMEM)] * 3,
        out_specs=(pl.BlockSpec(memory_space=pl.ANY),) * 3,
        scratch_shapes=[pltpu.SemaphoreType.DMA((3,))],
        compiler_params=pltpu.CompilerParams(vmem_limit_bytes=16 * 1024 * 1024),
    )(*arrays)


def solution(mesh):
    act_spec = P('stage', ('dp', 'tp'))
    w_spec = P('stage', None, None, None, 'tp')
    vec_spec = P('stage', 'tp')
    chan_spec = P('stage', 'dp', None, None, 'tp')

    def device_step(act_in, w_conv, gamma_vec, beta_vec, z_grad):
        N, H, WD, CI = act_in.shape[1:]
        CO = w_conv.shape[-1]
        R = WD * N
        RP = 128 + 2 * PAD
        n_chunk = 18
        x = act_in[0].transpose(1, 2, 0, 3).reshape(H, R, CI)
        w = w_conv[0].reshape(9, CI, CO)
        dz = z_grad[0].transpose(1, 2, 0, 3).reshape(H, WD, 4, N, CO)
        dma = pltpu.SemaphoreType.DMA
        z, dx, dw = pl.pallas_call(
            functools.partial(block_kernel, H, WD, CI, CO, n_chunk),
            out_shape=(
                jax.ShapeDtypeStruct((H, WD, 4, N, CO), BF16),
                jax.ShapeDtypeStruct((H, R, CI), BF16),
                jax.ShapeDtypeStruct((9, CI, CO), F32),
            ),
            in_specs=[pl.BlockSpec(memory_space=pltpu.HBM)] * 5,
            out_specs=(pl.BlockSpec(memory_space=pltpu.VMEM),) * 3,
            scratch_shapes=[
                pltpu.VMEM((2, H + 2, RP, CI), BF16),
                pltpu.VMEM((2, H + 2, RP - 16, CI), BF16),
                pltpu.VMEM((2, H + 2, RP, 2 * CO), BF16),
                pltpu.VMEM((2, H + 2, RP - 16, 2 * CO), BF16),
                pltpu.VMEM((4, 9, CI, CO), BF16),
                pltpu.VMEM((2, 2, H, WD, N, CO), BF16),
                pltpu.VMEM((2, 2, H, WD, N, CO), BF16),
                pltpu.VMEM((2, 2, 1, CO), F32),
                pltpu.VMEM((2, 9, CI, CO), F32),
                pltpu.VMEM((9, CI, CO), F32),
                pltpu.VMEM((n_chunk, CI // 2, CO), F32),
                pltpu.VMEM((n_chunk, CI // 2, CO), F32),
                pltpu.VMEM((n_chunk, CI // 2, CO), F32),
                pltpu.VMEM((CI, 256), BF16),
                pltpu.VMEM((H, R, 2 * CO), BF16),
                dma((H,)), dma((2, H)), dma((H,)), dma((2, H)), dma((2, H)), dma((H,)), dma((H,)),
                dma, dma((3, 9)), dma((4, 9)), dma((2,)), dma((3,)), dma((3,)), dma((2,)), dma((2,)), dma((2,)),
                dma((2,)), dma((2,)), dma((9,)), dma((9,)),
                *[dma((n_chunk,))] * 10,
            ],
            compiler_params=pltpu.CompilerParams(collective_id=0, has_side_effects=True, vmem_limit_bytes=46 * 1024 * 1024),
        )(*[pltpu.with_memory_space_constraint(a, pltpu.HBM) for a in (x, w, gamma_vec, beta_vec, dz)])
        z, dx, dw = write_out(z, dx, dw)
        z_full = z.reshape(H, WD, 4 * N, CO).transpose(2, 0, 1, 3)
        dx_full = dx.reshape(H, WD, N, CI).transpose(2, 0, 1, 3)
        dw_full = dw.reshape(3, 3, CI, CO)
        return z_full[None], dx_full[None], dw_full[None]

    return jax.shard_map(device_step, mesh=mesh, in_specs=(act_spec, w_spec, vec_spec, vec_spec, chan_spec), out_specs=(chan_spec, act_spec, w_spec), check_vma=False)
```

```python
import functools

import jax
import jax.numpy as jnp
from jax import lax
from jax.experimental import pallas as pl
from jax.experimental.pallas import tpu as pltpu
from jax.sharding import PartitionSpec as P

MESH = pl.DeviceIdType.MESH
F32 = jnp.float32
BF16 = jnp.bfloat16
PAD = 16
AHEAD = 2
LAG = 2
N_B = 8


def remote(src, dst, send_sem, recv_sem, dev):
    return pltpu.make_async_remote_copy(src_ref=src, dst_ref=dst, send_sem=send_sem, recv_sem=recv_sem, device_id=dev, device_id_type=MESH)


def block_kernel(H, WD, CI, CO, n_chunk, x_ref, w_ref, gam_ref, bet_ref, dz_ref, z_ref, dx_ref, dw_ref,
                 xe, xo, ge, go, wall, dzb, zb, vec, acc, prx, pb, rb, mb, xt, relay, *sems):
    (s_xs, s_xr, s_xf, s_gs, s_gr, s_gl, s_gf, s_wl, s_ws, s_wr, s_vl, s_vs, s_vr, s_dl, s_ds, s_dr,
     s_zs, s_zr, s_ps, s_pr, s_os, s_or, s_ms, s_mr, s_ts, s_tr,
     s_bs, s_br, s_us, s_ur) = sems
    R = WD * 8
    half = CI // 2
    quarter = CI // 4
    n_a = n_chunk - N_B
    CW = 2 * CO
    zi = lax.axis_index("dp")
    st = lax.axis_index("stage")
    tp = lax.axis_index("tp")
    xi = tp // 2
    c = tp % 2
    y_dev = (zi, 1 - st, tp)
    x_dev = (zi, st, 2 * (1 - xi) + c)
    c_dev = (zi, st, 2 * xi + 1 - c)
    z_mate = jnp.where(zi == 1, 2, 1)
    z_out = jnp.where(zi < 2, 0, 3)
    z_in = jnp.where(zi < 2, 1, 2)
    inner = jnp.logical_or(zi == 1, zi == 2)
    mate_dev = (z_mate, st, tp)
    outer_dev = (z_out, st, tp)
    inner_dev = (z_in, st, tp)

    barrier = pltpu.get_barrier_semaphore()
    for dev in (y_dev, x_dev, c_dev):
        pl.semaphore_signal(barrier, inc=1, device_id=dev, device_id_type=MESH)

    @pl.when(inner)
    def _():
        for dev in (mate_dev, outer_dev):
            pl.semaphore_signal(barrier, inc=1, device_id=dev, device_id_type=MESH)
        pl.semaphore_wait(barrier, 5)

    @pl.when(jnp.logical_not(inner))
    def _():
        pl.semaphore_signal(barrier, inc=1, device_id=inner_dev, device_id_type=MESH)
        pl.semaphore_wait(barrier, 4)

    def zero_borders(buf):
        ch = buf.shape[-1]

        def rows(h, _):
            for s in range(2):
                buf[s, h, 0:PAD, :] = jnp.zeros((PAD, ch), BF16)
                buf[s, h, PAD + R:, :] = jnp.zeros((buf.shape[2] - PAD - R, ch), BF16)
            return 0

        lax.fori_loop(0, H + 2, rows, 0)

    def zero_planes(buf):
        for s in range(2):
            for h in (0, H + 1):
                buf[s, h] = jnp.zeros(buf.shape[2:], BF16)

    def odd_copy(even, odd, s, h):
        n = odd.shape[2]
        odd[s, h] = even[s, h, 8:8 + n, :]

    def tap_rows(even, odd, s, plane, shift, n):
        if shift == 0:
            return even[s, plane, PAD:PAD + n, :]
        start = PAD + 8 * shift - 8
        return odd[s, plane, start:start + n, :]

    def dw_view(k):
        return dw_ref.at[k // 2, pl.ds(pl.multiple_of((k % 2) * half, half), half), :]

    def part_up(k):
        return remote(pb.at[k], pb.at[k], s_os.at[k], s_or.at[k], y_dev)

    def to_mate(k):
        return remote(pb.at[k], mb.at[k], s_ms.at[k], s_mr.at[k], mate_dev)

    def total_down(src, k):
        return remote(src.at[k], dw_view(k), s_ts.at[k], s_tr.at[k], y_dev)

    @pl.when(st == 0)
    def _():
        def x_copy(h):
            return remote(x_ref.at[h], xe.at[xi, h + 1, pl.ds(PAD, R), :], s_xs.at[h], s_xr.at[xi, h], y_dev)

        lax.fori_loop(0, H, lambda h, _: (x_copy(h).start(), 0)[1], 0)
        zero_borders(ge)
        zero_planes(ge)
        zero_planes(go)

        def zero_out(h, _):
            z_ref[h] = jnp.zeros(z_ref.shape[1:], BF16)
            return 0

        lax.fori_loop(0, H, zero_out, 0)

        def zero_dw(t, _):
            dw_ref[t] = jnp.zeros((CI, CO), F32)
            return 0

        lax.fori_loop(0, 9, zero_dw, 0)

        def g_in(j, b):
            return remote(ge.at[b, j + 1, pl.ds(PAD, R), :], ge.at[b, j + 1, pl.ds(PAD, R), :], s_gf.at[j], s_gr.at[b, j], y_dev)

        def relay_in(j):
            return remote(relay.at[j], relay.at[j], s_gf.at[j], s_gl.at[j], y_dev)

        def relay_out(j):
            return remote(relay.at[j], ge.at[xi, j + 1, pl.ds(PAD, R), :], s_gf.at[j], s_gr.at[xi, j], x_dev)

        def g_relay(j):
            relay_in(j).wait_recv()
            relay_out(j).start()

        def relay_rows(lo, hi):
            lax.fori_loop(lo, min(hi, H), lambda j, _: (g_relay(j), 0)[1], 0)

        tp_x = 2 * (1 - xi) + c
        left_dev = (jnp.maximum(zi - 1, 0), st, tp)
        right_dev = (jnp.minimum(zi + 1, 3), st, tp)

        def w_unit(b, q, send_sem, dev):
            view = wall.at[b, :, pl.ds(pl.multiple_of(q * quarter, quarter), quarter), :]
            return remote(view, view, send_sem, s_wr.at[b, q], dev)

        def w_got(q, go_right, go_left):
            w_unit(tp, q, s_ws.at[0, q], y_dev).wait_recv()
            if go_right:
                @pl.when(zi < 3)
                def _():
                    w_unit(tp, q, s_ws.at[2, q], right_dev).start()
            if go_left:
                @pl.when(zi > 0)
                def _():
                    w_unit(tp, q, s_ws.at[3, q], left_dev).start()
            w_unit(tp, q, s_ws.at[0, q], x_dev).start()
            w_unit(tp, q, s_ws.at[1, q], c_dev).start()

        w_got(zi, True, True)
        for d in range(1, 4):
            @pl.when(zi - d >= 0)
            def _():
                w_got(zi - d, True, False)

            @pl.when(zi + d <= 3)
            def _():
                w_got(zi + d, False, True)

            relay_rows(3 * (d - 1), 3 * d)

        def w_cross(q, _):
            w_unit(tp_x, q, s_ws.at[4, q], x_dev).wait_recv()
            w_unit(tp_x, q, s_ws.at[4, q], c_dev).start()
            return 0

        lax.fori_loop(0, 4, w_cross, 0)

        def w_all(q, _):
            for b in (2 * xi + 1 - c, 2 * (1 - xi) + 1 - c):
                w_unit(b, q, s_ws.at[1, q], c_dev).wait_recv()
            return 0

        lax.fori_loop(0, 4, w_all, 0)
        relay_rows(9, 9 + AHEAD)

        def g_step(j, _):
            @pl.when(jnp.logical_and(j + AHEAD >= min(9 + AHEAD, H), j + AHEAD < H))
            def _():
                g_relay(j + AHEAD)

            @pl.when(j < H)
            def _():
                g_in(j, xi).wait_recv()
                g_in(j, 1 - xi).wait_recv()
                for b in range(2):
                    odd_copy(ge, go, b, j + 1)

            @pl.when(j >= 1)
            def _():
                h = j - 1
                tot = jnp.zeros((R, CI), F32)
                for b in range(2):
                    for ky in range(3):
                        for kx in range(3):
                            t = 3 * ky + kx
                            lhs = tap_rows(ge, go, b, h + 2 - ky, 1 - kx, R)
                            rhs = jnp.concatenate([wall[2 * b, t], wall[2 * b + 1, t]], axis=1)
                            tot = tot + lax.dot_general(lhs, rhs, (((1,), (1,)), ((), ())), preferred_element_type=F32)
                dx_ref[h] = tot.astype(BF16)

            return 0

        lax.fori_loop(0, H + 1, g_step, 0)

        def b_to_inner(k, dev):
            return remote(pb.at[k], rb.at[k], s_bs.at[k], s_br.at[k], dev)

        def b_to_outer(k, dev):
            return remote(rb.at[k], mb.at[k], s_us.at[k], s_ur.at[k], dev)

        @pl.when(jnp.logical_not(inner))
        def _():
            def up(k, _):
                part_up(k).wait_recv()
                b_to_inner(k, inner_dev).start()
                return 0

            lax.fori_loop(n_a, n_chunk, up, 0)

            def down(k, _):
                b_to_outer(k, inner_dev).wait_recv()
                total_down(mb, k).start()
                return 0

            lax.fori_loop(n_a, n_chunk, down, 0)

            def done(k, _):
                b_to_inner(k, inner_dev).wait_send()
                total_down(mb, k).wait_send()
                return 0

            lax.fori_loop(n_a, n_chunk, done, 0)

        @pl.when(inner)
        def _():
            def both(k, _):
                @pl.when(k < n_chunk)
                def _():
                    part_up(k).wait_recv()
                    b_to_inner(k, outer_dev).wait_recv()
                    pb[k] = pb[k] + rb[k]
                    to_mate(k).start()

                @pl.when(k >= n_a + LAG)
                def _():
                    m = k - LAG
                    to_mate(m).wait_recv()
                    rb[m] = pb[m] + mb[m]
                    b_to_outer(m, outer_dev).start()
                    total_down(rb, m).start()

                return 0

            lax.fori_loop(n_a, n_chunk + LAG, both, 0)

            def done(k, _):
                to_mate(k).wait_send()
                b_to_outer(k, outer_dev).wait_send()
                total_down(rb, k).wait_send()
                return 0

            lax.fori_loop(n_a, n_chunk, done, 0)

        def drain(h, _):
            x_copy(h).wait_send()
            relay_out(h).wait_send()
            return 0

        lax.fori_loop(0, H, drain, 0)

        def drain_w(q, _):
            w_unit(tp, q, s_ws.at[0, q], x_dev).wait_send()
            w_unit(tp, q, s_ws.at[1, q], c_dev).wait_send()
            w_unit(tp_x, q, s_ws.at[4, q], c_dev).wait_send()

            @pl.when(jnp.logical_and(zi < 3, q <= zi))
            def _():
                w_unit(tp, q, s_ws.at[2, q], right_dev).wait_send()

            @pl.when(jnp.logical_and(zi > 0, q >= zi))
            def _():
                w_unit(tp, q, s_ws.at[3, q], left_dev).wait_send()

            return 0

        lax.fori_loop(0, 4, drain_w, 0)

    @pl.when(st == 1)
    def _():
        w_loc = pltpu.make_async_copy(w_ref, wall.at[c], s_wl)
        w_core = remote(w_ref, wall.at[c], s_vs.at[2], s_vr.at[2], c_dev)
        vecs_l = [pltpu.make_async_copy(r, vec.at[k, c], s_vl.at[k]) for k, r in enumerate((gam_ref, bet_ref))]
        vecs_r = [remote(r, vec.at[k, c], s_vs.at[k], s_vr.at[k], c_dev) for k, r in enumerate((gam_ref, bet_ref))]
        dz_l = [pltpu.make_async_copy(dz_ref.at[:, :, 2 * s + c], dzb.at[s, c], s_dl.at[s]) for s in range(2)]
        dz_r = [remote(dz_ref.at[:, :, 2 * s + 1 - c], dzb.at[s, c], s_ds.at[s], s_dr.at[s], c_dev) for s in range(2)]

        part = pl.ds(pl.multiple_of(zi * quarter, quarter), quarter)
        w_y = remote(w_ref.at[:, part, :], wall.at[tp, :, part, :], s_ws.at[0, zi], s_wr.at[tp, zi], y_dev)

        w_y.start()
        w_loc.start()
        w_core.start()
        for k in range(2):
            vecs_l[k].start()
            vecs_r[k].start()
            dz_l[k].start()
            dz_r[k].start()

        zero_borders(xe)
        zero_borders(ge)
        for buf in (xe, xo, ge, go):
            zero_planes(buf)

        def zero_acc(t, _):
            for k in range(2):
                acc[k, t] = jnp.zeros((CI, CO), F32)
            return 0

        lax.fori_loop(0, 9, zero_acc, 0)

        def zero_dx(h, _):
            dx_ref[h] = jnp.zeros((R, CI), BF16)
            return 0

        lax.fori_loop(0, H, zero_dx, 0)
        for k in range(2):
            vecs_l[k].wait()
            vecs_r[k].wait_recv()
            dz_l[k].wait()
            dz_r[k].wait_recv()
        w_loc.wait()
        w_core.wait_recv()

        def x_in(j, s):
            view = xe.at[s, j + 1, pl.ds(PAD, R), :]
            return remote(view, view, s_xf.at[j], s_xr.at[s, j], y_dev)

        def x_fwd(j):
            view = xe.at[xi, j + 1, pl.ds(PAD, R), :]
            return remote(view, view, s_xf.at[j], s_xr.at[xi, j], x_dev)

        def g_own(h):
            return remote(ge.at[xi, h + 1, pl.ds(PAD, R), :], ge.at[xi, h + 1, pl.ds(PAD, R), :], s_gs.at[0, h], s_gr.at[xi, h], y_dev)

        def g_other(h):
            return remote(ge.at[1 - xi, h + 1, pl.ds(PAD, R), :], relay.at[h], s_gs.at[1, h], s_gl.at[h], y_dev)

        def x_relay(j):
            x_in(j, xi).wait_recv()
            x_fwd(j).start()

        lax.fori_loop(0, AHEAD, lambda j, _: (x_relay(j), 0)[1], 0)

        def step(j, _):
            @pl.when(j + AHEAD < H)
            def _():
                x_relay(j + AHEAD)

            @pl.when(j < H)
            def _():
                x_in(j, 1 - xi).wait_recv()
                for s in range(2):
                    odd_copy(xe, xo, s, j + 1)

            @pl.when(jnp.logical_and(j >= 1, j < H + 1))
            def _():
                h = j - 1
                pre = jnp.zeros((2 * R, CW), F32)
                for ky in range(3):
                    for kx in range(3):
                        t = 3 * ky + kx
                        lhs = jnp.concatenate([tap_rows(xe, xo, s, h + ky, kx - 1, R) for s in range(2)], axis=0)
                        rhs = jnp.concatenate([wall[0, t], wall[1, t]], axis=1)
                        pre = pre + jnp.dot(lhs, rhs, preferred_element_type=F32)
                for k in range(2):
                    gam = vec[0, k]
                    bet = vec[1, k]
                    for s in range(2):
                        y = pre[s * R:(s + 1) * R, k * CO:(k + 1) * CO] * gam + bet
                        zb[s, k, h] = jnp.maximum(y, 0.0).reshape(WD, 8, CO).astype(BF16)
                        dzr = dzb[s, k, h].astype(F32).reshape(R, CO)
                        ge[s, h + 1, PAD:PAD + R, k * CO:(k + 1) * CO] = jnp.where(y > 0, dzr * gam, 0.0).astype(BF16)
                g_own(h).start()
                g_other(h).start()
                for s in range(2):
                    odd_copy(ge, go, s, h + 1)
                    z_ref[h, :, 2 * s + c] = zb[s, c, h]

            @pl.when(j >= 2)
            def _():
                q = j - 2
                rows = jnp.concatenate([xe[s, q + 1, PAD:PAD + 128, :] for s in range(2)], axis=0)
                xt[...] = rows.T
                for ky in range(3):
                    for kx in range(3):
                        t = 3 * ky + kx
                        rhs = jnp.concatenate([tap_rows(ge, go, s, q + 2 - ky, 1 - kx, 128) for s in range(2)], axis=0)
                        part = jnp.dot(xt[...], rhs, preferred_element_type=F32)
                        for k in range(2):
                            acc[k, t] += part[:, k * CO:(k + 1) * CO]

            return 0

        lax.fori_loop(0, H + 2, step, 0)

        def pair(t):
            return remote(acc.at[1 - c, t], prx.at[t], s_ps.at[t], s_pr.at[t], c_dev)

        lax.fori_loop(0, 9, lambda i, _: (pair((i + n_a // 2) % 9).start(), 0)[1], 0)
        z_r = [remote(zb.at[s, 1 - c], z_ref.at[:, :, 2 * s + c], s_zs.at[s], s_zr.at[s], c_dev) for s in range(2)]
        z_w = [remote(zb.at[s, 1 - c], z_ref.at[:, :, 2 * s + 1 - c], s_zs.at[s], s_zr.at[s], c_dev) for s in range(2)]
        for s in range(2):
            z_r[s].start()

        def own_part(k, fresh):
            t = k // 2
            q = pl.multiple_of((k % 2) * half, half)

            @pl.when(fresh)
            def _():
                pair(t).wait_recv()

            return acc[c, t, pl.ds(q, half), :] + prx[t, pl.ds(q, half), :]

        def part_a(k):
            return own_part(k, jnp.logical_and(k % 2 == 0, k // 2 < n_a // 2))

        def send_b(k, _):
            pb[k] = own_part(k, jnp.logical_or(k % 2 == 0, k == n_a))
            part_up(k).start()
            return 0

        lax.fori_loop(n_a, n_chunk, send_b, 0)

        def to_inner(k):
            return remote(pb.at[k], rb.at[k], s_os.at[k], s_or.at[k], inner_dev)

        def from_outer(k):
            return remote(pb.at[k], rb.at[k], s_os.at[k], s_or.at[k], outer_dev)

        def to_outer(k):
            return remote(dw_view(k), dw_view(k), s_ts.at[k], s_tr.at[k], outer_dev)

        def from_inner(k):
            return remote(dw_view(k), dw_view(k), s_ts.at[k], s_tr.at[k], inner_dev)

        @pl.when(jnp.logical_not(inner))
        def _():
            def send(k, _):
                pb[k] = part_a(k)
                to_inner(k).start()
                return 0

            lax.fori_loop(0, n_a, send, 0)

            def take(k, _):
                from_inner(k).wait_recv()
                to_inner(k).wait_send()
                return 0

            lax.fori_loop(0, n_a, take, 0)

        @pl.when(inner)
        def _():
            def both(k, _):
                @pl.when(k < n_a)
                def _():
                    part = part_a(k)
                    from_outer(k).wait_recv()
                    pb[k] = part + rb[k]
                    to_mate(k).start()

                @pl.when(k >= LAG)
                def _():
                    m = k - LAG
                    to_mate(m).wait_recv()
                    dw_ref[m // 2, pl.ds(pl.multiple_of((m % 2) * half, half), half), :] = pb[m] + mb[m]
                    to_outer(m).start()

                return 0

            lax.fori_loop(0, n_a + LAG, both, 0)

            def done(k, _):
                to_mate(k).wait_send()
                to_outer(k).wait_send()
                return 0

            lax.fori_loop(0, n_a, done, 0)

        def done_b(k, _):
            total_down(rb, k).wait_recv()
            part_up(k).wait_send()
            return 0

        lax.fori_loop(n_a, n_chunk, done_b, 0)

        def drain(h, _):
            x_fwd(h).wait_send()
            g_own(h).wait_send()
            g_other(h).wait_send()
            return 0

        lax.fori_loop(0, H, drain, 0)

        def drain_w(t, _):
            pair(t).wait_send()
            return 0

        lax.fori_loop(0, 9, drain_w, 0)
        w_core.wait_send()
        w_y.wait_send()
        for k in range(2):
            vecs_r[k].wait_send()
            dz_r[k].wait_send()
            z_r[k].wait_send()
            z_w[k].wait_recv()


def out_kernel(*refs):
    srcs, dsts, sem = refs[:3], refs[3:6], refs[6]
    copies = [pltpu.make_async_copy(a, b, sem.at[i]) for i, (a, b) in enumerate(zip(srcs, dsts))]
    for cp in copies:
        cp.start()
    for cp in copies:
        cp.wait()


def write_out(*arrays):
    return pl.pallas_call(
        out_kernel,
        out_shape=tuple(jax.ShapeDtypeStruct(a.shape, a.dtype) for a in arrays),
        in_specs=[pl.BlockSpec(memory_space=pltpu.VMEM)] * 3,
        out_specs=(pl.BlockSpec(memory_space=pl.ANY),) * 3,
        scratch_shapes=[pltpu.SemaphoreType.DMA((3,))],
        compiler_params=pltpu.CompilerParams(vmem_limit_bytes=16 * 1024 * 1024),
    )(*arrays)


def solution(mesh):
    act_spec = P('stage', ('dp', 'tp'))
    w_spec = P('stage', None, None, None, 'tp')
    vec_spec = P('stage', 'tp')
    chan_spec = P('stage', 'dp', None, None, 'tp')

    def device_step(act_in, w_conv, gamma_vec, beta_vec, z_grad):
        N, H, WD, CI = act_in.shape[1:]
        CO = w_conv.shape[-1]
        R = WD * N
        RP = 128 + 2 * PAD
        n_chunk = 18
        x = act_in[0].transpose(1, 2, 0, 3).reshape(H, R, CI)
        w = w_conv[0].reshape(9, CI, CO)
        dz = z_grad[0].transpose(1, 2, 0, 3).reshape(H, WD, 4, N, CO)
        dma = pltpu.SemaphoreType.DMA
        z, dx, dw = pl.pallas_call(
            functools.partial(block_kernel, H, WD, CI, CO, n_chunk),
            out_shape=(
                jax.ShapeDtypeStruct((H, WD, 4, N, CO), BF16),
                jax.ShapeDtypeStruct((H, R, CI), BF16),
                jax.ShapeDtypeStruct((9, CI, CO), F32),
            ),
            in_specs=[pl.BlockSpec(memory_space=pltpu.HBM)] * 5,
            out_specs=(pl.BlockSpec(memory_space=pltpu.VMEM),) * 3,
            scratch_shapes=[
                pltpu.VMEM((2, H + 2, RP, CI), BF16),
                pltpu.VMEM((2, H + 2, RP - 16, CI), BF16),
                pltpu.VMEM((2, H + 2, RP, 2 * CO), BF16),
                pltpu.VMEM((2, H + 2, RP - 16, 2 * CO), BF16),
                pltpu.VMEM((4, 9, CI, CO), BF16),
                pltpu.VMEM((2, 2, H, WD, N, CO), BF16),
                pltpu.VMEM((2, 2, H, WD, N, CO), BF16),
                pltpu.VMEM((2, 2, 1, CO), F32),
                pltpu.VMEM((2, 9, CI, CO), F32),
                pltpu.VMEM((9, CI, CO), F32),
                pltpu.VMEM((n_chunk, CI // 2, CO), F32),
                pltpu.VMEM((n_chunk, CI // 2, CO), F32),
                pltpu.VMEM((n_chunk, CI // 2, CO), F32),
                pltpu.VMEM((CI, 256), BF16),
                pltpu.VMEM((H, R, 2 * CO), BF16),
                dma((H,)), dma((2, H)), dma((H,)), dma((2, H)), dma((2, H)), dma((H,)), dma((H,)),
                dma, dma((5, 4)), dma((4, 4)), dma((2,)), dma((3,)), dma((3,)), dma((2,)), dma((2,)), dma((2,)),
                dma((2,)), dma((2,)), dma((9,)), dma((9,)),
                *[dma((n_chunk,))] * 10,
            ],
            compiler_params=pltpu.CompilerParams(collective_id=0, has_side_effects=True, vmem_limit_bytes=46 * 1024 * 1024),
        )(*[pltpu.with_memory_space_constraint(a, pltpu.HBM) for a in (x, w, gamma_vec, beta_vec, dz)])
        z, dx, dw = write_out(z, dx, dw)
        z_full = z.reshape(H, WD, 4 * N, CO).transpose(2, 0, 1, 3)
        dx_full = dx.reshape(H, WD, N, CI).transpose(2, 0, 1, 3)
        dw_full = dw.reshape(3, 3, CI, CO)
        return z_full[None], dx_full[None], dw_full[None]

    return jax.shard_map(device_step, mesh=mesh, in_specs=(act_spec, w_spec, vec_spec, vec_spec, chan_spec), out_specs=(chan_spec, act_spec, w_spec), check_vma=False)
```

```python
import functools

import jax
import jax.numpy as jnp
from jax import lax
from jax.experimental import pallas as pl
from jax.experimental.pallas import tpu as pltpu
from jax.sharding import PartitionSpec as P

MESH = pl.DeviceIdType.MESH
F32 = jnp.float32
BF16 = jnp.bfloat16
PAD = 16
AHEAD = 2
LAG = 3
LAG_OUT = 8
N_B = 16


def remote(src, dst, send_sem, recv_sem, dev):
    return pltpu.make_async_remote_copy(src_ref=src, dst_ref=dst, send_sem=send_sem, recv_sem=recv_sem, device_id=dev, device_id_type=MESH)


def block_kernel(H, WD, CI, CO, n_chunk, x_ref, w_ref, gam_ref, bet_ref, dz_ref, z_ref, dx_ref, dw_ref,
                 xe, xo, ge, go, wall, dzb, zb, vec, acc, prx, pb, rb, mb, xt, relay, *sems):
    (s_xs, s_xr, s_xf, s_gs, s_gr, s_gl, s_gf, s_wl, s_ws, s_wr, s_vl, s_vs, s_vr, s_dl, s_ds, s_dr,
     s_zs, s_zr, s_ps, s_pr, s_os, s_or, s_ms, s_mr, s_ts, s_tr,
     s_bs, s_br, s_us, s_ur) = sems
    R = WD * 8
    sub = n_chunk // 9
    piece = CI // sub
    quarter = CI // 4
    n_a = n_chunk - N_B
    CW = 2 * CO
    zi = lax.axis_index("dp")
    st = lax.axis_index("stage")
    tp = lax.axis_index("tp")
    xi = tp // 2
    c = tp % 2
    y_dev = (zi, 1 - st, tp)
    x_dev = (zi, st, 2 * (1 - xi) + c)
    c_dev = (zi, st, 2 * xi + 1 - c)
    z_mate = jnp.where(zi == 1, 2, 1)
    z_out = jnp.where(zi < 2, 0, 3)
    z_in = jnp.where(zi < 2, 1, 2)
    inner = jnp.logical_or(zi == 1, zi == 2)
    mate_dev = (z_mate, st, tp)
    outer_dev = (z_out, st, tp)
    inner_dev = (z_in, st, tp)

    barrier = pltpu.get_barrier_semaphore()
    for dev in (y_dev, x_dev, c_dev):
        pl.semaphore_signal(barrier, inc=1, device_id=dev, device_id_type=MESH)

    @pl.when(inner)
    def _():
        for dev in (mate_dev, outer_dev):
            pl.semaphore_signal(barrier, inc=1, device_id=dev, device_id_type=MESH)
        pl.semaphore_wait(barrier, 5)

    @pl.when(jnp.logical_not(inner))
    def _():
        pl.semaphore_signal(barrier, inc=1, device_id=inner_dev, device_id_type=MESH)
        pl.semaphore_wait(barrier, 4)

    def zero_borders(buf):
        ch = buf.shape[-1]

        def rows(h, _):
            for s in range(2):
                buf[s, h, 0:PAD, :] = jnp.zeros((PAD, ch), BF16)
                buf[s, h, PAD + R:, :] = jnp.zeros((buf.shape[2] - PAD - R, ch), BF16)
            return 0

        lax.fori_loop(0, H + 2, rows, 0)

    def zero_planes(buf):
        for s in range(2):
            for h in (0, H + 1):
                buf[s, h] = jnp.zeros(buf.shape[2:], BF16)

    def odd_copy(even, odd, s, h):
        n = odd.shape[2]
        odd[s, h] = even[s, h, 8:8 + n, :]

    def tap_rows(even, odd, s, plane, shift, n):
        if shift == 0:
            return even[s, plane, PAD:PAD + n, :]
        start = PAD + 8 * shift - 8
        return odd[s, plane, start:start + n, :]

    def dw_view(k):
        return dw_ref.at[k // sub, pl.ds(pl.multiple_of((k % sub) * piece, piece), piece), :]

    def part_up(k):
        return remote(pb.at[k], pb.at[k], s_os.at[k], s_or.at[k], y_dev)

    def to_mate(k):
        return remote(pb.at[k], mb.at[k], s_ms.at[k], s_mr.at[k], mate_dev)

    def total_down(src, k):
        return remote(src.at[k], dw_view(k), s_ts.at[k], s_tr.at[k], y_dev)

    @pl.when(st == 0)
    def _():
        def x_copy(h):
            return remote(x_ref.at[h], xe.at[xi, h + 1, pl.ds(PAD, R), :], s_xs.at[h], s_xr.at[xi, h], y_dev)

        lax.fori_loop(0, H, lambda h, _: (x_copy(h).start(), 0)[1], 0)
        zero_borders(ge)
        zero_planes(ge)
        zero_planes(go)

        def zero_out(h, _):
            z_ref[h] = jnp.zeros(z_ref.shape[1:], BF16)
            return 0

        lax.fori_loop(0, H, zero_out, 0)

        def zero_dw(t, _):
            dw_ref[t] = jnp.zeros((CI, CO), F32)
            return 0

        lax.fori_loop(0, 9, zero_dw, 0)

        def g_in(j, b):
            return remote(ge.at[b, j + 1, pl.ds(PAD, R), :], ge.at[b, j + 1, pl.ds(PAD, R), :], s_gf.at[j], s_gr.at[b, j], y_dev)

        def relay_in(j):
            return remote(relay.at[j], relay.at[j], s_gf.at[j], s_gl.at[j], y_dev)

        def relay_out(j):
            return remote(relay.at[j], ge.at[xi, j + 1, pl.ds(PAD, R), :], s_gf.at[j], s_gr.at[xi, j], x_dev)

        def g_relay(j):
            relay_in(j).wait_recv()
            relay_out(j).start()

        def relay_rows(lo, hi):
            lax.fori_loop(lo, min(hi, H), lambda j, _: (g_relay(j), 0)[1], 0)

        tp_x = 2 * (1 - xi) + c
        left_dev = (jnp.maximum(zi - 1, 0), st, tp)
        right_dev = (jnp.minimum(zi + 1, 3), st, tp)

        def w_unit(b, q, send_sem, dev):
            view = wall.at[b, :, pl.ds(pl.multiple_of(q * quarter, quarter), quarter), :]
            return remote(view, view, send_sem, s_wr.at[b, q], dev)

        def w_got(q, go_right, go_left):
            w_unit(tp, q, s_ws.at[0, q], y_dev).wait_recv()
            if go_right:
                @pl.when(zi < 3)
                def _():
                    w_unit(tp, q, s_ws.at[2, q], right_dev).start()
            if go_left:
                @pl.when(zi > 0)
                def _():
                    w_unit(tp, q, s_ws.at[3, q], left_dev).start()
            w_unit(tp, q, s_ws.at[0, q], x_dev).start()
            w_unit(tp, q, s_ws.at[1, q], c_dev).start()

        w_got(zi, True, True)
        for d in range(1, 4):
            @pl.when(zi - d >= 0)
            def _():
                w_got(zi - d, True, False)

            @pl.when(zi + d <= 3)
            def _():
                w_got(zi + d, False, True)

            relay_rows(3 * (d - 1), 3 * d)

        def w_cross(q, _):
            w_unit(tp_x, q, s_ws.at[4, q], x_dev).wait_recv()
            w_unit(tp_x, q, s_ws.at[4, q], c_dev).start()
            return 0

        lax.fori_loop(0, 4, w_cross, 0)

        def w_all(q, _):
            for b in (2 * xi + 1 - c, 2 * (1 - xi) + 1 - c):
                w_unit(b, q, s_ws.at[1, q], c_dev).wait_recv()
            return 0

        lax.fori_loop(0, 4, w_all, 0)
        relay_rows(9, H)

        def g_step(j):
            @pl.when(j < H)
            def _():
                g_in(j, xi).wait_recv()
                g_in(j, 1 - xi).wait_recv()
                for b in range(2):
                    odd_copy(ge, go, b, j + 1)

            @pl.when(j >= 1)
            def _():
                h = j - 1
                tot = jnp.zeros((R, CI), F32)
                for b in range(2):
                    for ky in range(3):
                        for kx in range(3):
                            t = 3 * ky + kx
                            lhs = tap_rows(ge, go, b, h + 2 - ky, 1 - kx, R)
                            rhs = jnp.concatenate([wall[2 * b, t], wall[2 * b + 1, t]], axis=1)
                            tot = tot + lax.dot_general(lhs, rhs, (((1,), (1,)), ((), ())), preferred_element_type=F32)
                dx_ref[h] = tot.astype(BF16)

        def b_to_inner(k, dev):
            return remote(pb.at[k], rb.at[k], s_bs.at[k], s_br.at[k], dev)

        def b_to_outer(k, dev):
            return remote(rb.at[k], mb.at[k], s_us.at[k], s_ur.at[k], dev)

        def b_step(i, _):
            k = n_a + i

            @pl.when(k < n_chunk)
            def _():
                part_up(k).wait_recv()

                @pl.when(jnp.logical_not(inner))
                def _():
                    b_to_inner(k, inner_dev).start()

                @pl.when(inner)
                def _():
                    b_to_inner(k, outer_dev).wait_recv()
                    pb[k] = pb[k] + rb[k]
                    to_mate(k).start()

            @pl.when(jnp.logical_and(inner, jnp.logical_and(i >= LAG, k < n_chunk + LAG)))
            def _():
                m = k - LAG
                to_mate(m).wait_recv()
                rb[m] = pb[m] + mb[m]
                b_to_outer(m, outer_dev).start()
                total_down(rb, m).start()

            @pl.when(jnp.logical_and(jnp.logical_not(inner), i >= LAG_OUT))
            def _():
                m = k - LAG_OUT
                b_to_outer(m, inner_dev).wait_recv()
                total_down(mb, m).start()

            @pl.when(i <= H)
            def _():
                g_step(i)

            return 0

        lax.fori_loop(0, N_B + LAG_OUT, b_step, 0)

        def b_done(k, _):
            total_down(rb, k).wait_send()

            @pl.when(jnp.logical_not(inner))
            def _():
                b_to_inner(k, inner_dev).wait_send()

            @pl.when(inner)
            def _():
                to_mate(k).wait_send()
                b_to_outer(k, outer_dev).wait_send()

            return 0

        lax.fori_loop(n_a, n_chunk, b_done, 0)

        def drain(h, _):
            x_copy(h).wait_send()
            relay_out(h).wait_send()
            return 0

        lax.fori_loop(0, H, drain, 0)

        def drain_w(q, _):
            w_unit(tp, q, s_ws.at[0, q], x_dev).wait_send()
            w_unit(tp, q, s_ws.at[1, q], c_dev).wait_send()
            w_unit(tp_x, q, s_ws.at[4, q], c_dev).wait_send()

            @pl.when(jnp.logical_and(zi < 3, q <= zi))
            def _():
                w_unit(tp, q, s_ws.at[2, q], right_dev).wait_send()

            @pl.when(jnp.logical_and(zi > 0, q >= zi))
            def _():
                w_unit(tp, q, s_ws.at[3, q], left_dev).wait_send()

            return 0

        lax.fori_loop(0, 4, drain_w, 0)

    @pl.when(st == 1)
    def _():
        w_loc = pltpu.make_async_copy(w_ref, wall.at[c], s_wl)
        w_core = remote(w_ref, wall.at[c], s_vs.at[2], s_vr.at[2], c_dev)
        vecs_l = [pltpu.make_async_copy(r, vec.at[k, c], s_vl.at[k]) for k, r in enumerate((gam_ref, bet_ref))]
        vecs_r = [remote(r, vec.at[k, c], s_vs.at[k], s_vr.at[k], c_dev) for k, r in enumerate((gam_ref, bet_ref))]
        dz_l = [pltpu.make_async_copy(dz_ref.at[:, :, 2 * s + c], dzb.at[s, c], s_dl.at[s]) for s in range(2)]
        dz_r = [remote(dz_ref.at[:, :, 2 * s + 1 - c], dzb.at[s, c], s_ds.at[s], s_dr.at[s], c_dev) for s in range(2)]

        part = pl.ds(pl.multiple_of(zi * quarter, quarter), quarter)
        w_y = remote(w_ref.at[:, part, :], wall.at[tp, :, part, :], s_ws.at[0, zi], s_wr.at[tp, zi], y_dev)

        w_y.start()
        w_loc.start()
        w_core.start()
        for k in range(2):
            vecs_l[k].start()
            vecs_r[k].start()
            dz_l[k].start()
            dz_r[k].start()

        zero_borders(xe)
        zero_borders(ge)
        for buf in (xe, xo, ge, go):
            zero_planes(buf)

        def zero_acc(t, _):
            for k in range(2):
                acc[k, t] = jnp.zeros((CI, CO), F32)
            return 0

        lax.fori_loop(0, 9, zero_acc, 0)

        def zero_dx(h, _):
            dx_ref[h] = jnp.zeros((R, CI), BF16)
            return 0

        lax.fori_loop(0, H, zero_dx, 0)
        for k in range(2):
            vecs_l[k].wait()
            vecs_r[k].wait_recv()
            dz_l[k].wait()
            dz_r[k].wait_recv()
        w_loc.wait()
        w_core.wait_recv()

        def x_in(j, s):
            view = xe.at[s, j + 1, pl.ds(PAD, R), :]
            return remote(view, view, s_xf.at[j], s_xr.at[s, j], y_dev)

        def x_fwd(j):
            view = xe.at[xi, j + 1, pl.ds(PAD, R), :]
            return remote(view, view, s_xf.at[j], s_xr.at[xi, j], x_dev)

        def g_own(h):
            return remote(ge.at[xi, h + 1, pl.ds(PAD, R), :], ge.at[xi, h + 1, pl.ds(PAD, R), :], s_gs.at[0, h], s_gr.at[xi, h], y_dev)

        def g_other(h):
            return remote(ge.at[1 - xi, h + 1, pl.ds(PAD, R), :], relay.at[h], s_gs.at[1, h], s_gl.at[h], y_dev)

        def x_relay(j):
            x_in(j, xi).wait_recv()
            x_fwd(j).start()

        lax.fori_loop(0, AHEAD, lambda j, _: (x_relay(j), 0)[1], 0)

        def step(j, _):
            @pl.when(j + AHEAD < H)
            def _():
                x_relay(j + AHEAD)

            @pl.when(j < H)
            def _():
                x_in(j, 1 - xi).wait_recv()
                for s in range(2):
                    odd_copy(xe, xo, s, j + 1)

            @pl.when(jnp.logical_and(j >= 1, j < H + 1))
            def _():
                h = j - 1
                pre = jnp.zeros((2 * R, CW), F32)
                for ky in range(3):
                    for kx in range(3):
                        t = 3 * ky + kx
                        lhs = jnp.concatenate([tap_rows(xe, xo, s, h + ky, kx - 1, R) for s in range(2)], axis=0)
                        rhs = jnp.concatenate([wall[0, t], wall[1, t]], axis=1)
                        pre = pre + jnp.dot(lhs, rhs, preferred_element_type=F32)
                for k in range(2):
                    gam = vec[0, k]
                    bet = vec[1, k]
                    for s in range(2):
                        y = pre[s * R:(s + 1) * R, k * CO:(k + 1) * CO] * gam + bet
                        zb[s, k, h] = jnp.maximum(y, 0.0).reshape(WD, 8, CO).astype(BF16)
                        dzr = dzb[s, k, h].astype(F32).reshape(R, CO)
                        ge[s, h + 1, PAD:PAD + R, k * CO:(k + 1) * CO] = jnp.where(y > 0, dzr * gam, 0.0).astype(BF16)
                g_own(h).start()
                g_other(h).start()
                for s in range(2):
                    odd_copy(ge, go, s, h + 1)
                    z_ref[h, :, 2 * s + c] = zb[s, c, h]

            @pl.when(j >= 2)
            def _():
                q = j - 2
                rows = jnp.concatenate([xe[s, q + 1, PAD:PAD + 128, :] for s in range(2)], axis=0)
                xt[...] = rows.T
                for ky in range(3):
                    for kx in range(3):
                        t = 3 * ky + kx
                        rhs = jnp.concatenate([tap_rows(ge, go, s, q + 2 - ky, 1 - kx, 128) for s in range(2)], axis=0)
                        part = jnp.dot(xt[...], rhs, preferred_element_type=F32)
                        for k in range(2):
                            acc[k, t] += part[:, k * CO:(k + 1) * CO]

            return 0

        lax.fori_loop(0, H + 2, step, 0)

        def pair(t):
            return remote(acc.at[1 - c, t], prx.at[t], s_ps.at[t], s_pr.at[t], c_dev)

        lax.fori_loop(0, 9, lambda i, _: (pair((i + n_a // sub) % 9).start(), 0)[1], 0)
        z_r = [remote(zb.at[s, 1 - c], z_ref.at[:, :, 2 * s + c], s_zs.at[s], s_zr.at[s], c_dev) for s in range(2)]
        z_w = [remote(zb.at[s, 1 - c], z_ref.at[:, :, 2 * s + 1 - c], s_zs.at[s], s_zr.at[s], c_dev) for s in range(2)]
        for s in range(2):
            z_r[s].start()

        def own_part(k, fresh):
            t = k // sub
            q = pl.multiple_of((k % sub) * piece, piece)

            @pl.when(fresh)
            def _():
                pair(t).wait_recv()

            return acc[c, t, pl.ds(q, piece), :] + prx[t, pl.ds(q, piece), :]

        def part_a(k):
            return own_part(k, jnp.logical_and(k % sub == 0, k // sub < n_a // sub))

        def send_b(k, _):
            pb[k] = own_part(k, jnp.logical_or(k % sub == 0, k == n_a))
            part_up(k).start()
            return 0

        lax.fori_loop(n_a, n_chunk, send_b, 0)

        def to_inner(k):
            return remote(pb.at[k], rb.at[k], s_os.at[k], s_or.at[k], inner_dev)

        def from_outer(k):
            return remote(pb.at[k], rb.at[k], s_os.at[k], s_or.at[k], outer_dev)

        def to_outer(k):
            return remote(dw_view(k), dw_view(k), s_ts.at[k], s_tr.at[k], outer_dev)

        def from_inner(k):
            return remote(dw_view(k), dw_view(k), s_ts.at[k], s_tr.at[k], inner_dev)

        @pl.when(jnp.logical_not(inner))
        def _():
            def send(k, _):
                pb[k] = part_a(k)
                to_inner(k).start()
                return 0

            lax.fori_loop(0, n_a, send, 0)

            def take(k, _):
                from_inner(k).wait_recv()
                to_inner(k).wait_send()
                return 0

            lax.fori_loop(0, n_a, take, 0)

        @pl.when(inner)
        def _():
            def both(k, _):
                @pl.when(k < n_a)
                def _():
                    part = part_a(k)
                    from_outer(k).wait_recv()
                    pb[k] = part + rb[k]
                    to_mate(k).start()

                @pl.when(k >= LAG)
                def _():
                    m = k - LAG
                    to_mate(m).wait_recv()
                    dw_ref[m // sub, pl.ds(pl.multiple_of((m % sub) * piece, piece), piece), :] = pb[m] + mb[m]
                    to_outer(m).start()

                return 0

            lax.fori_loop(0, n_a + LAG, both, 0)

            def done(k, _):
                to_mate(k).wait_send()
                to_outer(k).wait_send()
                return 0

            lax.fori_loop(0, n_a, done, 0)

        def done_b(k, _):
            total_down(rb, k).wait_recv()
            part_up(k).wait_send()
            return 0

        lax.fori_loop(n_a, n_chunk, done_b, 0)

        def drain(h, _):
            x_fwd(h).wait_send()
            g_own(h).wait_send()
            g_other(h).wait_send()
            return 0

        lax.fori_loop(0, H, drain, 0)

        def drain_w(t, _):
            pair(t).wait_send()
            return 0

        lax.fori_loop(0, 9, drain_w, 0)
        w_core.wait_send()
        w_y.wait_send()
        for k in range(2):
            vecs_r[k].wait_send()
            dz_r[k].wait_send()
            z_r[k].wait_send()
            z_w[k].wait_recv()


def out_kernel(*refs):
    srcs, dsts, sem = refs[:3], refs[3:6], refs[6]
    copies = [pltpu.make_async_copy(a, b, sem.at[i]) for i, (a, b) in enumerate(zip(srcs, dsts))]
    for cp in copies:
        cp.start()
    for cp in copies:
        cp.wait()


def write_out(*arrays):
    return pl.pallas_call(
        out_kernel,
        out_shape=tuple(jax.ShapeDtypeStruct(a.shape, a.dtype) for a in arrays),
        in_specs=[pl.BlockSpec(memory_space=pltpu.VMEM)] * 3,
        out_specs=(pl.BlockSpec(memory_space=pl.ANY),) * 3,
        scratch_shapes=[pltpu.SemaphoreType.DMA((3,))],
        compiler_params=pltpu.CompilerParams(vmem_limit_bytes=16 * 1024 * 1024),
    )(*arrays)


def solution(mesh):
    act_spec = P('stage', ('dp', 'tp'))
    w_spec = P('stage', None, None, None, 'tp')
    vec_spec = P('stage', 'tp')
    chan_spec = P('stage', 'dp', None, None, 'tp')

    def device_step(act_in, w_conv, gamma_vec, beta_vec, z_grad):
        N, H, WD, CI = act_in.shape[1:]
        CO = w_conv.shape[-1]
        R = WD * N
        RP = 128 + 2 * PAD
        n_chunk = 36
        x = act_in[0].transpose(1, 2, 0, 3).reshape(H, R, CI)
        w = w_conv[0].reshape(9, CI, CO)
        dz = z_grad[0].transpose(1, 2, 0, 3).reshape(H, WD, 4, N, CO)
        dma = pltpu.SemaphoreType.DMA
        z, dx, dw = pl.pallas_call(
            functools.partial(block_kernel, H, WD, CI, CO, n_chunk),
            out_shape=(
                jax.ShapeDtypeStruct((H, WD, 4, N, CO), BF16),
                jax.ShapeDtypeStruct((H, R, CI), BF16),
                jax.ShapeDtypeStruct((9, CI, CO), F32),
            ),
            in_specs=[pl.BlockSpec(memory_space=pltpu.HBM)] * 5,
            out_specs=(pl.BlockSpec(memory_space=pltpu.VMEM),) * 3,
            scratch_shapes=[
                pltpu.VMEM((2, H + 2, RP, CI), BF16),
                pltpu.VMEM((2, H + 2, RP - 16, CI), BF16),
                pltpu.VMEM((2, H + 2, RP, 2 * CO), BF16),
                pltpu.VMEM((2, H + 2, RP - 16, 2 * CO), BF16),
                pltpu.VMEM((4, 9, CI, CO), BF16),
                pltpu.VMEM((2, 2, H, WD, N, CO), BF16),
                pltpu.VMEM((2, 2, H, WD, N, CO), BF16),
                pltpu.VMEM((2, 2, 1, CO), F32),
                pltpu.VMEM((2, 9, CI, CO), F32),
                pltpu.VMEM((9, CI, CO), F32),
                pltpu.VMEM((n_chunk, CI // 4, CO), F32),
                pltpu.VMEM((n_chunk, CI // 4, CO), F32),
                pltpu.VMEM((n_chunk, CI // 4, CO), F32),
                pltpu.VMEM((CI, 256), BF16),
                pltpu.VMEM((H, R, 2 * CO), BF16),
                dma((H,)), dma((2, H)), dma((H,)), dma((2, H)), dma((2, H)), dma((H,)), dma((H,)),
                dma, dma((5, 4)), dma((4, 4)), dma((2,)), dma((3,)), dma((3,)), dma((2,)), dma((2,)), dma((2,)),
                dma((2,)), dma((2,)), dma((9,)), dma((9,)),
                *[dma((n_chunk,))] * 10,
            ],
            compiler_params=pltpu.CompilerParams(collective_id=0, has_side_effects=True, vmem_limit_bytes=46 * 1024 * 1024),
        )(*[pltpu.with_memory_space_constraint(a, pltpu.HBM) for a in (x, w, gamma_vec, beta_vec, dz)])
        z, dx, dw = write_out(z, dx, dw)
        z_full = z.reshape(H, WD, 4 * N, CO).transpose(2, 0, 1, 3)
        dx_full = dx.reshape(H, WD, N, CI).transpose(2, 0, 1, 3)
        dw_full = dw.reshape(3, 3, CI, CO)
        return z_full[None], dx_full[None], dw_full[None]

    return jax.shard_map(device_step, mesh=mesh, in_specs=(act_spec, w_spec, vec_spec, vec_spec, chan_spec), out_specs=(chan_spec, act_spec, w_spec), check_vma=False)
```

```python
import functools

import jax
import jax.numpy as jnp
from jax import lax
from jax.experimental import pallas as pl
from jax.experimental.pallas import tpu as pltpu
from jax.sharding import PartitionSpec as P

MESH = pl.DeviceIdType.MESH
F32 = jnp.float32
BF16 = jnp.bfloat16
PAD = 16
AHEAD = 2
LAG = 3
LAG_OUT = 8
N_B = 16


def remote(src, dst, send_sem, recv_sem, dev):
    return pltpu.make_async_remote_copy(src_ref=src, dst_ref=dst, send_sem=send_sem, recv_sem=recv_sem, device_id=dev, device_id_type=MESH)


def block_kernel(H, WD, CI, CO, n_chunk, x_ref, w_ref, gam_ref, bet_ref, dz_ref, z_ref, dx_ref, dw_ref,
                 xe, xo, ge, go, wall, dzb, zb, vec, acc, prx, pb, rb, mb, xt, relay, *sems):
    (s_xs, s_xr, s_xf, s_gs, s_gr, s_gl, s_gf, s_wl, s_ws, s_wr, s_vl, s_vs, s_vr, s_dl, s_ds, s_dr,
     s_zs, s_zr, s_ps, s_pr, s_os, s_or, s_ms, s_mr, s_ts, s_tr,
     s_bs, s_br, s_us, s_ur) = sems
    R = WD * 8
    sub = n_chunk // 9
    piece = CI // sub
    quarter = CI // 4
    n_a = n_chunk - N_B
    CW = 2 * CO
    zi = lax.axis_index("dp")
    st = lax.axis_index("stage")
    tp = lax.axis_index("tp")
    xi = tp // 2
    c = tp % 2
    y_dev = (zi, 1 - st, tp)
    x_dev = (zi, st, 2 * (1 - xi) + c)
    c_dev = (zi, st, 2 * xi + 1 - c)
    z_mate = jnp.where(zi == 1, 2, 1)
    z_out = jnp.where(zi < 2, 0, 3)
    z_in = jnp.where(zi < 2, 1, 2)
    inner = jnp.logical_or(zi == 1, zi == 2)
    mate_dev = (z_mate, st, tp)
    outer_dev = (z_out, st, tp)
    inner_dev = (z_in, st, tp)

    barrier = pltpu.get_barrier_semaphore()
    for dev in (y_dev, x_dev, c_dev):
        pl.semaphore_signal(barrier, inc=1, device_id=dev, device_id_type=MESH)

    @pl.when(inner)
    def _():
        for dev in (mate_dev, outer_dev):
            pl.semaphore_signal(barrier, inc=1, device_id=dev, device_id_type=MESH)
        pl.semaphore_wait(barrier, 5)

    @pl.when(jnp.logical_not(inner))
    def _():
        pl.semaphore_signal(barrier, inc=1, device_id=inner_dev, device_id_type=MESH)
        pl.semaphore_wait(barrier, 4)

    def zero_borders(buf):
        ch = buf.shape[-1]

        def rows(h, _):
            for s in range(2):
                buf[s, h, 0:PAD, :] = jnp.zeros((PAD, ch), BF16)
                buf[s, h, PAD + R:, :] = jnp.zeros((buf.shape[2] - PAD - R, ch), BF16)
            return 0

        lax.fori_loop(0, H + 2, rows, 0)

    def zero_planes(buf):
        for s in range(2):
            for h in (0, H + 1):
                buf[s, h] = jnp.zeros(buf.shape[2:], BF16)

    def odd_copy(even, odd, s, h):
        n = odd.shape[2]
        odd[s, h] = even[s, h, 8:8 + n, :]

    def tap_rows(even, odd, s, plane, shift, n):
        if shift == 0:
            return even[s, plane, PAD:PAD + n, :]
        start = PAD + 8 * shift - 8
        return odd[s, plane, start:start + n, :]

    x_cut = ((0, R // 2 // 16 * 16), (R // 2 // 16 * 16, R - R // 2 // 16 * 16))

    def x_view(s, h, p):
        return xe.at[s, h + 1, pl.ds(PAD + x_cut[p][0], x_cut[p][1]), :]

    def dw_view(k):
        return dw_ref.at[k // sub, pl.ds(pl.multiple_of((k % sub) * piece, piece), piece), :]

    def part_up(k):
        return remote(pb.at[k], pb.at[k], s_os.at[k], s_or.at[k], y_dev)

    def to_mate(k):
        return remote(pb.at[k], mb.at[k], s_ms.at[k], s_mr.at[k], mate_dev)

    def total_down(src, k):
        return remote(src.at[k], dw_view(k), s_ts.at[k], s_tr.at[k], y_dev)

    @pl.when(st == 0)
    def _():
        def x_copy(h, p):
            return remote(x_ref.at[h, pl.ds(*x_cut[p]), :], x_view(xi, h, p), s_xs.at[p, h], s_xr.at[xi, p, h], y_dev)

        def x_send(h, _):
            for p in range(2):
                x_copy(h, p).start()
            return 0

        lax.fori_loop(0, H, x_send, 0)
        zero_borders(ge)
        zero_planes(ge)
        zero_planes(go)

        def zero_out(h, _):
            z_ref[h] = jnp.zeros(z_ref.shape[1:], BF16)
            return 0

        lax.fori_loop(0, H, zero_out, 0)

        def zero_dw(t, _):
            dw_ref[t] = jnp.zeros((CI, CO), F32)
            return 0

        lax.fori_loop(0, 9, zero_dw, 0)

        def g_in(j, b):
            return remote(ge.at[b, j + 1, pl.ds(PAD, R), :], ge.at[b, j + 1, pl.ds(PAD, R), :], s_gf.at[j], s_gr.at[b, j], y_dev)

        def relay_in(j):
            return remote(relay.at[j], relay.at[j], s_gf.at[j], s_gl.at[j], y_dev)

        def relay_out(j):
            return remote(relay.at[j], ge.at[xi, j + 1, pl.ds(PAD, R), :], s_gf.at[j], s_gr.at[xi, j], x_dev)

        def g_relay(j):
            relay_in(j).wait_recv()
            relay_out(j).start()

        def relay_rows(lo, hi):
            lax.fori_loop(lo, min(hi, H), lambda j, _: (g_relay(j), 0)[1], 0)

        tp_x = 2 * (1 - xi) + c
        left_dev = (jnp.maximum(zi - 1, 0), st, tp)
        right_dev = (jnp.minimum(zi + 1, 3), st, tp)

        def w_unit(b, q, send_sem, dev):
            view = wall.at[b, :, pl.ds(pl.multiple_of(q * quarter, quarter), quarter), :]
            return remote(view, view, send_sem, s_wr.at[b, q], dev)

        def w_got(q, go_right, go_left):
            w_unit(tp, q, s_ws.at[0, q], y_dev).wait_recv()
            if go_right:
                @pl.when(zi < 3)
                def _():
                    w_unit(tp, q, s_ws.at[2, q], right_dev).start()
            if go_left:
                @pl.when(zi > 0)
                def _():
                    w_unit(tp, q, s_ws.at[3, q], left_dev).start()
            w_unit(tp, q, s_ws.at[0, q], x_dev).start()
            w_unit(tp, q, s_ws.at[1, q], c_dev).start()

        w_got(zi, True, True)
        for d in range(1, 4):
            @pl.when(zi - d >= 0)
            def _():
                w_got(zi - d, True, False)

            @pl.when(zi + d <= 3)
            def _():
                w_got(zi + d, False, True)

            if d > 1:
                relay_rows(3 * (d - 2), 3 * (d - 1))

        relay_rows(6, 8)

        def w_cross(q, _):
            w_unit(tp_x, q, s_ws.at[4, q], x_dev).wait_recv()
            w_unit(tp_x, q, s_ws.at[4, q], c_dev).start()
            return 0

        lax.fori_loop(0, 4, w_cross, 0)
        relay_rows(8, H)

        def w_all(q, _):
            for b in (2 * xi + 1 - c, 2 * (1 - xi) + 1 - c):
                w_unit(b, q, s_ws.at[1, q], c_dev).wait_recv()
            return 0

        lax.fori_loop(0, 4, w_all, 0)

        def g_step(j):
            @pl.when(j < H)
            def _():
                g_in(j, xi).wait_recv()
                g_in(j, 1 - xi).wait_recv()
                for b in range(2):
                    odd_copy(ge, go, b, j + 1)

            @pl.when(j >= 1)
            def _():
                h = j - 1
                tot = jnp.zeros((R, CI), F32)
                for b in range(2):
                    for ky in range(3):
                        for kx in range(3):
                            t = 3 * ky + kx
                            lhs = tap_rows(ge, go, b, h + 2 - ky, 1 - kx, R)
                            rhs = jnp.concatenate([wall[2 * b, t], wall[2 * b + 1, t]], axis=1)
                            tot = tot + lax.dot_general(lhs, rhs, (((1,), (1,)), ((), ())), preferred_element_type=F32)
                dx_ref[h] = tot.astype(BF16)

        def b_to_inner(k, dev):
            return remote(pb.at[k], rb.at[k], s_bs.at[k], s_br.at[k], dev)

        def b_to_outer(k, dev):
            return remote(rb.at[k], mb.at[k], s_us.at[k], s_ur.at[k], dev)

        def b_step(i, _):
            k = n_a + i

            @pl.when(k < n_chunk)
            def _():
                part_up(k).wait_recv()

                @pl.when(jnp.logical_not(inner))
                def _():
                    b_to_inner(k, inner_dev).start()

                @pl.when(inner)
                def _():
                    b_to_inner(k, outer_dev).wait_recv()
                    pb[k] = pb[k] + rb[k]
                    to_mate(k).start()

            @pl.when(jnp.logical_and(inner, jnp.logical_and(i >= LAG, k < n_chunk + LAG)))
            def _():
                m = k - LAG
                to_mate(m).wait_recv()
                rb[m] = pb[m] + mb[m]
                b_to_outer(m, outer_dev).start()
                total_down(rb, m).start()

            @pl.when(jnp.logical_and(jnp.logical_not(inner), i >= LAG_OUT))
            def _():
                m = k - LAG_OUT
                b_to_outer(m, inner_dev).wait_recv()
                total_down(mb, m).start()

            @pl.when(i <= H)
            def _():
                g_step(i)

            return 0

        lax.fori_loop(0, N_B + LAG_OUT, b_step, 0)

        def b_done(k, _):
            total_down(rb, k).wait_send()

            @pl.when(jnp.logical_not(inner))
            def _():
                b_to_inner(k, inner_dev).wait_send()

            @pl.when(inner)
            def _():
                to_mate(k).wait_send()
                b_to_outer(k, outer_dev).wait_send()

            return 0

        lax.fori_loop(n_a, n_chunk, b_done, 0)

        def drain(h, _):
            for p in range(2):
                x_copy(h, p).wait_send()
            relay_out(h).wait_send()
            return 0

        lax.fori_loop(0, H, drain, 0)

        def drain_w(q, _):
            w_unit(tp, q, s_ws.at[0, q], x_dev).wait_send()
            w_unit(tp, q, s_ws.at[1, q], c_dev).wait_send()
            w_unit(tp_x, q, s_ws.at[4, q], c_dev).wait_send()

            @pl.when(jnp.logical_and(zi < 3, q <= zi))
            def _():
                w_unit(tp, q, s_ws.at[2, q], right_dev).wait_send()

            @pl.when(jnp.logical_and(zi > 0, q >= zi))
            def _():
                w_unit(tp, q, s_ws.at[3, q], left_dev).wait_send()

            return 0

        lax.fori_loop(0, 4, drain_w, 0)

    @pl.when(st == 1)
    def _():
        w_loc = pltpu.make_async_copy(w_ref, wall.at[c], s_wl)
        w_core = remote(w_ref, wall.at[c], s_vs.at[2], s_vr.at[2], c_dev)
        vecs_l = [pltpu.make_async_copy(r, vec.at[k, c], s_vl.at[k]) for k, r in enumerate((gam_ref, bet_ref))]
        vecs_r = [remote(r, vec.at[k, c], s_vs.at[k], s_vr.at[k], c_dev) for k, r in enumerate((gam_ref, bet_ref))]
        dz_l = [pltpu.make_async_copy(dz_ref.at[:, :, 2 * s + c], dzb.at[s, c], s_dl.at[s]) for s in range(2)]
        dz_r = [remote(dz_ref.at[:, :, 2 * s + 1 - c], dzb.at[s, c], s_ds.at[s], s_dr.at[s], c_dev) for s in range(2)]

        part = pl.ds(pl.multiple_of(zi * quarter, quarter), quarter)
        w_y = remote(w_ref.at[:, part, :], wall.at[tp, :, part, :], s_ws.at[0, zi], s_wr.at[tp, zi], y_dev)

        w_y.start()
        w_loc.start()
        w_core.start()
        for k in range(2):
            vecs_l[k].start()
            vecs_r[k].start()
            dz_l[k].start()
            dz_r[k].start()

        zero_borders(xe)
        zero_borders(ge)
        for buf in (xe, xo, ge, go):
            zero_planes(buf)

        def zero_acc(t, _):
            for k in range(2):
                acc[k, t] = jnp.zeros((CI, CO), F32)
            return 0

        lax.fori_loop(0, 9, zero_acc, 0)

        def zero_dx(h, _):
            dx_ref[h] = jnp.zeros((R, CI), BF16)
            return 0

        lax.fori_loop(0, H, zero_dx, 0)
        for k in range(2):
            vecs_l[k].wait()
            vecs_r[k].wait_recv()
            dz_l[k].wait()
            dz_r[k].wait_recv()
        w_loc.wait()
        w_core.wait_recv()

        def x_in(j, s, p):
            return remote(x_view(s, j, p), x_view(s, j, p), s_xf.at[p, j], s_xr.at[s, p, j], y_dev)

        def x_fwd(j, p):
            return remote(x_view(xi, j, p), x_view(xi, j, p), s_xf.at[p, j], s_xr.at[xi, p, j], x_dev)

        def g_own(h):
            return remote(ge.at[xi, h + 1, pl.ds(PAD, R), :], ge.at[xi, h + 1, pl.ds(PAD, R), :], s_gs.at[0, h], s_gr.at[xi, h], y_dev)

        def g_other(h):
            return remote(ge.at[1 - xi, h + 1, pl.ds(PAD, R), :], relay.at[h], s_gs.at[1, h], s_gl.at[h], y_dev)

        def x_relay(j):
            for p in range(2):
                x_in(j, xi, p).wait_recv()
                x_fwd(j, p).start()

        lax.fori_loop(0, AHEAD, lambda j, _: (x_relay(j), 0)[1], 0)

        def turn_x(q):
            rows = jnp.concatenate([xe[s, q + 1, PAD:PAD + 128, :] for s in range(2)], axis=0)
            xt[...] = rows.T

        def add_dw(q, t):
            rhs = jnp.concatenate([tap_rows(ge, go, s, q + 2 - t // 3, 1 - t % 3, 128) for s in range(2)], axis=0)
            prod = jnp.dot(xt[...], rhs, preferred_element_type=F32)
            for k in range(2):
                acc[k, t] += prod[:, k * CO:(k + 1) * CO]

        def step(j, _):
            @pl.when(j + AHEAD < H)
            def _():
                x_relay(j + AHEAD)

            @pl.when(j < H)
            def _():
                for p in range(2):
                    x_in(j, 1 - xi, p).wait_recv()
                for s in range(2):
                    odd_copy(xe, xo, s, j + 1)

            @pl.when(jnp.logical_and(j >= 1, j < H + 1))
            def _():
                h = j - 1
                pre = jnp.zeros((2 * R, CW), F32)
                for ky in range(3):
                    for kx in range(3):
                        t = 3 * ky + kx
                        lhs = jnp.concatenate([tap_rows(xe, xo, s, h + ky, kx - 1, R) for s in range(2)], axis=0)
                        rhs = jnp.concatenate([wall[0, t], wall[1, t]], axis=1)
                        pre = pre + jnp.dot(lhs, rhs, preferred_element_type=F32)
                for k in range(2):
                    gam = vec[0, k]
                    bet = vec[1, k]
                    for s in range(2):
                        y = pre[s * R:(s + 1) * R, k * CO:(k + 1) * CO] * gam + bet
                        zb[s, k, h] = jnp.maximum(y, 0.0).reshape(WD, 8, CO).astype(BF16)
                        dzr = dzb[s, k, h].astype(F32).reshape(R, CO)
                        ge[s, h + 1, PAD:PAD + R, k * CO:(k + 1) * CO] = jnp.where(y > 0, dzr * gam, 0.0).astype(BF16)
                g_own(h).start()
                g_other(h).start()
                for s in range(2):
                    odd_copy(ge, go, s, h + 1)
                    z_ref[h, :, 2 * s + c] = zb[s, c, h]

            @pl.when(j >= 2)
            def _():
                turn_x(j - 2)
                for t in range(9):
                    add_dw(j - 2, t)

            return 0

        lax.fori_loop(0, H + 1, step, 0)

        def pair(t):
            return remote(acc.at[1 - c, t], prx.at[t], s_ps.at[t], s_pr.at[t], c_dev)

        n_t = n_a // sub
        order = sorted(range(9), key=lambda t: 2 * (t - n_t) if t >= n_t else 2 * t + 1)
        turn_x(H - 1)
        for t in order:
            if t >= 3:
                add_dw(H - 1, t)
            pair(t).start()
        z_r = [remote(zb.at[s, 1 - c], z_ref.at[:, :, 2 * s + c], s_zs.at[s], s_zr.at[s], c_dev) for s in range(2)]
        z_w = [remote(zb.at[s, 1 - c], z_ref.at[:, :, 2 * s + 1 - c], s_zs.at[s], s_zr.at[s], c_dev) for s in range(2)]
        for s in range(2):
            z_r[s].start()

        def own_part(k, fresh):
            t = k // sub
            q = pl.multiple_of((k % sub) * piece, piece)

            @pl.when(fresh)
            def _():
                pair(t).wait_recv()

            return acc[c, t, pl.ds(q, piece), :] + prx[t, pl.ds(q, piece), :]

        def part_a(k):
            return own_part(k, jnp.logical_and(k % sub == 0, k // sub < n_a // sub))

        def send_b(i):
            @pl.when(i < N_B)
            def _():
                k = n_a + i
                pb[k] = own_part(k, jnp.logical_or(k % sub == 0, k == n_a))
                part_up(k).start()

        def to_inner(k):
            return remote(pb.at[k], rb.at[k], s_os.at[k], s_or.at[k], inner_dev)

        def from_outer(k):
            return remote(pb.at[k], rb.at[k], s_os.at[k], s_or.at[k], outer_dev)

        def to_outer(k):
            return remote(dw_view(k), dw_view(k), s_ts.at[k], s_tr.at[k], outer_dev)

        def from_inner(k):
            return remote(dw_view(k), dw_view(k), s_ts.at[k], s_tr.at[k], inner_dev)

        @pl.when(jnp.logical_not(inner))
        def _():
            def send(k, _):
                send_b(k)

                @pl.when(k < n_a)
                def _():
                    pb[k] = part_a(k)
                    to_inner(k).start()

                return 0

            lax.fori_loop(0, max(n_a, N_B), send, 0)

            def take(k, _):
                from_inner(k).wait_recv()
                to_inner(k).wait_send()
                return 0

            lax.fori_loop(0, n_a, take, 0)

        @pl.when(inner)
        def _():
            def both(k, _):
                for i in range(2):
                    send_b(2 * k + i)

                @pl.when(k < n_a)
                def _():
                    part = part_a(k)
                    from_outer(k).wait_recv()
                    pb[k] = part + rb[k]
                    to_mate(k).start()

                @pl.when(k >= LAG)
                def _():
                    m = k - LAG
                    to_mate(m).wait_recv()
                    dw_ref[m // sub, pl.ds(pl.multiple_of((m % sub) * piece, piece), piece), :] = pb[m] + mb[m]
                    to_outer(m).start()

                return 0

            lax.fori_loop(0, n_a + LAG, both, 0)

            def done(k, _):
                to_mate(k).wait_send()
                to_outer(k).wait_send()
                return 0

            lax.fori_loop(0, n_a, done, 0)

        def done_b(k, _):
            total_down(rb, k).wait_recv()
            part_up(k).wait_send()
            return 0

        lax.fori_loop(n_a, n_chunk, done_b, 0)

        def drain(h, _):
            for p in range(2):
                x_fwd(h, p).wait_send()
            g_own(h).wait_send()
            g_other(h).wait_send()
            return 0

        lax.fori_loop(0, H, drain, 0)

        def drain_w(t, _):
            pair(t).wait_send()
            return 0

        lax.fori_loop(0, 9, drain_w, 0)
        w_core.wait_send()
        w_y.wait_send()
        for k in range(2):
            vecs_r[k].wait_send()
            dz_r[k].wait_send()
            z_r[k].wait_send()
            z_w[k].wait_recv()


def out_kernel(*refs):
    srcs, dsts, sem = refs[:3], refs[3:6], refs[6]
    copies = [pltpu.make_async_copy(a, b, sem.at[i]) for i, (a, b) in enumerate(zip(srcs, dsts))]
    for cp in copies:
        cp.start()
    for cp in copies:
        cp.wait()


def write_out(*arrays):
    return pl.pallas_call(
        out_kernel,
        out_shape=tuple(jax.ShapeDtypeStruct(a.shape, a.dtype) for a in arrays),
        in_specs=[pl.BlockSpec(memory_space=pltpu.VMEM)] * 3,
        out_specs=(pl.BlockSpec(memory_space=pl.ANY),) * 3,
        scratch_shapes=[pltpu.SemaphoreType.DMA((3,))],
        compiler_params=pltpu.CompilerParams(vmem_limit_bytes=16 * 1024 * 1024),
    )(*arrays)


def solution(mesh):
    act_spec = P('stage', ('dp', 'tp'))
    w_spec = P('stage', None, None, None, 'tp')
    vec_spec = P('stage', 'tp')
    chan_spec = P('stage', 'dp', None, None, 'tp')

    def device_step(act_in, w_conv, gamma_vec, beta_vec, z_grad):
        N, H, WD, CI = act_in.shape[1:]
        CO = w_conv.shape[-1]
        R = WD * N
        RP = 128 + 2 * PAD
        n_chunk = 36
        x = act_in[0].transpose(1, 2, 0, 3).reshape(H, R, CI)
        w = w_conv[0].reshape(9, CI, CO)
        dz = z_grad[0].transpose(1, 2, 0, 3).reshape(H, WD, 4, N, CO)
        dma = pltpu.SemaphoreType.DMA
        z, dx, dw = pl.pallas_call(
            functools.partial(block_kernel, H, WD, CI, CO, n_chunk),
            out_shape=(
                jax.ShapeDtypeStruct((H, WD, 4, N, CO), BF16),
                jax.ShapeDtypeStruct((H, R, CI), BF16),
                jax.ShapeDtypeStruct((9, CI, CO), F32),
            ),
            in_specs=[pl.BlockSpec(memory_space=pltpu.HBM)] * 5,
            out_specs=(pl.BlockSpec(memory_space=pltpu.VMEM),) * 3,
            scratch_shapes=[
                pltpu.VMEM((2, H + 2, RP, CI), BF16),
                pltpu.VMEM((2, H + 2, RP - 16, CI), BF16),
                pltpu.VMEM((2, H + 2, RP, 2 * CO), BF16),
                pltpu.VMEM((2, H + 2, RP - 16, 2 * CO), BF16),
                pltpu.VMEM((4, 9, CI, CO), BF16),
                pltpu.VMEM((2, 2, H, WD, N, CO), BF16),
                pltpu.VMEM((2, 2, H, WD, N, CO), BF16),
                pltpu.VMEM((2, 2, 1, CO), F32),
                pltpu.VMEM((2, 9, CI, CO), F32),
                pltpu.VMEM((9, CI, CO), F32),
                pltpu.VMEM((n_chunk, CI // 4, CO), F32),
                pltpu.VMEM((n_chunk, CI // 4, CO), F32),
                pltpu.VMEM((n_chunk, CI // 4, CO), F32),
                pltpu.VMEM((CI, 256), BF16),
                pltpu.VMEM((H, R, 2 * CO), BF16),
                dma((2, H)), dma((2, 2, H)), dma((2, H)), dma((2, H)), dma((2, H)), dma((H,)), dma((H,)),
                dma, dma((5, 4)), dma((4, 4)), dma((2,)), dma((3,)), dma((3,)), dma((2,)), dma((2,)), dma((2,)),
                dma((2,)), dma((2,)), dma((9,)), dma((9,)),
                *[dma((n_chunk,))] * 10,
            ],
            compiler_params=pltpu.CompilerParams(collective_id=0, has_side_effects=True, vmem_limit_bytes=46 * 1024 * 1024),
        )(*[pltpu.with_memory_space_constraint(a, pltpu.HBM) for a in (x, w, gamma_vec, beta_vec, dz)])
        z, dx, dw = write_out(z, dx, dw)
        z_full = z.reshape(H, WD, 4 * N, CO).transpose(2, 0, 1, 3)
        dx_full = dx.reshape(H, WD, N, CI).transpose(2, 0, 1, 3)
        dw_full = dw.reshape(3, 3, CI, CO)
        return z_full[None], dx_full[None], dw_full[None]

    return jax.shard_map(device_step, mesh=mesh, in_specs=(act_spec, w_spec, vec_spec, vec_spec, chan_spec), out_specs=(chan_spec, act_spec, w_spec), check_vma=False)
```

```python
import functools

import jax
import jax.numpy as jnp
from jax import lax
from jax.experimental import pallas as pl
from jax.experimental.pallas import tpu as pltpu
from jax.sharding import PartitionSpec as P

MESH = pl.DeviceIdType.MESH
F32 = jnp.float32
BF16 = jnp.bfloat16
PAD = 16
AHEAD = 2
LAG = 5
LAG_OUT = 14
N_B = 30


def remote(src, dst, send_sem, recv_sem, dev):
    return pltpu.make_async_remote_copy(src_ref=src, dst_ref=dst, send_sem=send_sem, recv_sem=recv_sem, device_id=dev, device_id_type=MESH)


def block_kernel(H, WD, CI, CO, n_chunk, x_ref, w_ref, gam_ref, bet_ref, dz_ref, z_ref, dx_ref, dw_ref,
                 xe, xo, ge, go, wall, dzb, zb, vec, acc, prx, pb, rb, mb, xt, relay, *sems):
    (s_xs, s_xr, s_xf, s_gs, s_gr, s_gl, s_gf, s_wl, s_ws, s_wr, s_vl, s_vs, s_vr, s_dl, s_ds, s_dr,
     s_zs, s_zr, s_ps, s_pr, s_os, s_or, s_ms, s_mr, s_ts, s_tr) = sems
    R = WD * 8
    sub = n_chunk // 9
    piece = CI // sub
    quarter = CI // 4
    n_blk = min(CI, 256)
    n_a = n_chunk - N_B
    CW = 2 * CO
    zi = lax.axis_index("dp")
    st = lax.axis_index("stage")
    tp = lax.axis_index("tp")
    xi = tp // 2
    c = tp % 2
    y_dev = (zi, 1 - st, tp)
    x_dev = (zi, st, 2 * (1 - xi) + c)
    c_dev = (zi, st, 2 * xi + 1 - c)
    z_mate = jnp.where(zi == 1, 2, 1)
    z_out = jnp.where(zi < 2, 0, 3)
    z_in = jnp.where(zi < 2, 1, 2)
    inner = jnp.logical_or(zi == 1, zi == 2)
    mate_dev = (z_mate, st, tp)
    outer_dev = (z_out, st, tp)
    inner_dev = (z_in, st, tp)

    barrier = pltpu.get_barrier_semaphore()
    for dev in (y_dev, x_dev, c_dev):
        pl.semaphore_signal(barrier, inc=1, device_id=dev, device_id_type=MESH)

    @pl.when(inner)
    def _():
        for dev in (mate_dev, outer_dev):
            pl.semaphore_signal(barrier, inc=1, device_id=dev, device_id_type=MESH)
        pl.semaphore_wait(barrier, 5)

    @pl.when(jnp.logical_not(inner))
    def _():
        pl.semaphore_signal(barrier, inc=1, device_id=inner_dev, device_id_type=MESH)
        pl.semaphore_wait(barrier, 4)

    def zero_borders(buf):
        ch = buf.shape[-1]

        def rows(h, _):
            for s in range(2):
                buf[s, h, 0:PAD, :] = jnp.zeros((PAD, ch), BF16)
                buf[s, h, PAD + R:, :] = jnp.zeros((buf.shape[2] - PAD - R, ch), BF16)
            return 0

        lax.fori_loop(0, H + 2, rows, 0)

    def zero_planes(buf):
        for s in range(2):
            for h in (0, H + 1):
                buf[s, h] = jnp.zeros(buf.shape[2:], BF16)

    def odd_copy(even, odd, s, h):
        n = odd.shape[2]
        odd[s, h] = even[s, h, 8:8 + n, :]

    def tap_rows(even, odd, s, plane, shift, n):
        if shift == 0:
            return even[s, plane, PAD:PAD + n, :]
        start = PAD + 8 * shift - 8
        return odd[s, plane, start:start + n, :]

    x_cut = ((0, R // 2 // 16 * 16), (R // 2 // 16 * 16, R - R // 2 // 16 * 16))

    def x_view(s, h, p):
        return xe.at[s, h + 1, pl.ds(PAD + x_cut[p][0], x_cut[p][1]), :]

    def dw_view(k):
        return dw_ref.at[k // sub, pl.ds(pl.multiple_of((k % sub) * piece, piece), piece), :]

    def part_up(k):
        return remote(pb.at[k], pb.at[k], s_os.at[k], s_or.at[k], y_dev)

    def to_mate(k):
        return remote(pb.at[k], mb.at[k], s_ms.at[k], s_mr.at[k], mate_dev)

    def total_down(src, k):
        return remote(src.at[k], dw_view(k), s_ts.at[k], s_tr.at[k], y_dev)

    @pl.when(st == 0)
    def _():
        def x_copy(h, p):
            return remote(x_ref.at[h, pl.ds(*x_cut[p]), :], x_view(xi, h, p), s_xs.at[p, h], s_xr.at[xi, p, h], y_dev)

        def x_send(h, _):
            for p in range(2):
                x_copy(h, p).start()
            return 0

        lax.fori_loop(0, H, x_send, 0)
        zero_borders(ge)
        zero_planes(ge)
        zero_planes(go)

        def zero_out(h, _):
            z_ref[h] = jnp.zeros(z_ref.shape[1:], BF16)
            return 0

        lax.fori_loop(0, H, zero_out, 0)

        def zero_dw(t, _):
            dw_ref[t] = jnp.zeros((CI, CO), F32)
            return 0

        lax.fori_loop(0, 9, zero_dw, 0)

        def g_in(j, b):
            return remote(ge.at[b, j + 1, pl.ds(PAD, R), :], ge.at[b, j + 1, pl.ds(PAD, R), :], s_gf.at[j], s_gr.at[b, j], y_dev)

        def relay_in(j):
            return remote(relay.at[j], relay.at[j], s_gf.at[j], s_gl.at[j], y_dev)

        def relay_out(j):
            return remote(relay.at[j], ge.at[xi, j + 1, pl.ds(PAD, R), :], s_gf.at[j], s_gr.at[xi, j], x_dev)

        def g_relay(j):
            relay_in(j).wait_recv()
            relay_out(j).start()

        def relay_rows(lo, hi):
            lax.fori_loop(lo, min(hi, H), lambda j, _: (g_relay(j), 0)[1], 0)

        tp_x = 2 * (1 - xi) + c
        left_dev = (jnp.maximum(zi - 1, 0), st, tp)
        right_dev = (jnp.minimum(zi + 1, 3), st, tp)

        def w_unit(b, q, y, kind, dev):
            view = wall.at[b, pl.ds(3 * y, 3), pl.ds(pl.multiple_of(q * quarter, quarter), quarter), :]
            return remote(view, view, s_ws.at[kind, q, y], s_wr.at[b, q, y], dev)

        def w_got(q, go_right, go_left):
            def take(y, _):
                w_unit(tp, q, y, 0, y_dev).wait_recv()
                if go_right:
                    @pl.when(zi < 3)
                    def _():
                        w_unit(tp, q, y, 2, right_dev).start()
                if go_left:
                    @pl.when(zi > 0)
                    def _():
                        w_unit(tp, q, y, 3, left_dev).start()
                w_unit(tp, q, y, 0, x_dev).start()
                w_unit(tp, q, y, 1, c_dev).start()
                return 0

            lax.fori_loop(0, 3, take, 0)

        w_got(zi, True, True)
        for d in range(1, 4):
            @pl.when(zi - d >= 0)
            def _():
                w_got(zi - d, True, False)

            @pl.when(zi + d <= 3)
            def _():
                w_got(zi + d, False, True)

            relay_rows(2 * (d - 1), 2 * d)

        def w_cross(q, _):
            for y in range(3):
                w_unit(tp_x, q, y, 4, x_dev).wait_recv()
                w_unit(tp_x, q, y, 4, c_dev).start()
            return 0

        lax.fori_loop(0, 4, w_cross, 0)
        relay_rows(6, 10)

        def w_all(q, _):
            for y in range(3):
                for b in (2 * xi + 1 - c, 2 * (1 - xi) + 1 - c):
                    w_unit(b, q, y, 1, c_dev).wait_recv()
            return 0

        lax.fori_loop(0, 4, w_all, 0)

        G = 4

        def g_take(j, _):
            g_in(j, xi).wait_recv()
            g_in(j, 1 - xi).wait_recv()
            for b in range(2):
                odd_copy(ge, go, b, j + 1)
            return 0

        def dx_rows(h0):
            for n in range(CI // n_blk):
                tot = jnp.zeros((G * R, n_blk), F32)
                for b in range(2):
                    for t in range(9):
                        lhs = jnp.concatenate([tap_rows(ge, go, b, h0 + r + 2 - t // 3, 1 - t % 3, R) for r in range(G)], axis=0)
                        rhs = jnp.concatenate([wall[2 * b + i, t, n * n_blk:(n + 1) * n_blk, :] for i in range(2)], axis=1)
                        tot = tot + lax.dot_general(lhs, rhs, (((1,), (1,)), ((), ())), preferred_element_type=F32)
                for r in range(G):
                    dx_ref[h0 + r, :, n * n_blk:(n + 1) * n_blk] = tot[r * R:(r + 1) * R].astype(BF16)

        def dx_step(i, _):
            lo = jnp.where(i == 0, 0, G * i + 1)
            hi = jnp.minimum(G * i + G + 1, H)
            @pl.when(i >= 1)
            def _():
                lax.fori_loop(jnp.minimum(8 + 2 * i, H), jnp.minimum(10 + 2 * i, H), lambda j, _: (g_relay(j), 0)[1], 0)

            lax.fori_loop(lo, hi, g_take, 0)
            dx_rows(jnp.minimum(G * i, H - G))
            return 0

        lax.fori_loop(0, -(-H // G), dx_step, 0)

        def b_to_inner(k, dev):
            return remote(pb.at[k], rb.at[k], s_os.at[k], s_tr.at[k], dev)

        def b_to_outer(k, dev):
            return remote(rb.at[k], mb.at[k], s_os.at[k], s_mr.at[k], dev)

        def b_step(i, _):
            k = n_a + i

            @pl.when(k < n_chunk)
            def _():
                part_up(k).wait_recv()

                @pl.when(jnp.logical_not(inner))
                def _():
                    b_to_inner(k, inner_dev).start()

                @pl.when(inner)
                def _():
                    b_to_inner(k, outer_dev).wait_recv()
                    pb[k] = pb[k] + rb[k]
                    to_mate(k).start()

            @pl.when(jnp.logical_and(inner, jnp.logical_and(i >= LAG, k < n_chunk + LAG)))
            def _():
                m = k - LAG
                to_mate(m).wait_recv()
                rb[m] = pb[m] + mb[m]
                b_to_outer(m, outer_dev).start()
                total_down(rb, m).start()

            @pl.when(jnp.logical_and(jnp.logical_not(inner), jnp.logical_and(i >= LAG_OUT, i < N_B + LAG_OUT)))
            def _():
                m = k - LAG_OUT
                b_to_outer(m, inner_dev).wait_recv()
                total_down(mb, m).start()

            return 0

        lax.fori_loop(0, N_B + LAG_OUT, b_step, 0)

        def b_done(k, _):
            total_down(rb, k).wait_send()

            @pl.when(jnp.logical_not(inner))
            def _():
                b_to_inner(k, inner_dev).wait_send()

            @pl.when(inner)
            def _():
                to_mate(k).wait_send()
                b_to_outer(k, outer_dev).wait_send()

            return 0

        lax.fori_loop(n_a, n_chunk, b_done, 0)

        def drain(h, _):
            for p in range(2):
                x_copy(h, p).wait_send()
            relay_out(h).wait_send()
            return 0

        lax.fori_loop(0, H, drain, 0)

        def drain_w(q, _):
            for y in range(3):
                w_unit(tp, q, y, 0, x_dev).wait_send()
                w_unit(tp, q, y, 1, c_dev).wait_send()
                w_unit(tp_x, q, y, 4, c_dev).wait_send()

                @pl.when(jnp.logical_and(zi < 3, q <= zi))
                def _():
                    w_unit(tp, q, y, 2, right_dev).wait_send()

                @pl.when(jnp.logical_and(zi > 0, q >= zi))
                def _():
                    w_unit(tp, q, y, 3, left_dev).wait_send()

            return 0

        lax.fori_loop(0, 4, drain_w, 0)

    @pl.when(st == 1)
    def _():
        w_loc = pltpu.make_async_copy(w_ref, wall.at[c], s_wl)
        w_core = remote(w_ref, wall.at[c], s_vs.at[2], s_vr.at[2], c_dev)
        vecs_l = [pltpu.make_async_copy(r, vec.at[k, c], s_vl.at[k]) for k, r in enumerate((gam_ref, bet_ref))]
        vecs_r = [remote(r, vec.at[k, c], s_vs.at[k], s_vr.at[k], c_dev) for k, r in enumerate((gam_ref, bet_ref))]
        dz_l = [pltpu.make_async_copy(dz_ref.at[:, :, 2 * s + c], dzb.at[s, c], s_dl.at[s]) for s in range(2)]
        dz_r = [remote(dz_ref.at[:, :, 2 * s + 1 - c], dzb.at[s, c], s_ds.at[s], s_dr.at[s], c_dev) for s in range(2)]

        part = pl.ds(pl.multiple_of(zi * quarter, quarter), quarter)
        w_y = [remote(w_ref.at[3 * y:3 * y + 3, part, :], wall.at[tp, 3 * y:3 * y + 3, part, :], s_ws.at[0, zi, y], s_wr.at[tp, zi, y], y_dev) for y in range(3)]

        for y in range(3):
            w_y[y].start()
        w_loc.start()
        w_core.start()
        for k in range(2):
            vecs_l[k].start()
            vecs_r[k].start()
            dz_l[k].start()
            dz_r[k].start()

        zero_borders(xe)
        zero_borders(ge)
        for buf in (xe, xo, ge, go):
            zero_planes(buf)

        def zero_acc(t, _):
            for k in range(2):
                acc[k, t] = jnp.zeros((CI, CO), F32)
            return 0

        lax.fori_loop(0, 9, zero_acc, 0)

        def zero_dx(h, _):
            dx_ref[h] = jnp.zeros((R, CI), BF16)
            return 0

        lax.fori_loop(0, H, zero_dx, 0)
        for k in range(2):
            vecs_l[k].wait()
            vecs_r[k].wait_recv()
            dz_l[k].wait()
            dz_r[k].wait_recv()
        w_loc.wait()
        w_core.wait_recv()

        def x_in(j, s, p):
            return remote(x_view(s, j, p), x_view(s, j, p), s_xf.at[p, j], s_xr.at[s, p, j], y_dev)

        def x_fwd(j, p):
            return remote(x_view(xi, j, p), x_view(xi, j, p), s_xf.at[p, j], s_xr.at[xi, p, j], x_dev)

        def g_own(h):
            return remote(ge.at[xi, h + 1, pl.ds(PAD, R), :], ge.at[xi, h + 1, pl.ds(PAD, R), :], s_gs.at[0, h], s_gr.at[xi, h], y_dev)

        def g_other(h):
            return remote(ge.at[1 - xi, h + 1, pl.ds(PAD, R), :], relay.at[h], s_gs.at[1, h], s_gl.at[h], y_dev)

        def x_relay(j):
            for p in range(2):
                x_in(j, xi, p).wait_recv()
                x_fwd(j, p).start()

        lax.fori_loop(0, AHEAD, lambda j, _: (x_relay(j), 0)[1], 0)

        def turn_x(q):
            rows = jnp.concatenate([xe[s, q + 1, PAD:PAD + 128, :] for s in range(2)], axis=0)
            xt[...] = rows.T

        def add_dw(q, t):
            rhs = jnp.concatenate([tap_rows(ge, go, s, q + 2 - t // 3, 1 - t % 3, 128) for s in range(2)], axis=0)
            prod = jnp.dot(xt[...], rhs, preferred_element_type=F32)
            for k in range(2):
                acc[k, t] += prod[:, k * CO:(k + 1) * CO]

        def step(j, _):
            @pl.when(j + AHEAD < H)
            def _():
                x_relay(j + AHEAD)

            @pl.when(j < H)
            def _():
                for p in range(2):
                    x_in(j, 1 - xi, p).wait_recv()
                for s in range(2):
                    odd_copy(xe, xo, s, j + 1)

            @pl.when(jnp.logical_and(j >= 1, j < H + 1))
            def _():
                h = j - 1
                pre = jnp.zeros((2 * R, CW), F32)
                for ky in range(3):
                    for kx in range(3):
                        t = 3 * ky + kx
                        lhs = jnp.concatenate([tap_rows(xe, xo, s, h + ky, kx - 1, R) for s in range(2)], axis=0)
                        rhs = jnp.concatenate([wall[0, t], wall[1, t]], axis=1)
                        pre = pre + jnp.dot(lhs, rhs, preferred_element_type=F32)
                for k in range(2):
                    gam = vec[0, k]
                    bet = vec[1, k]
                    for s in range(2):
                        y = pre[s * R:(s + 1) * R, k * CO:(k + 1) * CO] * gam + bet
                        zb[s, k, h] = jnp.maximum(y, 0.0).reshape(WD, 8, CO).astype(BF16)
                        dzr = dzb[s, k, h].astype(F32).reshape(R, CO)
                        ge[s, h + 1, PAD:PAD + R, k * CO:(k + 1) * CO] = jnp.where(y > 0, dzr * gam, 0.0).astype(BF16)
                g_own(h).start()
                g_other(h).start()
                for s in range(2):
                    odd_copy(ge, go, s, h + 1)
                    z_ref[h, :, 2 * s + c] = zb[s, c, h]

            @pl.when(j >= 2)
            def _():
                turn_x(j - 2)
                for t in range(9):
                    add_dw(j - 2, t)

            return 0

        lax.fori_loop(0, H + 1, step, 0)

        def pair(t):
            return remote(acc.at[1 - c, t], prx.at[t], s_ps.at[t], s_pr.at[t], c_dev)

        n_t = n_a // sub
        order = sorted(range(9), key=lambda t: 2 * (t - n_t) if t >= n_t else 2 * t + 1)
        turn_x(H - 1)
        for t in order:
            if t >= 3:
                add_dw(H - 1, t)
            pair(t).start()
        z_r = [remote(zb.at[s, 1 - c], z_ref.at[:, :, 2 * s + c], s_zs.at[s], s_zr.at[s], c_dev) for s in range(2)]
        z_w = [remote(zb.at[s, 1 - c], z_ref.at[:, :, 2 * s + 1 - c], s_zs.at[s], s_zr.at[s], c_dev) for s in range(2)]
        for s in range(2):
            z_r[s].start()

        def own_part(k, fresh):
            t = k // sub
            q = pl.multiple_of((k % sub) * piece, piece)

            @pl.when(fresh)
            def _():
                pair(t).wait_recv()

            return acc[c, t, pl.ds(q, piece), :] + prx[t, pl.ds(q, piece), :]

        def part_a(k):
            return own_part(k, jnp.logical_and(k % sub == 0, k // sub < n_a // sub))

        def send_b(i):
            @pl.when(i < N_B)
            def _():
                k = n_a + i
                pb[k] = own_part(k, jnp.logical_or(k % sub == 0, k == n_a))
                part_up(k).start()

        def to_inner(k):
            return remote(pb.at[k], rb.at[k], s_os.at[k], s_or.at[k], inner_dev)

        def from_outer(k):
            return remote(pb.at[k], rb.at[k], s_os.at[k], s_or.at[k], outer_dev)

        def to_outer(k):
            return remote(dw_view(k), dw_view(k), s_ts.at[k], s_tr.at[k], outer_dev)

        def from_inner(k):
            return remote(dw_view(k), dw_view(k), s_ts.at[k], s_tr.at[k], inner_dev)

        @pl.when(jnp.logical_not(inner))
        def _():
            def send(k, _):
                send_b(k)

                @pl.when(k < n_a)
                def _():
                    pb[k] = part_a(k)
                    to_inner(k).start()

                return 0

            lax.fori_loop(0, max(n_a, N_B), send, 0)

            def take(k, _):
                from_inner(k).wait_recv()
                to_inner(k).wait_send()
                return 0

            lax.fori_loop(0, n_a, take, 0)

        @pl.when(inner)
        def _():
            def both(k, _):
                for i in range(2):
                    send_b(2 * k + i)

                @pl.when(k < n_a)
                def _():
                    part = part_a(k)
                    from_outer(k).wait_recv()
                    pb[k] = part + rb[k]
                    to_mate(k).start()

                @pl.when(k >= LAG)
                def _():
                    m = k - LAG
                    to_mate(m).wait_recv()
                    dw_ref[m // sub, pl.ds(pl.multiple_of((m % sub) * piece, piece), piece), :] = pb[m] + mb[m]
                    to_outer(m).start()

                return 0

            lax.fori_loop(0, n_a + LAG, both, 0)

            def done(k, _):
                to_mate(k).wait_send()
                to_outer(k).wait_send()
                return 0

            lax.fori_loop(0, n_a, done, 0)

        def done_b(k, _):
            total_down(rb, k).wait_recv()
            part_up(k).wait_send()
            return 0

        lax.fori_loop(n_a, n_chunk, done_b, 0)

        def drain(h, _):
            for p in range(2):
                x_fwd(h, p).wait_send()
            g_own(h).wait_send()
            g_other(h).wait_send()
            return 0

        lax.fori_loop(0, H, drain, 0)

        def drain_w(t, _):
            pair(t).wait_send()
            return 0

        lax.fori_loop(0, 9, drain_w, 0)
        w_core.wait_send()
        for y in range(3):
            w_y[y].wait_send()
        for k in range(2):
            vecs_r[k].wait_send()
            dz_r[k].wait_send()
            z_r[k].wait_send()
            z_w[k].wait_recv()


def out_kernel(*refs):
    srcs, dsts, sem = refs[:3], refs[3:6], refs[6]
    copies = [pltpu.make_async_copy(a, b, sem.at[i]) for i, (a, b) in enumerate(zip(srcs, dsts))]
    for cp in copies:
        cp.start()
    for cp in copies:
        cp.wait()


def write_out(*arrays):
    return pl.pallas_call(
        out_kernel,
        out_shape=tuple(jax.ShapeDtypeStruct(a.shape, a.dtype) for a in arrays),
        in_specs=[pl.BlockSpec(memory_space=pltpu.VMEM)] * 3,
        out_specs=(pl.BlockSpec(memory_space=pl.ANY),) * 3,
        scratch_shapes=[pltpu.SemaphoreType.DMA((3,))],
        compiler_params=pltpu.CompilerParams(vmem_limit_bytes=16 * 1024 * 1024),
    )(*arrays)


def solution(mesh):
    act_spec = P('stage', ('dp', 'tp'))
    w_spec = P('stage', None, None, None, 'tp')
    vec_spec = P('stage', 'tp')
    chan_spec = P('stage', 'dp', None, None, 'tp')

    def device_step(act_in, w_conv, gamma_vec, beta_vec, z_grad):
        N, H, WD, CI = act_in.shape[1:]
        CO = w_conv.shape[-1]
        R = WD * N
        RP = 128 + 2 * PAD
        n_chunk = 72
        x = act_in[0].transpose(1, 2, 0, 3).reshape(H, R, CI)
        w = w_conv[0].reshape(9, CI, CO)
        dz = z_grad[0].transpose(1, 2, 0, 3).reshape(H, WD, 4, N, CO)
        dma = pltpu.SemaphoreType.DMA
        z, dx, dw = pl.pallas_call(
            functools.partial(block_kernel, H, WD, CI, CO, n_chunk),
            out_shape=(
                jax.ShapeDtypeStruct((H, WD, 4, N, CO), BF16),
                jax.ShapeDtypeStruct((H, R, CI), BF16),
                jax.ShapeDtypeStruct((9, CI, CO), F32),
            ),
            in_specs=[pl.BlockSpec(memory_space=pltpu.HBM)] * 5,
            out_specs=(pl.BlockSpec(memory_space=pltpu.VMEM),) * 3,
            scratch_shapes=[
                pltpu.VMEM((2, H + 2, RP, CI), BF16),
                pltpu.VMEM((2, H + 2, RP - 16, CI), BF16),
                pltpu.VMEM((2, H + 2, RP, 2 * CO), BF16),
                pltpu.VMEM((2, H + 2, RP - 16, 2 * CO), BF16),
                pltpu.VMEM((4, 9, CI, CO), BF16),
                pltpu.VMEM((2, 2, H, WD, N, CO), BF16),
                pltpu.VMEM((2, 2, H, WD, N, CO), BF16),
                pltpu.VMEM((2, 2, 1, CO), F32),
                pltpu.VMEM((2, 9, CI, CO), F32),
                pltpu.VMEM((9, CI, CO), F32),
                pltpu.VMEM((n_chunk, CI // 8, CO), F32),
                pltpu.VMEM((n_chunk, CI // 8, CO), F32),
                pltpu.VMEM((n_chunk, CI // 8, CO), F32),
                pltpu.VMEM((CI, 256), BF16),
                pltpu.VMEM((H, R, 2 * CO), BF16),
                dma((2, H)), dma((2, 2, H)), dma((2, H)), dma((2, H)), dma((2, H)), dma((H,)), dma((H,)),
                dma, dma((5, 4, 3)), dma((4, 4, 3)), dma((2,)), dma((3,)), dma((3,)), dma((2,)), dma((2,)), dma((2,)),
                dma((2,)), dma((2,)), dma((9,)), dma((9,)),
                *[dma((n_chunk,))] * 6,
            ],
            compiler_params=pltpu.CompilerParams(collective_id=0, has_side_effects=True, vmem_limit_bytes=46 * 1024 * 1024),
        )(*[pltpu.with_memory_space_constraint(a, pltpu.HBM) for a in (x, w, gamma_vec, beta_vec, dz)])
        z, dx, dw = write_out(z, dx, dw)
        z_full = z.reshape(H, WD, 4 * N, CO).transpose(2, 0, 1, 3)
        dx_full = dx.reshape(H, WD, N, CI).transpose(2, 0, 1, 3)
        dw_full = dw.reshape(3, 3, CI, CO)
        return z_full[None], dx_full[None], dw_full[None]

    return jax.shard_map(device_step, mesh=mesh, in_specs=(act_spec, w_spec, vec_spec, vec_spec, chan_spec), out_specs=(chan_spec, act_spec, w_spec), check_vma=False)
```

```python
import functools

import jax
import jax.numpy as jnp
from jax import lax
from jax.experimental import pallas as pl
from jax.experimental.pallas import tpu as pltpu
from jax.sharding import PartitionSpec as P

MESH = pl.DeviceIdType.MESH
F32 = jnp.float32
BF16 = jnp.bfloat16
PAD = 16
AHEAD = 2
LAG = 1
LAG_OUT = 3
CHUNKS_A = ((0, 0, 1), (0, 1, 1), (0, 2, 2), (1, 0, 4), (2, 0, 4), (3, 0, 4), (4, 0, 2), (4, 2, 1), (4, 3, 1))
CHUNKS_B = ((5, 0, 1), (5, 1, 1), (5, 2, 2), (6, 0, 4), (7, 0, 4), (8, 0, 2), (8, 2, 1), (8, 3, 1))
CHUNKS = CHUNKS_A + CHUNKS_B
N_A, N_B = len(CHUNKS_A), len(CHUNKS_B)


def remote(src, dst, send_sem, recv_sem, dev):
    return pltpu.make_async_remote_copy(src_ref=src, dst_ref=dst, send_sem=send_sem, recv_sem=recv_sem, device_id=dev, device_id_type=MESH)


def block_kernel(H, WD, CI, CO, x_ref, w_ref, gam_ref, bet_ref, dz_ref, z_ref, dx_ref, dw_ref,
                 xe, xo, ge, go, wall, dzb, zb, vec, acc, prx, pb, rb, mb, xt, relay, *sems):
    (s_xs, s_xr, s_xf, s_gs, s_gr, s_gl, s_gf, s_wl, s_ws, s_wr, s_vl, s_vs, s_vr, s_dl, s_ds, s_dr,
     s_zs, s_zr, s_ps, s_pr, s_os, s_or, s_ms, s_mr, s_ts, s_tr) = sems
    R = WD * 8
    quarter = CI // 4
    n_blk = min(CI, 256)
    CW = 2 * CO
    zi = lax.axis_index("dp")
    st = lax.axis_index("stage")
    tp = lax.axis_index("tp")
    xi = tp // 2
    c = tp % 2
    y_dev = (zi, 1 - st, tp)
    x_dev = (zi, st, 2 * (1 - xi) + c)
    c_dev = (zi, st, 2 * xi + 1 - c)
    z_mate = jnp.where(zi == 1, 2, 1)
    z_out = jnp.where(zi < 2, 0, 3)
    z_in = jnp.where(zi < 2, 1, 2)
    inner = jnp.logical_or(zi == 1, zi == 2)
    mate_dev = (z_mate, st, tp)
    outer_dev = (z_out, st, tp)
    inner_dev = (z_in, st, tp)

    barrier = pltpu.get_barrier_semaphore()
    for dev in (y_dev, x_dev, c_dev):
        pl.semaphore_signal(barrier, inc=1, device_id=dev, device_id_type=MESH)

    @pl.when(inner)
    def _():
        for dev in (mate_dev, outer_dev):
            pl.semaphore_signal(barrier, inc=1, device_id=dev, device_id_type=MESH)
        pl.semaphore_wait(barrier, 5)

    @pl.when(jnp.logical_not(inner))
    def _():
        pl.semaphore_signal(barrier, inc=1, device_id=inner_dev, device_id_type=MESH)
        pl.semaphore_wait(barrier, 4)

    def zero_borders(buf):
        ch = buf.shape[-1]

        def rows(h, _):
            for s in range(2):
                buf[s, h, 0:PAD, :] = jnp.zeros((PAD, ch), BF16)
                buf[s, h, PAD + R:, :] = jnp.zeros((buf.shape[2] - PAD - R, ch), BF16)
            return 0

        lax.fori_loop(0, H + 2, rows, 0)

    def zero_planes(buf):
        for s in range(2):
            for h in (0, H + 1):
                buf[s, h] = jnp.zeros(buf.shape[2:], BF16)

    def odd_copy(even, odd, s, h):
        n = odd.shape[2]
        odd[s, h] = even[s, h, 8:8 + n, :]

    def tap_rows(even, odd, s, plane, shift, n):
        if shift == 0:
            return even[s, plane, PAD:PAD + n, :]
        start = PAD + 8 * shift - 8
        return odd[s, plane, start:start + n, :]

    x_cut = ((0, R),)

    def x_view(s, h, p):
        return xe.at[s, h + 1, pl.ds(PAD + x_cut[p][0], x_cut[p][1]), :]

    def place(k):
        t, q0, nq = CHUNKS[k]
        return t, slice(q0 * quarter, (q0 + nq) * quarter)

    def cut(buf, k):
        t, rows = place(k)
        return buf.at[t, rows, :]

    def value(buf, k):
        t, rows = place(k)
        return buf[t, rows, :]

    def put(buf, k, val):
        t, rows = place(k)
        buf[t, rows, :] = val

    def part_up(k):
        return remote(cut(pb, k), cut(pb, k), s_os.at[k], s_or.at[k], y_dev)

    def to_mate(k):
        return remote(cut(pb, k), cut(mb, k), s_ms.at[k], s_mr.at[k], mate_dev)

    def total_down(src, k):
        return remote(cut(src, k), cut(dw_ref, k), s_ts.at[k], s_tr.at[k], y_dev)

    @pl.when(st == 0)
    def _():
        def x_copy(h, p):
            return remote(x_ref.at[h, pl.ds(*x_cut[p]), :], x_view(xi, h, p), s_xs.at[p, h], s_xr.at[xi, p, h], y_dev)

        def x_send(h, _):
            for p in range(len(x_cut)):
                x_copy(h, p).start()
            return 0

        lax.fori_loop(0, H, x_send, 0)
        zero_borders(ge)
        zero_planes(ge)
        zero_planes(go)

        def zero_out(h, _):
            z_ref[h] = jnp.zeros(z_ref.shape[1:], BF16)
            return 0

        lax.fori_loop(0, H, zero_out, 0)

        def zero_dw(t, _):
            dw_ref[t] = jnp.zeros((CI, CO), F32)
            return 0

        lax.fori_loop(0, 9, zero_dw, 0)

        def g_in(j, b):
            return remote(ge.at[b, j + 1, pl.ds(PAD, R), :], ge.at[b, j + 1, pl.ds(PAD, R), :], s_gf.at[j], s_gr.at[b, j], x_dev)

        def relay_in(j):
            return remote(relay.at[:, j], relay.at[:, j], s_gf.at[j], s_gl.at[j], y_dev)

        def relay_out(j):
            return remote(relay.at[1 - xi, j], ge.at[xi, j + 1, pl.ds(PAD, R), :], s_gf.at[j], s_gr.at[xi, j], x_dev)

        def g_relay(j):
            relay_in(j).wait_recv()
            relay_out(j).start()
            ge[xi, j + 1, PAD:PAD + R, :] = relay[xi, j]

        def relay_rows(lo, hi):
            lax.fori_loop(lo, min(hi, H), lambda j, _: (g_relay(j), 0)[1], 0)

        tp_x = 2 * (1 - xi) + c
        left_dev = (jnp.maximum(zi - 1, 0), st, tp)
        right_dev = (jnp.minimum(zi + 1, 3), st, tp)

        def w_unit(b, q, y, kind, dev):
            view = wall.at[b, pl.ds(3 * y, 3), pl.ds(pl.multiple_of(q * quarter, quarter), quarter), :]
            return remote(view, view, s_ws.at[kind, q, y], s_wr.at[b, q, y], dev)

        def w_got(q, go_right, go_left):
            def take(y, _):
                w_unit(tp, q, y, 0, y_dev).wait_recv()
                if go_right:
                    @pl.when(zi < 3)
                    def _():
                        w_unit(tp, q, y, 2, right_dev).start()
                if go_left:
                    @pl.when(zi > 0)
                    def _():
                        w_unit(tp, q, y, 3, left_dev).start()
                w_unit(tp, q, y, 0, x_dev).start()
                w_unit(tp, q, y, 1, c_dev).start()
                return 0

            lax.fori_loop(0, 3, take, 0)

        w_got(zi, True, True)
        for d in range(1, 4):
            @pl.when(zi - d >= 0)
            def _():
                w_got(zi - d, True, False)

            @pl.when(zi + d <= 3)
            def _():
                w_got(zi + d, False, True)

            relay_rows(2 * (d - 1), 2 * d)

        def w_cross(q, _):
            for y in range(3):
                w_unit(tp_x, q, y, 4, x_dev).wait_recv()
                w_unit(tp_x, q, y, 4, c_dev).start()
            return 0

        relay_rows(6, 9)
        lax.fori_loop(0, 4, w_cross, 0)
        relay_rows(9, H)

        def w_all(q, _):
            for y in range(3):
                for b in (2 * xi + 1 - c, 2 * (1 - xi) + 1 - c):
                    w_unit(b, q, y, 1, c_dev).wait_recv()
            return 0

        lax.fori_loop(0, 4, w_all, 0)

        G = 4

        def g_take(j, _):
            g_in(j, 1 - xi).wait_recv()
            for b in range(2):
                odd_copy(ge, go, b, j + 1)
            return 0

        def dx_rows(h0):
            for n in range(CI // n_blk):
                tot = jnp.zeros((G * R, n_blk), F32)
                for b in range(2):
                    for t in range(9):
                        lhs = jnp.concatenate([tap_rows(ge, go, b, h0 + r + 2 - t // 3, 1 - t % 3, R) for r in range(G)], axis=0)
                        rhs = jnp.concatenate([wall[2 * b + i, t, n * n_blk:(n + 1) * n_blk, :] for i in range(2)], axis=1)
                        tot = tot + lax.dot_general(lhs, rhs, (((1,), (1,)), ((), ())), preferred_element_type=F32)
                for r in range(G):
                    dx_ref[h0 + r, :, n * n_blk:(n + 1) * n_blk] = tot[r * R:(r + 1) * R].astype(BF16)

        def dx_step(i):
            @pl.when(i >= 0)
            def _():
                lo = jnp.where(i == 0, 0, G * i + 1)
                lax.fori_loop(lo, jnp.minimum(G * i + G + 1, H), g_take, 0)
                dx_rows(jnp.minimum(G * i, H - G))

        def b_to_inner(k, dev):
            return remote(cut(pb, k), cut(rb, k), s_os.at[k], s_tr.at[k], dev)

        def b_to_outer(k, dev):
            return remote(cut(rb, k), cut(mb, k), s_os.at[k], s_mr.at[k], dev)

        def b_up(k):
            part_up(k).wait_recv()

            @pl.when(jnp.logical_not(inner))
            def _():
                b_to_inner(k, inner_dev).start()

            @pl.when(inner)
            def _():
                b_to_inner(k, outer_dev).wait_recv()
                put(pb, k, value(pb, k) + value(rb, k))
                to_mate(k).start()

        def b_total(k):
            to_mate(k).wait_recv()
            put(rb, k, value(pb, k) + value(mb, k))
            b_to_outer(k, outer_dev).start()
            total_down(rb, k).start()

        def b_down(k):
            b_to_outer(k, inner_dev).wait_recv()
            total_down(mb, k).start()

        n_g = -(-H // G)
        slots = N_A + N_B

        def dx_loop(lo, hi):
            lax.fori_loop(min(lo, n_g), min(hi, n_g), lambda i, _: (dx_step(i), 0)[1], 0)

        def b_some(lo, hi):
            for k in range(lo, hi):
                b_up(k)

                @pl.when(inner)
                def _():
                    if k - LAG >= N_A:
                        b_total(k - LAG)

                @pl.when(jnp.logical_not(inner))
                def _():
                    if k - LAG_OUT >= N_A:
                        b_down(k - LAG_OUT)

        b_some(N_A, N_A + 3)

        def dx_between(i, _):
            for m in range(3):
                @pl.when(i == m)
                def _():
                    b_some(N_A + 3 + m, N_A + 4 + m)

            dx_step(i)
            return 0

        lax.fori_loop(0, n_g, dx_between, 0)
        if n_g < 3:
            b_some(N_A + 3 + n_g, N_A + 6)
        b_some(N_A + 6, slots)

        @pl.when(inner)
        def _():
            for k in range(slots - LAG, slots):
                b_total(k)

        @pl.when(jnp.logical_not(inner))
        def _():
            for k in range(slots - LAG_OUT, slots):
                b_down(k)

        for k in range(N_A, slots):
            total_down(rb, k).wait_send()

            @pl.when(jnp.logical_not(inner))
            def _():
                b_to_inner(k, inner_dev).wait_send()

            @pl.when(inner)
            def _():
                to_mate(k).wait_send()
                b_to_outer(k, outer_dev).wait_send()

        def drain(h, _):
            for p in range(len(x_cut)):
                x_copy(h, p).wait_send()
            relay_out(h).wait_send()
            return 0

        lax.fori_loop(0, H, drain, 0)

        def drain_w(q, _):
            for y in range(3):
                w_unit(tp, q, y, 0, x_dev).wait_send()
                w_unit(tp, q, y, 1, c_dev).wait_send()
                w_unit(tp_x, q, y, 4, c_dev).wait_send()

                @pl.when(jnp.logical_and(zi < 3, q <= zi))
                def _():
                    w_unit(tp, q, y, 2, right_dev).wait_send()

                @pl.when(jnp.logical_and(zi > 0, q >= zi))
                def _():
                    w_unit(tp, q, y, 3, left_dev).wait_send()

            return 0

        lax.fori_loop(0, 4, drain_w, 0)

    @pl.when(st == 1)
    def _():
        w_loc = pltpu.make_async_copy(w_ref, wall.at[c], s_wl)
        w_core = remote(w_ref, wall.at[c], s_vs.at[2], s_vr.at[2], c_dev)
        vecs_l = [pltpu.make_async_copy(r, vec.at[k, c], s_vl.at[k]) for k, r in enumerate((gam_ref, bet_ref))]
        vecs_r = [remote(r, vec.at[k, c], s_vs.at[k], s_vr.at[k], c_dev) for k, r in enumerate((gam_ref, bet_ref))]
        dz_l = [pltpu.make_async_copy(dz_ref.at[:, :, 2 * s + c], dzb.at[s, c], s_dl.at[s]) for s in range(2)]
        dz_r = [remote(dz_ref.at[:, :, 2 * s + 1 - c], dzb.at[s, c], s_ds.at[s], s_dr.at[s], c_dev) for s in range(2)]

        part = pl.ds(pl.multiple_of(zi * quarter, quarter), quarter)
        w_y = [remote(w_ref.at[3 * y:3 * y + 3, part, :], wall.at[tp, 3 * y:3 * y + 3, part, :], s_ws.at[0, zi, y], s_wr.at[tp, zi, y], y_dev) for y in range(3)]

        for y in range(3):
            w_y[y].start()
        w_loc.start()
        w_core.start()
        for k in range(2):
            vecs_l[k].start()
            vecs_r[k].start()
            dz_l[k].start()
            dz_r[k].start()

        zero_borders(xe)
        zero_borders(ge)
        for buf in (xe, xo, ge, go):
            zero_planes(buf)

        def zero_acc(t, _):
            for k in range(2):
                acc[k, t] = jnp.zeros((CI, CO), F32)
            return 0

        lax.fori_loop(0, 9, zero_acc, 0)

        def zero_dx(h, _):
            dx_ref[h] = jnp.zeros((R, CI), BF16)
            return 0

        lax.fori_loop(0, H, zero_dx, 0)
        for k in range(2):
            vecs_l[k].wait()
            vecs_r[k].wait_recv()
            dz_l[k].wait()
            dz_r[k].wait_recv()
        w_loc.wait()
        w_core.wait_recv()

        def x_in(j, s, p):
            return remote(x_view(s, j, p), x_view(s, j, p), s_xf.at[p, j], s_xr.at[s, p, j], y_dev)

        def x_fwd(j, p):
            return remote(x_view(xi, j, p), x_view(xi, j, p), s_xf.at[p, j], s_xr.at[xi, p, j], x_dev)

        def g_send(h):
            return remote(ge.at[:, h + 1, pl.ds(PAD, R), :], relay.at[:, h], s_gs.at[h], s_gl.at[h], y_dev)

        def x_relay(j):
            for p in range(len(x_cut)):
                x_in(j, xi, p).wait_recv()
                x_fwd(j, p).start()

        lax.fori_loop(0, AHEAD, lambda j, _: (x_relay(j), 0)[1], 0)

        def turn_x(q):
            rows = jnp.concatenate([xe[s, q + 1, PAD:PAD + 128, :] for s in range(2)], axis=0)
            xt[...] = rows.T

        def add_dw(q, t):
            rhs = jnp.concatenate([tap_rows(ge, go, s, q + 2 - t // 3, 1 - t % 3, 128) for s in range(2)], axis=0)
            prod = jnp.dot(xt[...], rhs, preferred_element_type=F32)
            for k in range(2):
                acc[k, t] += prod[:, k * CO:(k + 1) * CO]

        def step(j, _):
            @pl.when(j + AHEAD < H)
            def _():
                x_relay(j + AHEAD)

            @pl.when(j < H)
            def _():
                for p in range(len(x_cut)):
                    x_in(j, 1 - xi, p).wait_recv()
                for s in range(2):
                    odd_copy(xe, xo, s, j + 1)

            @pl.when(jnp.logical_and(j >= 1, j < H + 1))
            def _():
                h = j - 1
                pre = jnp.zeros((2 * R, CW), F32)
                for ky in range(3):
                    for kx in range(3):
                        t = 3 * ky + kx
                        lhs = jnp.concatenate([tap_rows(xe, xo, s, h + ky, kx - 1, R) for s in range(2)], axis=0)
                        rhs = jnp.concatenate([wall[0, t], wall[1, t]], axis=1)
                        pre = pre + jnp.dot(lhs, rhs, preferred_element_type=F32)
                for k in range(2):
                    gam = vec[0, k]
                    bet = vec[1, k]
                    for s in range(2):
                        y = pre[s * R:(s + 1) * R, k * CO:(k + 1) * CO] * gam + bet
                        zb[s, k, h] = jnp.maximum(y, 0.0).reshape(WD, 8, CO).astype(BF16)
                        dzr = dzb[s, k, h].astype(F32).reshape(R, CO)
                        ge[s, h + 1, PAD:PAD + R, k * CO:(k + 1) * CO] = jnp.where(y > 0, dzr * gam, 0.0).astype(BF16)
                g_send(h).start()
                for s in range(2):
                    odd_copy(ge, go, s, h + 1)
                    z_ref[h, :, 2 * s + c] = zb[s, c, h]

            @pl.when(j >= 2)
            def _():
                turn_x(j - 2)
                for t in range(9):
                    add_dw(j - 2, t)

            return 0

        lax.fori_loop(0, H + 1, step, 0)

        def pair(t):
            return remote(acc.at[1 - c, t], prx.at[t], s_ps.at[t], s_pr.at[t], c_dev)

        n_t = CHUNKS_B[0][0]
        order = sorted(range(9), key=lambda t: 2 * (t - n_t) if t >= n_t else 2 * t + 1)
        turn_x(H - 1)
        for t in order:
            if t >= 3:
                add_dw(H - 1, t)
            pair(t).start()
        z_r = [remote(zb.at[s, 1 - c], z_ref.at[:, :, 2 * s + c], s_zs.at[s], s_zr.at[s], c_dev) for s in range(2)]
        z_w = [remote(zb.at[s, 1 - c], z_ref.at[:, :, 2 * s + 1 - c], s_zs.at[s], s_zr.at[s], c_dev) for s in range(2)]
        for s in range(2):
            z_r[s].start()

        def own_part(k):
            t, rows = place(k)
            if rows.start == 0:
                pair(t).wait_recv()
            return acc[c, t, rows, :] + prx[t, rows, :]

        def send_b(i):
            if i < N_B:
                put(pb, N_A + i, own_part(N_A + i))
                part_up(N_A + i).start()

        def to_inner(k):
            return remote(cut(pb, k), cut(rb, k), s_os.at[k], s_or.at[k], inner_dev)

        def from_outer(k):
            return remote(cut(pb, k), cut(rb, k), s_os.at[k], s_or.at[k], outer_dev)

        def to_outer(k):
            return remote(cut(dw_ref, k), cut(dw_ref, k), s_ts.at[k], s_tr.at[k], outer_dev)

        def from_inner(k):
            return remote(cut(dw_ref, k), cut(dw_ref, k), s_ts.at[k], s_tr.at[k], inner_dev)

        @pl.when(jnp.logical_not(inner))
        def _():
            for k in range(max(N_A, N_B)):
                send_b(k)
                if k < N_A:
                    put(pb, k, own_part(k))
                    to_inner(k).start()
            for k in range(N_A):
                from_inner(k).wait_recv()
                to_inner(k).wait_send()

        @pl.when(inner)
        def _():
            send_b(0)
            for k in range(max(N_A + LAG, N_B)):
                send_b(k + 1)
                if k < N_A:
                    part = own_part(k)
                    from_outer(k).wait_recv()
                    put(pb, k, part + value(rb, k))
                    to_mate(k).start()
                m = k - LAG
                if 0 <= m < N_A:
                    to_mate(m).wait_recv()
                    put(dw_ref, m, value(pb, m) + value(mb, m))
                    to_outer(m).start()
            for k in range(N_A):
                to_mate(k).wait_send()
                to_outer(k).wait_send()

        for k in range(N_A, N_A + N_B):
            total_down(rb, k).wait_recv()
            part_up(k).wait_send()

        def drain(h, _):
            for p in range(len(x_cut)):
                x_fwd(h, p).wait_send()
            g_send(h).wait_send()
            return 0

        lax.fori_loop(0, H, drain, 0)

        def drain_w(t, _):
            pair(t).wait_send()
            return 0

        lax.fori_loop(0, 9, drain_w, 0)
        w_core.wait_send()
        for y in range(3):
            w_y[y].wait_send()
        for k in range(2):
            vecs_r[k].wait_send()
            dz_r[k].wait_send()
            z_r[k].wait_send()
            z_w[k].wait_recv()


def out_kernel(*refs):
    srcs, dsts, sem = refs[:3], refs[3:6], refs[6]
    copies = [pltpu.make_async_copy(a, b, sem.at[i]) for i, (a, b) in enumerate(zip(srcs, dsts))]
    for cp in copies:
        cp.start()
    for cp in copies:
        cp.wait()


def write_out(*arrays):
    return pl.pallas_call(
        out_kernel,
        out_shape=tuple(jax.ShapeDtypeStruct(a.shape, a.dtype) for a in arrays),
        in_specs=[pl.BlockSpec(memory_space=pltpu.VMEM)] * 3,
        out_specs=(pl.BlockSpec(memory_space=pl.ANY),) * 3,
        scratch_shapes=[pltpu.SemaphoreType.DMA((3,))],
        compiler_params=pltpu.CompilerParams(vmem_limit_bytes=16 * 1024 * 1024),
    )(*arrays)


def solution(mesh):
    act_spec = P('stage', ('dp', 'tp'))
    w_spec = P('stage', None, None, None, 'tp')
    vec_spec = P('stage', 'tp')
    chan_spec = P('stage', 'dp', None, None, 'tp')

    def device_step(act_in, w_conv, gamma_vec, beta_vec, z_grad):
        N, H, WD, CI = act_in.shape[1:]
        CO = w_conv.shape[-1]
        R = WD * N
        RP = 128 + 2 * PAD
        x = act_in[0].transpose(1, 2, 0, 3).reshape(H, R, CI)
        w = w_conv[0].reshape(9, CI, CO)
        dz = z_grad[0].transpose(1, 2, 0, 3).reshape(H, WD, 4, N, CO)
        dma = pltpu.SemaphoreType.DMA
        z, dx, dw = pl.pallas_call(
            functools.partial(block_kernel, H, WD, CI, CO),
            out_shape=(
                jax.ShapeDtypeStruct((H, WD, 4, N, CO), BF16),
                jax.ShapeDtypeStruct((H, R, CI), BF16),
                jax.ShapeDtypeStruct((9, CI, CO), F32),
            ),
            in_specs=[pl.BlockSpec(memory_space=pltpu.HBM)] * 5,
            out_specs=(pl.BlockSpec(memory_space=pltpu.VMEM),) * 3,
            scratch_shapes=[
                pltpu.VMEM((2, H + 2, RP, CI), BF16),
                pltpu.VMEM((2, H + 2, RP - 16, CI), BF16),
                pltpu.VMEM((2, H + 2, RP, 2 * CO), BF16),
                pltpu.VMEM((2, H + 2, RP - 16, 2 * CO), BF16),
                pltpu.VMEM((4, 9, CI, CO), BF16),
                pltpu.VMEM((2, 2, H, WD, N, CO), BF16),
                pltpu.VMEM((2, 2, H, WD, N, CO), BF16),
                pltpu.VMEM((2, 2, 1, CO), F32),
                pltpu.VMEM((2, 9, CI, CO), F32),
                pltpu.VMEM((9, CI, CO), F32),
                pltpu.VMEM((9, CI, CO), F32),
                pltpu.VMEM((9, CI, CO), F32),
                pltpu.VMEM((9, CI, CO), F32),
                pltpu.VMEM((CI, 256), BF16),
                pltpu.VMEM((2, H, R, 2 * CO), BF16),
                dma((1, H)), dma((2, 1, H)), dma((1, H)), dma((H,)), dma((2, H)), dma((H,)), dma((H,)),
                dma, dma((5, 4, 3)), dma((4, 4, 3)), dma((2,)), dma((3,)), dma((3,)), dma((2,)), dma((2,)), dma((2,)),
                dma((2,)), dma((2,)), dma((9,)), dma((9,)),
                *[dma((N_A + N_B,))] * 6,
            ],
            compiler_params=pltpu.CompilerParams(collective_id=0, has_side_effects=True, vmem_limit_bytes=46 * 1024 * 1024),
        )(*[pltpu.with_memory_space_constraint(a, pltpu.HBM) for a in (x, w, gamma_vec, beta_vec, dz)])
        z, dx, dw = write_out(z, dx, dw)
        z_full = z.reshape(H, WD, 4 * N, CO).transpose(2, 0, 1, 3)
        dx_full = dx.reshape(H, WD, N, CI).transpose(2, 0, 1, 3)
        dw_full = dw.reshape(3, 3, CI, CO)
        return z_full[None], dx_full[None], dw_full[None]

    return jax.shard_map(device_step, mesh=mesh, in_specs=(act_spec, w_spec, vec_spec, vec_spec, chan_spec), out_specs=(chan_spec, act_spec, w_spec), check_vma=False)
```

```python
import functools

import jax
import jax.numpy as jnp
from jax import lax
from jax.experimental import pallas as pl
from jax.experimental.pallas import tpu as pltpu
from jax.sharding import PartitionSpec as P

MESH = pl.DeviceIdType.MESH
F32 = jnp.float32
BF16 = jnp.bfloat16
PAD = 16
AHEAD = 2
LAG = 3
LAG_OUT = 8
N_B = 14
CHUNKS = tuple((t, q, 1) for t in range(9) for q in range(4))
N_A = len(CHUNKS) - N_B


def remote(src, dst, send_sem, recv_sem, dev):
    return pltpu.make_async_remote_copy(src_ref=src, dst_ref=dst, send_sem=send_sem, recv_sem=recv_sem, device_id=dev, device_id_type=MESH)


def block_kernel(H, WD, CI, CO, x_ref, w_ref, gam_ref, bet_ref, dz_ref, z_ref, dx_ref, dw_ref,
                 xe, xo, ge, go, wall, dzb, zb, vec, acc, prx, pb, rb, mb, xt, relay, *sems):
    (s_xs, s_xr, s_xf, s_gs, s_gr, s_gl, s_gf, s_wl, s_ws, s_wr, s_vl, s_vs, s_vr, s_dl, s_ds, s_dr,
     s_zs, s_zr, s_ps, s_pr, s_os, s_or, s_ms, s_mr, s_ts, s_tr) = sems
    R = WD * 8
    quarter = CI // 4
    n_blk = min(CI, 256)
    CW = 2 * CO
    zi = lax.axis_index("dp")
    st = lax.axis_index("stage")
    tp = lax.axis_index("tp")
    xi = tp // 2
    c = tp % 2
    y_dev = (zi, 1 - st, tp)
    x_dev = (zi, st, 2 * (1 - xi) + c)
    c_dev = (zi, st, 2 * xi + 1 - c)
    z_mate = jnp.where(zi == 1, 2, 1)
    z_out = jnp.where(zi < 2, 0, 3)
    z_in = jnp.where(zi < 2, 1, 2)
    inner = jnp.logical_or(zi == 1, zi == 2)
    mate_dev = (z_mate, st, tp)
    outer_dev = (z_out, st, tp)
    inner_dev = (z_in, st, tp)

    barrier = pltpu.get_barrier_semaphore()
    for dev in (y_dev, x_dev, c_dev):
        pl.semaphore_signal(barrier, inc=1, device_id=dev, device_id_type=MESH)

    @pl.when(inner)
    def _():
        for dev in (mate_dev, outer_dev):
            pl.semaphore_signal(barrier, inc=1, device_id=dev, device_id_type=MESH)
        pl.semaphore_wait(barrier, 5)

    @pl.when(jnp.logical_not(inner))
    def _():
        pl.semaphore_signal(barrier, inc=1, device_id=inner_dev, device_id_type=MESH)
        pl.semaphore_wait(barrier, 4)

    def zero_borders(buf):
        ch = buf.shape[-1]

        def rows(h, _):
            for s in range(2):
                buf[s, h, 0:PAD, :] = jnp.zeros((PAD, ch), BF16)
                buf[s, h, PAD + R:, :] = jnp.zeros((buf.shape[2] - PAD - R, ch), BF16)
            return 0

        lax.fori_loop(0, H + 2, rows, 0)

    def zero_planes(buf):
        for s in range(2):
            for h in (0, H + 1):
                buf[s, h] = jnp.zeros(buf.shape[2:], BF16)

    def odd_copy(even, odd, s, h):
        n = odd.shape[2]
        odd[s, h] = even[s, h, 8:8 + n, :]

    def tap_rows(even, odd, s, plane, shift, n):
        if shift == 0:
            return even[s, plane, PAD:PAD + n, :]
        start = PAD + 8 * shift - 8
        return odd[s, plane, start:start + n, :]

    x_cut = ((0, R),)

    def x_view(s, h, p):
        return xe.at[s, h + 1, pl.ds(PAD + x_cut[p][0], x_cut[p][1]), :]

    def place(k):
        t, q0, nq = CHUNKS[k]
        return t, slice(q0 * quarter, (q0 + nq) * quarter)

    def cut(buf, k):
        t, rows = place(k)
        return buf.at[t, rows, :]

    def value(buf, k):
        t, rows = place(k)
        return buf[t, rows, :]

    def put(buf, k, val):
        t, rows = place(k)
        buf[t, rows, :] = val

    def part_up(k):
        return remote(cut(pb, k), cut(pb, k), s_os.at[k], s_or.at[k], y_dev)

    def to_mate(k):
        return remote(cut(pb, k), cut(mb, k), s_ms.at[k], s_mr.at[k], mate_dev)

    def total_down(src, k):
        return remote(cut(src, k), cut(dw_ref, k), s_ts.at[k], s_tr.at[k], y_dev)

    @pl.when(st == 0)
    def _():
        def x_copy(h, p):
            return remote(x_ref.at[h, pl.ds(*x_cut[p]), :], x_view(xi, h, p), s_xs.at[p, h], s_xr.at[xi, p, h], y_dev)

        def x_send(h, _):
            for p in range(len(x_cut)):
                x_copy(h, p).start()
            return 0

        lax.fori_loop(0, H, x_send, 0)
        zero_borders(ge)
        zero_planes(ge)
        zero_planes(go)

        def zero_out(h, _):
            z_ref[h] = jnp.zeros(z_ref.shape[1:], BF16)
            return 0

        lax.fori_loop(0, H, zero_out, 0)

        def zero_dw(t, _):
            dw_ref[t] = jnp.zeros((CI, CO), F32)
            return 0

        lax.fori_loop(0, 9, zero_dw, 0)

        def g_in(j, b):
            return remote(ge.at[b, j + 1, pl.ds(PAD, R), :], ge.at[b, j + 1, pl.ds(PAD, R), :], s_gf.at[j], s_gr.at[b, j], x_dev)

        def relay_in(j):
            return remote(relay.at[:, j], relay.at[:, j], s_gf.at[j], s_gl.at[j], y_dev)

        def relay_out(j):
            return remote(relay.at[1 - xi, j], ge.at[xi, j + 1, pl.ds(PAD, R), :], s_gf.at[j], s_gr.at[xi, j], x_dev)

        def g_relay(j):
            relay_in(j).wait_recv()
            relay_out(j).start()
            ge[xi, j + 1, PAD:PAD + R, :] = relay[xi, j]

        def relay_rows(lo, hi):
            lax.fori_loop(lo, min(hi, H), lambda j, _: (g_relay(j), 0)[1], 0)

        tp_x = 2 * (1 - xi) + c
        left_dev = (jnp.maximum(zi - 1, 0), st, tp)
        right_dev = (jnp.minimum(zi + 1, 3), st, tp)

        def w_unit(b, q, y, kind, dev):
            view = wall.at[b, pl.ds(3 * y, 3), pl.ds(pl.multiple_of(q * quarter, quarter), quarter), :]
            return remote(view, view, s_ws.at[kind, q, y], s_wr.at[b, q, y], dev)

        def w_got(q, go_right, go_left):
            def take(y, _):
                w_unit(tp, q, y, 0, y_dev).wait_recv()
                if go_right:
                    @pl.when(zi < 3)
                    def _():
                        w_unit(tp, q, y, 2, right_dev).start()
                if go_left:
                    @pl.when(zi > 0)
                    def _():
                        w_unit(tp, q, y, 3, left_dev).start()
                w_unit(tp, q, y, 0, x_dev).start()
                w_unit(tp, q, y, 1, c_dev).start()
                return 0

            lax.fori_loop(0, 3, take, 0)

        w_got(zi, True, True)
        for d in range(1, 4):
            @pl.when(zi - d >= 0)
            def _():
                w_got(zi - d, True, False)

            @pl.when(zi + d <= 3)
            def _():
                w_got(zi + d, False, True)

            relay_rows(2 * (d - 1), 2 * d)

        def w_cross(q, _):
            for y in range(3):
                w_unit(tp_x, q, y, 4, x_dev).wait_recv()
                w_unit(tp_x, q, y, 4, c_dev).start()
            return 0

        relay_rows(6, 9)
        lax.fori_loop(0, 4, w_cross, 0)
        relay_rows(9, H)

        def w_all(q, _):
            for y in range(3):
                for b in (2 * xi + 1 - c, 2 * (1 - xi) + 1 - c):
                    w_unit(b, q, y, 1, c_dev).wait_recv()
            return 0

        lax.fori_loop(0, 4, w_all, 0)

        G = 4

        def g_take(j, _):
            g_in(j, 1 - xi).wait_recv()
            for b in range(2):
                odd_copy(ge, go, b, j + 1)
            return 0

        def dx_rows(h0):
            for n in range(CI // n_blk):
                tot = jnp.zeros((G * R, n_blk), F32)
                for b in range(2):
                    for t in range(9):
                        lhs = jnp.concatenate([tap_rows(ge, go, b, h0 + r + 2 - t // 3, 1 - t % 3, R) for r in range(G)], axis=0)
                        rhs = jnp.concatenate([wall[2 * b + i, t, n * n_blk:(n + 1) * n_blk, :] for i in range(2)], axis=1)
                        tot = tot + lax.dot_general(lhs, rhs, (((1,), (1,)), ((), ())), preferred_element_type=F32)
                for r in range(G):
                    dx_ref[h0 + r, :, n * n_blk:(n + 1) * n_blk] = tot[r * R:(r + 1) * R].astype(BF16)

        def dx_step(i):
            @pl.when(i >= 0)
            def _():
                lo = jnp.where(i == 0, 0, G * i + 1)
                lax.fori_loop(lo, jnp.minimum(G * i + G + 1, H), g_take, 0)
                dx_rows(jnp.minimum(G * i, H - G))

        def b_to_inner(k, dev):
            return remote(cut(pb, k), cut(rb, k), s_os.at[k], s_tr.at[k], dev)

        def b_to_outer(k, dev):
            return remote(cut(rb, k), cut(mb, k), s_os.at[k], s_mr.at[k], dev)

        def b_up(k):
            part_up(k).wait_recv()

            @pl.when(jnp.logical_not(inner))
            def _():
                b_to_inner(k, inner_dev).start()

            @pl.when(inner)
            def _():
                b_to_inner(k, outer_dev).wait_recv()
                put(pb, k, value(pb, k) + value(rb, k))
                to_mate(k).start()

        def b_total(k):
            to_mate(k).wait_recv()
            put(rb, k, value(pb, k) + value(mb, k))
            b_to_outer(k, outer_dev).start()
            total_down(rb, k).start()

        def b_down(k):
            b_to_outer(k, inner_dev).wait_recv()
            total_down(mb, k).start()

        n_g = -(-H // G)
        slots = N_A + N_B

        def dx_loop(lo, hi):
            lax.fori_loop(min(lo, n_g), min(hi, n_g), lambda i, _: (dx_step(i), 0)[1], 0)

        def b_some(lo, hi):
            for k in range(lo, hi):
                b_up(k)

                @pl.when(inner)
                def _():
                    if k - LAG >= N_A:
                        b_total(k - LAG)

                @pl.when(jnp.logical_not(inner))
                def _():
                    if k - LAG_OUT >= N_A:
                        b_down(k - LAG_OUT)

        b_some(N_A, N_A + 2)

        def dx_between(i, _):
            for m in range(n_g):
                @pl.when(i == m)
                def _():
                    b_some(N_A + 2 + 2 * m, N_A + 4 + 2 * m)

            dx_step(i)
            return 0

        lax.fori_loop(0, n_g, dx_between, 0)
        b_some(N_A + 2 + 2 * n_g, slots)

        @pl.when(inner)
        def _():
            for k in range(slots - LAG, slots):
                b_total(k)

        @pl.when(jnp.logical_not(inner))
        def _():
            for k in range(slots - LAG_OUT, slots):
                b_down(k)

        for k in range(N_A, slots):
            total_down(rb, k).wait_send()

            @pl.when(jnp.logical_not(inner))
            def _():
                b_to_inner(k, inner_dev).wait_send()

            @pl.when(inner)
            def _():
                to_mate(k).wait_send()
                b_to_outer(k, outer_dev).wait_send()

        def drain(h, _):
            for p in range(len(x_cut)):
                x_copy(h, p).wait_send()
            relay_out(h).wait_send()
            return 0

        lax.fori_loop(0, H, drain, 0)

        def drain_w(q, _):
            for y in range(3):
                w_unit(tp, q, y, 0, x_dev).wait_send()
                w_unit(tp, q, y, 1, c_dev).wait_send()
                w_unit(tp_x, q, y, 4, c_dev).wait_send()

                @pl.when(jnp.logical_and(zi < 3, q <= zi))
                def _():
                    w_unit(tp, q, y, 2, right_dev).wait_send()

                @pl.when(jnp.logical_and(zi > 0, q >= zi))
                def _():
                    w_unit(tp, q, y, 3, left_dev).wait_send()

            return 0

        lax.fori_loop(0, 4, drain_w, 0)

    @pl.when(st == 1)
    def _():
        w_loc = pltpu.make_async_copy(w_ref, wall.at[c], s_wl)
        w_core = remote(w_ref, wall.at[c], s_vs.at[2], s_vr.at[2], c_dev)
        vecs_l = [pltpu.make_async_copy(r, vec.at[k, c], s_vl.at[k]) for k, r in enumerate((gam_ref, bet_ref))]
        vecs_r = [remote(r, vec.at[k, c], s_vs.at[k], s_vr.at[k], c_dev) for k, r in enumerate((gam_ref, bet_ref))]
        dz_l = [pltpu.make_async_copy(dz_ref.at[:, :, 2 * s + c], dzb.at[s, c], s_dl.at[s]) for s in range(2)]
        dz_r = [remote(dz_ref.at[:, :, 2 * s + 1 - c], dzb.at[s, c], s_ds.at[s], s_dr.at[s], c_dev) for s in range(2)]

        part = pl.ds(pl.multiple_of(zi * quarter, quarter), quarter)
        w_y = [remote(w_ref.at[3 * y:3 * y + 3, part, :], wall.at[tp, 3 * y:3 * y + 3, part, :], s_ws.at[0, zi, y], s_wr.at[tp, zi, y], y_dev) for y in range(3)]

        for y in range(3):
            w_y[y].start()
        w_loc.start()
        w_core.start()
        for k in range(2):
            vecs_l[k].start()
            vecs_r[k].start()
            dz_l[k].start()
            dz_r[k].start()

        zero_borders(xe)
        zero_borders(ge)
        for buf in (xe, xo, ge, go):
            zero_planes(buf)

        def zero_acc(t, _):
            for k in range(2):
                acc[k, t] = jnp.zeros((CI, CO), F32)
            return 0

        lax.fori_loop(0, 9, zero_acc, 0)

        def zero_dx(h, _):
            dx_ref[h] = jnp.zeros((R, CI), BF16)
            return 0

        lax.fori_loop(0, H, zero_dx, 0)
        for k in range(2):
            vecs_l[k].wait()
            vecs_r[k].wait_recv()
            dz_l[k].wait()
            dz_r[k].wait_recv()
        w_loc.wait()
        w_core.wait_recv()

        def x_in(j, s, p):
            return remote(x_view(s, j, p), x_view(s, j, p), s_xf.at[p, j], s_xr.at[s, p, j], y_dev)

        def x_fwd(j, p):
            return remote(x_view(xi, j, p), x_view(xi, j, p), s_xf.at[p, j], s_xr.at[xi, p, j], x_dev)

        def g_send(h):
            return remote(ge.at[:, h + 1, pl.ds(PAD, R), :], relay.at[:, h], s_gs.at[h], s_gl.at[h], y_dev)

        def x_relay(j):
            for p in range(len(x_cut)):
                x_in(j, xi, p).wait_recv()
                x_fwd(j, p).start()

        lax.fori_loop(0, AHEAD, lambda j, _: (x_relay(j), 0)[1], 0)

        def turn_x(q):
            rows = jnp.concatenate([xe[s, q + 1, PAD:PAD + 128, :] for s in range(2)], axis=0)
            xt[...] = rows.T

        def add_dw(q, t):
            rhs = jnp.concatenate([tap_rows(ge, go, s, q + 2 - t // 3, 1 - t % 3, 128) for s in range(2)], axis=0)
            prod = jnp.dot(xt[...], rhs, preferred_element_type=F32)
            for k in range(2):
                acc[k, t] += prod[:, k * CO:(k + 1) * CO]

        def step(j, _):
            @pl.when(j + AHEAD < H)
            def _():
                x_relay(j + AHEAD)

            @pl.when(j < H)
            def _():
                for p in range(len(x_cut)):
                    x_in(j, 1 - xi, p).wait_recv()
                for s in range(2):
                    odd_copy(xe, xo, s, j + 1)

            @pl.when(jnp.logical_and(j >= 1, j < H + 1))
            def _():
                h = j - 1
                pre = jnp.zeros((2 * R, CW), F32)
                for ky in range(3):
                    for kx in range(3):
                        t = 3 * ky + kx
                        lhs = jnp.concatenate([tap_rows(xe, xo, s, h + ky, kx - 1, R) for s in range(2)], axis=0)
                        rhs = jnp.concatenate([wall[0, t], wall[1, t]], axis=1)
                        pre = pre + jnp.dot(lhs, rhs, preferred_element_type=F32)
                for k in range(2):
                    gam = vec[0, k]
                    bet = vec[1, k]
                    for s in range(2):
                        y = pre[s * R:(s + 1) * R, k * CO:(k + 1) * CO] * gam + bet
                        zb[s, k, h] = jnp.maximum(y, 0.0).reshape(WD, 8, CO).astype(BF16)
                        dzr = dzb[s, k, h].astype(F32).reshape(R, CO)
                        ge[s, h + 1, PAD:PAD + R, k * CO:(k + 1) * CO] = jnp.where(y > 0, dzr * gam, 0.0).astype(BF16)
                g_send(h).start()
                for s in range(2):
                    odd_copy(ge, go, s, h + 1)
                    z_ref[h, :, 2 * s + c] = zb[s, c, h]

            @pl.when(j >= 2)
            def _():
                turn_x(j - 2)
                for t in range(9):
                    add_dw(j - 2, t)

            return 0

        lax.fori_loop(0, H + 1, step, 0)

        def pair(t):
            return remote(acc.at[1 - c, t], prx.at[t], s_ps.at[t], s_pr.at[t], c_dev)

        n_t = CHUNKS[N_A][0]
        order = sorted(range(9), key=lambda t: 2 * (t - n_t) if t >= n_t else 2 * t + 1)
        turn_x(H - 1)
        for t in order:
            if t >= 3:
                add_dw(H - 1, t)
            pair(t).start()
        z_r = [remote(zb.at[s, 1 - c], z_ref.at[:, :, 2 * s + c], s_zs.at[s], s_zr.at[s], c_dev) for s in range(2)]
        z_w = [remote(zb.at[s, 1 - c], z_ref.at[:, :, 2 * s + 1 - c], s_zs.at[s], s_zr.at[s], c_dev) for s in range(2)]
        for s in range(2):
            z_r[s].start()

        def own_part(k):
            t, rows = place(k)
            if k == N_A or (rows.start == 0 and (k > N_A or t < n_t)):
                pair(t).wait_recv()
            return acc[c, t, rows, :] + prx[t, rows, :]

        def send_b(i):
            if i < N_B:
                put(pb, N_A + i, own_part(N_A + i))
                part_up(N_A + i).start()

        def to_inner(k):
            return remote(cut(pb, k), cut(rb, k), s_os.at[k], s_or.at[k], inner_dev)

        def from_outer(k):
            return remote(cut(pb, k), cut(rb, k), s_os.at[k], s_or.at[k], outer_dev)

        def to_outer(k):
            return remote(cut(dw_ref, k), cut(dw_ref, k), s_ts.at[k], s_tr.at[k], outer_dev)

        def from_inner(k):
            return remote(cut(dw_ref, k), cut(dw_ref, k), s_ts.at[k], s_tr.at[k], inner_dev)

        @pl.when(jnp.logical_not(inner))
        def _():
            for k in range(max(N_A, N_B)):
                send_b(k)
                if k < N_A:
                    put(pb, k, own_part(k))
                    to_inner(k).start()
            for k in range(N_A):
                from_inner(k).wait_recv()
                to_inner(k).wait_send()

        @pl.when(inner)
        def _():
            send_b(0)
            for k in range(max(N_A + LAG, N_B)):
                send_b(k + 1)
                if k < N_A:
                    part = own_part(k)
                    from_outer(k).wait_recv()
                    put(pb, k, part + value(rb, k))
                    to_mate(k).start()
                m = k - LAG
                if 0 <= m < N_A:
                    to_mate(m).wait_recv()
                    put(dw_ref, m, value(pb, m) + value(mb, m))
                    to_outer(m).start()
            for k in range(N_A):
                to_mate(k).wait_send()
                to_outer(k).wait_send()

        for k in range(N_A, N_A + N_B):
            total_down(rb, k).wait_recv()
            part_up(k).wait_send()

        def drain(h, _):
            for p in range(len(x_cut)):
                x_fwd(h, p).wait_send()
            g_send(h).wait_send()
            return 0

        lax.fori_loop(0, H, drain, 0)

        def drain_w(t, _):
            pair(t).wait_send()
            return 0

        lax.fori_loop(0, 9, drain_w, 0)
        w_core.wait_send()
        for y in range(3):
            w_y[y].wait_send()
        for k in range(2):
            vecs_r[k].wait_send()
            dz_r[k].wait_send()
            z_r[k].wait_send()
            z_w[k].wait_recv()


def out_kernel(*refs):
    srcs, dsts, sem = refs[:3], refs[3:6], refs[6]
    copies = [pltpu.make_async_copy(a, b, sem.at[i]) for i, (a, b) in enumerate(zip(srcs, dsts))]
    for cp in copies:
        cp.start()
    for cp in copies:
        cp.wait()


def write_out(*arrays):
    return pl.pallas_call(
        out_kernel,
        out_shape=tuple(jax.ShapeDtypeStruct(a.shape, a.dtype) for a in arrays),
        in_specs=[pl.BlockSpec(memory_space=pltpu.VMEM)] * 3,
        out_specs=(pl.BlockSpec(memory_space=pl.ANY),) * 3,
        scratch_shapes=[pltpu.SemaphoreType.DMA((3,))],
        compiler_params=pltpu.CompilerParams(vmem_limit_bytes=16 * 1024 * 1024),
    )(*arrays)


def solution(mesh):
    act_spec = P('stage', ('dp', 'tp'))
    w_spec = P('stage', None, None, None, 'tp')
    vec_spec = P('stage', 'tp')
    chan_spec = P('stage', 'dp', None, None, 'tp')

    def device_step(act_in, w_conv, gamma_vec, beta_vec, z_grad):
        N, H, WD, CI = act_in.shape[1:]
        CO = w_conv.shape[-1]
        R = WD * N
        RP = 128 + 2 * PAD
        x = act_in[0].transpose(1, 2, 0, 3).reshape(H, R, CI)
        w = w_conv[0].reshape(9, CI, CO)
        dz = z_grad[0].transpose(1, 2, 0, 3).reshape(H, WD, 4, N, CO)
        dma = pltpu.SemaphoreType.DMA
        z, dx, dw = pl.pallas_call(
            functools.partial(block_kernel, H, WD, CI, CO),
            out_shape=(
                jax.ShapeDtypeStruct((H, WD, 4, N, CO), BF16),
                jax.ShapeDtypeStruct((H, R, CI), BF16),
                jax.ShapeDtypeStruct((9, CI, CO), F32),
            ),
            in_specs=[pl.BlockSpec(memory_space=pltpu.HBM)] * 5,
            out_specs=(pl.BlockSpec(memory_space=pltpu.VMEM),) * 3,
            scratch_shapes=[
                pltpu.VMEM((2, H + 2, RP, CI), BF16),
                pltpu.VMEM((2, H + 2, RP - 16, CI), BF16),
                pltpu.VMEM((2, H + 2, RP, 2 * CO), BF16),
                pltpu.VMEM((2, H + 2, RP - 16, 2 * CO), BF16),
                pltpu.VMEM((4, 9, CI, CO), BF16),
                pltpu.VMEM((2, 2, H, WD, N, CO), BF16),
                pltpu.VMEM((2, 2, H, WD, N, CO), BF16),
                pltpu.VMEM((2, 2, 1, CO), F32),
                pltpu.VMEM((2, 9, CI, CO), F32),
                pltpu.VMEM((9, CI, CO), F32),
                pltpu.VMEM((9, CI, CO), F32),
                pltpu.VMEM((9, CI, CO), F32),
                pltpu.VMEM((9, CI, CO), F32),
                pltpu.VMEM((CI, 256), BF16),
                pltpu.VMEM((2, H, R, 2 * CO), BF16),
                dma((1, H)), dma((2, 1, H)), dma((1, H)), dma((H,)), dma((2, H)), dma((H,)), dma((H,)),
                dma, dma((5, 4, 3)), dma((4, 4, 3)), dma((2,)), dma((3,)), dma((3,)), dma((2,)), dma((2,)), dma((2,)),
                dma((2,)), dma((2,)), dma((9,)), dma((9,)),
                *[dma((N_A + N_B,))] * 6,
            ],
            compiler_params=pltpu.CompilerParams(collective_id=0, has_side_effects=True, vmem_limit_bytes=46 * 1024 * 1024),
        )(*[pltpu.with_memory_space_constraint(a, pltpu.HBM) for a in (x, w, gamma_vec, beta_vec, dz)])
        z, dx, dw = write_out(z, dx, dw)
        z_full = z.reshape(H, WD, 4 * N, CO).transpose(2, 0, 1, 3)
        dx_full = dx.reshape(H, WD, N, CI).transpose(2, 0, 1, 3)
        dw_full = dw.reshape(3, 3, CI, CO)
        return z_full[None], dx_full[None], dw_full[None]

    return jax.shard_map(device_step, mesh=mesh, in_specs=(act_spec, w_spec, vec_spec, vec_spec, chan_spec), out_specs=(chan_spec, act_spec, w_spec), check_vma=False)
```

```python
import functools

import jax
import jax.numpy as jnp
from jax import lax
from jax.experimental import pallas as pl
from jax.experimental.pallas import tpu as pltpu
from jax.sharding import PartitionSpec as P

MESH = pl.DeviceIdType.MESH
F32 = jnp.float32
BF16 = jnp.bfloat16
PAD = 16
AHEAD = 2
LAG = 5
LAG_OUT = 14
N_B = 28
PIECES = 8
STEPS = 4
CHUNKS = tuple((t, q) for t in range(9) for q in range(PIECES))
N_A = len(CHUNKS) - N_B


def remote(src, dst, send_sem, recv_sem, dev):
    return pltpu.make_async_remote_copy(src_ref=src, dst_ref=dst, send_sem=send_sem, recv_sem=recv_sem, device_id=dev, device_id_type=MESH)


def block_kernel(H, WD, CI, CO, x_ref, w_ref, gam_ref, bet_ref, dz_ref, z_ref, dx_ref, dw_ref,
                 xe, xo, ge, go, wall, dzb, zb, vec, acc, prx, pb, rb, mb, xt, relay, *sems):
    (s_xs, s_xr, s_xf, s_gs, s_gr, s_gl, s_gf, s_wl, s_ws, s_wr, s_vl, s_vs, s_vr, s_dl, s_ds, s_dr,
     s_zs, s_zr, s_ps, s_pr, s_os, s_or, s_ms, s_mr, s_ts, s_tr) = sems
    R = WD * 8
    quarter = CI // 4
    n_blk = min(CI, 256)
    CW = 2 * CO
    zi = lax.axis_index("dp")
    st = lax.axis_index("stage")
    tp = lax.axis_index("tp")
    xi = tp // 2
    c = tp % 2
    y_dev = (zi, 1 - st, tp)
    x_dev = (zi, st, 2 * (1 - xi) + c)
    c_dev = (zi, st, 2 * xi + 1 - c)
    z_mate = jnp.where(zi == 1, 2, 1)
    z_out = jnp.where(zi < 2, 0, 3)
    z_in = jnp.where(zi < 2, 1, 2)
    inner = jnp.logical_or(zi == 1, zi == 2)
    mate_dev = (z_mate, st, tp)
    outer_dev = (z_out, st, tp)
    inner_dev = (z_in, st, tp)

    barrier = pltpu.get_barrier_semaphore()
    for dev in (y_dev, x_dev, c_dev):
        pl.semaphore_signal(barrier, inc=1, device_id=dev, device_id_type=MESH)

    @pl.when(inner)
    def _():
        for dev in (mate_dev, outer_dev):
            pl.semaphore_signal(barrier, inc=1, device_id=dev, device_id_type=MESH)
        pl.semaphore_wait(barrier, 5)

    @pl.when(jnp.logical_not(inner))
    def _():
        pl.semaphore_signal(barrier, inc=1, device_id=inner_dev, device_id_type=MESH)
        pl.semaphore_wait(barrier, 4)

    def zero_borders(buf):
        ch = buf.shape[-1]

        def rows(h, _):
            for s in range(2):
                buf[s, h, 0:PAD, :] = jnp.zeros((PAD, ch), BF16)
                buf[s, h, PAD + R:, :] = jnp.zeros((buf.shape[2] - PAD - R, ch), BF16)
            return 0

        lax.fori_loop(0, H + 2, rows, 0)

    def zero_planes(buf):
        for s in range(2):
            for h in (0, H + 1):
                buf[s, h] = jnp.zeros(buf.shape[2:], BF16)

    def odd_copy(even, odd, s, h):
        n = odd.shape[2]
        odd[s, h] = even[s, h, 8:8 + n, :]

    def tap_rows(even, odd, s, plane, shift, n):
        if shift == 0:
            return even[s, plane, PAD:PAD + n, :]
        start = PAD + 8 * shift - 8
        return odd[s, plane, start:start + n, :]

    x_cut = ((0, 48), (48, R - 48))

    def x_view(s, h, p):
        return xe.at[s, h + 1, pl.ds(PAD + x_cut[p][0], x_cut[p][1]), :]

    def place(k):
        t, q = CHUNKS[k]
        return t, slice(q * (CI // PIECES), (q + 1) * (CI // PIECES))

    def cut(buf, k):
        t, rows = place(k)
        return buf.at[t, rows, :]

    def value(buf, k):
        t, rows = place(k)
        return buf[t, rows, :]

    def put(buf, k, val):
        t, rows = place(k)
        buf[t, rows, :] = val

    def part_up(k):
        return remote(cut(pb, k), cut(pb, k), s_os.at[k], s_or.at[k], y_dev)

    def to_mate(k):
        return remote(cut(pb, k), cut(mb, k), s_ms.at[k], s_mr.at[k], mate_dev)

    def total_down(src, k):
        return remote(cut(src, k), cut(dw_ref, k), s_ts.at[k], s_tr.at[k], y_dev)

    @pl.when(st == 0)
    def _():
        def x_copy(h, p):
            return remote(x_ref.at[h, pl.ds(*x_cut[p]), :], x_view(xi, h, p), s_xs.at[p, h], s_xr.at[xi, p, h], y_dev)

        def x_send(h, _):
            for p in range(len(x_cut)):
                x_copy(h, p).start()
            return 0

        lax.fori_loop(0, H, x_send, 0)
        zero_borders(ge)
        zero_planes(ge)
        zero_planes(go)

        def zero_out(h, _):
            z_ref[h] = jnp.zeros(z_ref.shape[1:], BF16)
            return 0

        lax.fori_loop(0, H, zero_out, 0)

        def zero_dw(t, _):
            dw_ref[t] = jnp.zeros((CI, CO), F32)
            return 0

        lax.fori_loop(0, 9, zero_dw, 0)

        def g_in(j, b):
            return remote(ge.at[b, j + 1, pl.ds(PAD, R), :], ge.at[b, j + 1, pl.ds(PAD, R), :], s_gf.at[j], s_gr.at[b, j], x_dev)

        def relay_in(j):
            return remote(relay.at[:, j], relay.at[:, j], s_gf.at[j], s_gl.at[j], y_dev)

        def relay_out(j):
            return remote(relay.at[1 - xi, j], ge.at[xi, j + 1, pl.ds(PAD, R), :], s_gf.at[j], s_gr.at[xi, j], x_dev)

        def g_relay(j):
            relay_in(j).wait_recv()
            relay_out(j).start()
            ge[xi, j + 1, PAD:PAD + R, :] = relay[xi, j]

        def relay_rows(lo, hi):
            lax.fori_loop(lo, min(hi, H), lambda j, _: (g_relay(j), 0)[1], 0)

        tp_x = 2 * (1 - xi) + c
        left_dev = (jnp.maximum(zi - 1, 0), st, tp)
        right_dev = (jnp.minimum(zi + 1, 3), st, tp)

        def w_unit(b, q, y, kind, dev):
            view = wall.at[b, pl.ds(3 * y, 3), pl.ds(pl.multiple_of(q * quarter, quarter), quarter), :]
            return remote(view, view, s_ws.at[kind, q, y], s_wr.at[b, q, y], dev)

        def w_got(q, go_right, go_left):
            def take(y, _):
                w_unit(tp, q, y, 0, y_dev).wait_recv()
                if go_right:
                    @pl.when(zi < 3)
                    def _():
                        w_unit(tp, q, y, 2, right_dev).start()
                if go_left:
                    @pl.when(zi > 0)
                    def _():
                        w_unit(tp, q, y, 3, left_dev).start()
                w_unit(tp, q, y, 0, x_dev).start()
                w_unit(tp, q, y, 1, c_dev).start()
                return 0

            lax.fori_loop(0, 3, take, 0)

        w_got(zi, True, True)
        for d in range(1, 4):
            @pl.when(zi - d >= 0)
            def _():
                w_got(zi - d, True, False)

            @pl.when(zi + d <= 3)
            def _():
                w_got(zi + d, False, True)

            relay_rows(2 * (d - 1), 2 * d)

        def w_cross(q, _):
            for y in range(3):
                w_unit(tp_x, q, y, 4, x_dev).wait_recv()
                w_unit(tp_x, q, y, 4, c_dev).start()
            return 0

        relay_rows(6, 9)
        lax.fori_loop(0, 4, w_cross, 0)
        relay_rows(9, H)

        def w_all(q, _):
            for y in range(3):
                for b in (2 * xi + 1 - c, 2 * (1 - xi) + 1 - c):
                    w_unit(b, q, y, 1, c_dev).wait_recv()
            return 0

        lax.fori_loop(0, 4, w_all, 0)

        G = 4

        def g_take(j, _):
            g_in(j, 1 - xi).wait_recv()
            for b in range(2):
                odd_copy(ge, go, b, j + 1)
            return 0

        def dx_rows(h0):
            for n in range(CI // n_blk):
                tot = jnp.zeros((G * R, n_blk), F32)
                for b in range(2):
                    for t in range(9):
                        lhs = jnp.concatenate([tap_rows(ge, go, b, h0 + r + 2 - t // 3, 1 - t % 3, R) for r in range(G)], axis=0)
                        rhs = jnp.concatenate([wall[2 * b + i, t, n * n_blk:(n + 1) * n_blk, :] for i in range(2)], axis=1)
                        tot = tot + lax.dot_general(lhs, rhs, (((1,), (1,)), ((), ())), preferred_element_type=F32)
                for r in range(G):
                    dx_ref[h0 + r, :, n * n_blk:(n + 1) * n_blk] = tot[r * R:(r + 1) * R].astype(BF16)

        def dx_step(i):
            @pl.when(i >= 0)
            def _():
                lo = jnp.where(i == 0, 0, G * i + 1)
                lax.fori_loop(lo, jnp.minimum(G * i + G + 1, H), g_take, 0)
                dx_rows(jnp.minimum(G * i, H - G))

        def b_to_inner(k, dev):
            return remote(cut(pb, k), cut(rb, k), s_os.at[k], s_tr.at[k], dev)

        def b_to_outer(k, dev):
            return remote(cut(rb, k), cut(mb, k), s_os.at[k], s_mr.at[k], dev)

        def b_up(k):
            part_up(k).wait_recv()

            @pl.when(jnp.logical_not(inner))
            def _():
                b_to_inner(k, inner_dev).start()

            @pl.when(inner)
            def _():
                b_to_inner(k, outer_dev).wait_recv()
                put(pb, k, value(pb, k) + value(rb, k))
                to_mate(k).start()

        def b_total(k):
            to_mate(k).wait_recv()
            put(rb, k, value(pb, k) + value(mb, k))
            b_to_outer(k, outer_dev).start()
            total_down(rb, k).start()

        def b_down(k):
            b_to_outer(k, inner_dev).wait_recv()
            total_down(mb, k).start()

        n_g = -(-H // G)
        slots = N_A + N_B

        def dx_loop(lo, hi):
            lax.fori_loop(min(lo, n_g), min(hi, n_g), lambda i, _: (dx_step(i), 0)[1], 0)

        def b_some(lo, hi):
            for k in range(lo, hi):
                b_up(k)

                @pl.when(inner)
                def _():
                    if k - LAG >= N_A:
                        b_total(k - LAG)

                @pl.when(jnp.logical_not(inner))
                def _():
                    if k - LAG_OUT >= N_A:
                        b_down(k - LAG_OUT)

        b_some(N_A, N_A + STEPS)

        def dx_between(i, _):
            for m in range(n_g):
                @pl.when(i == m)
                def _():
                    b_some(N_A + STEPS * (m + 1), N_A + STEPS * (m + 2))

            dx_step(i)
            return 0

        lax.fori_loop(0, n_g, dx_between, 0)
        b_some(N_A + STEPS * (n_g + 1), slots)

        @pl.when(inner)
        def _():
            for k in range(slots - LAG, slots):
                b_total(k)

        @pl.when(jnp.logical_not(inner))
        def _():
            for k in range(slots - LAG_OUT, slots):
                b_down(k)

        for k in range(N_A, slots):
            total_down(rb, k).wait_send()

            @pl.when(jnp.logical_not(inner))
            def _():
                b_to_inner(k, inner_dev).wait_send()

            @pl.when(inner)
            def _():
                to_mate(k).wait_send()
                b_to_outer(k, outer_dev).wait_send()

        def drain(h, _):
            for p in range(len(x_cut)):
                x_copy(h, p).wait_send()
            relay_out(h).wait_send()
            return 0

        lax.fori_loop(0, H, drain, 0)

        def drain_w(q, _):
            for y in range(3):
                w_unit(tp, q, y, 0, x_dev).wait_send()
                w_unit(tp, q, y, 1, c_dev).wait_send()
                w_unit(tp_x, q, y, 4, c_dev).wait_send()

                @pl.when(jnp.logical_and(zi < 3, q <= zi))
                def _():
                    w_unit(tp, q, y, 2, right_dev).wait_send()

                @pl.when(jnp.logical_and(zi > 0, q >= zi))
                def _():
                    w_unit(tp, q, y, 3, left_dev).wait_send()

            return 0

        lax.fori_loop(0, 4, drain_w, 0)

    @pl.when(st == 1)
    def _():
        w_loc = pltpu.make_async_copy(w_ref, wall.at[c], s_wl)
        w_core = remote(w_ref, wall.at[c], s_vs.at[2], s_vr.at[2], c_dev)
        vecs_l = [pltpu.make_async_copy(r, vec.at[k, c], s_vl.at[k]) for k, r in enumerate((gam_ref, bet_ref))]
        vecs_r = [remote(r, vec.at[k, c], s_vs.at[k], s_vr.at[k], c_dev) for k, r in enumerate((gam_ref, bet_ref))]
        dz_l = [pltpu.make_async_copy(dz_ref.at[:, :, 2 * s + c], dzb.at[s, c], s_dl.at[s]) for s in range(2)]
        dz_r = [remote(dz_ref.at[:, :, 2 * s + 1 - c], dzb.at[s, c], s_ds.at[s], s_dr.at[s], c_dev) for s in range(2)]

        part = pl.ds(pl.multiple_of(zi * quarter, quarter), quarter)
        w_y = [remote(w_ref.at[3 * y:3 * y + 3, part, :], wall.at[tp, 3 * y:3 * y + 3, part, :], s_ws.at[0, zi, y], s_wr.at[tp, zi, y], y_dev) for y in range(3)]

        for y in range(3):
            w_y[y].start()
        w_loc.start()
        w_core.start()
        for k in range(2):
            vecs_l[k].start()
            vecs_r[k].start()
            dz_l[k].start()
            dz_r[k].start()

        zero_borders(xe)
        zero_borders(ge)
        for buf in (xe, xo, ge, go):
            zero_planes(buf)

        def zero_acc(t, _):
            for k in range(2):
                acc[k, t] = jnp.zeros((CI, CO), F32)
            return 0

        lax.fori_loop(0, 9, zero_acc, 0)

        def zero_dx(h, _):
            dx_ref[h] = jnp.zeros((R, CI), BF16)
            return 0

        lax.fori_loop(0, H, zero_dx, 0)
        for k in range(2):
            vecs_l[k].wait()
            vecs_r[k].wait_recv()
            dz_l[k].wait()
            dz_r[k].wait_recv()
        w_loc.wait()
        w_core.wait_recv()

        def x_in(j, s, p):
            return remote(x_view(s, j, p), x_view(s, j, p), s_xf.at[p, j], s_xr.at[s, p, j], y_dev)

        def x_fwd(j, p):
            return remote(x_view(xi, j, p), x_view(xi, j, p), s_xf.at[p, j], s_xr.at[xi, p, j], x_dev)

        def g_send(h):
            return remote(ge.at[:, h + 1, pl.ds(PAD, R), :], relay.at[:, h], s_gs.at[h], s_gl.at[h], y_dev)

        def x_relay(j):
            for p in range(len(x_cut)):
                x_in(j, xi, p).wait_recv()
                x_fwd(j, p).start()

        lax.fori_loop(0, AHEAD, lambda j, _: (x_relay(j), 0)[1], 0)

        def turn_x(q):
            rows = jnp.concatenate([xe[s, q + 1, PAD:PAD + 128, :] for s in range(2)], axis=0)
            xt[...] = rows.T

        def add_dw(q, t):
            rhs = jnp.concatenate([tap_rows(ge, go, s, q + 2 - t // 3, 1 - t % 3, 128) for s in range(2)], axis=0)
            prod = jnp.dot(xt[...], rhs, preferred_element_type=F32)
            for k in range(2):
                acc[k, t] += prod[:, k * CO:(k + 1) * CO]

        def step(j, _):
            @pl.when(j + AHEAD < H)
            def _():
                x_relay(j + AHEAD)

            @pl.when(j < H)
            def _():
                for p in range(len(x_cut)):
                    x_in(j, 1 - xi, p).wait_recv()
                for s in range(2):
                    odd_copy(xe, xo, s, j + 1)

            @pl.when(jnp.logical_and(j >= 1, j < H + 1))
            def _():
                h = j - 1
                pre = jnp.zeros((2 * R, CW), F32)
                for ky in range(3):
                    for kx in range(3):
                        t = 3 * ky + kx
                        lhs = jnp.concatenate([tap_rows(xe, xo, s, h + ky, kx - 1, R) for s in range(2)], axis=0)
                        rhs = jnp.concatenate([wall[0, t], wall[1, t]], axis=1)
                        pre = pre + jnp.dot(lhs, rhs, preferred_element_type=F32)
                for k in range(2):
                    gam = vec[0, k]
                    bet = vec[1, k]
                    for s in range(2):
                        y = pre[s * R:(s + 1) * R, k * CO:(k + 1) * CO] * gam + bet
                        zb[s, k, h] = jnp.maximum(y, 0.0).reshape(WD, 8, CO).astype(BF16)
                        dzr = dzb[s, k, h].astype(F32).reshape(R, CO)
                        ge[s, h + 1, PAD:PAD + R, k * CO:(k + 1) * CO] = jnp.where(y > 0, dzr * gam, 0.0).astype(BF16)
                g_send(h).start()
                for s in range(2):
                    odd_copy(ge, go, s, h + 1)
                    z_ref[h, :, 2 * s + c] = zb[s, c, h]

            @pl.when(j >= 2)
            def _():
                turn_x(j - 2)
                for t in range(9):
                    add_dw(j - 2, t)

            return 0

        lax.fori_loop(0, H + 1, step, 0)

        def pair(t):
            return remote(acc.at[1 - c, t], prx.at[t], s_ps.at[t], s_pr.at[t], c_dev)

        n_t = CHUNKS[N_A][0]
        order = sorted(range(9), key=lambda t: 2 * (t - n_t) if t >= n_t else 2 * t + 1)
        turn_x(H - 1)
        for t in order:
            if t >= 3:
                add_dw(H - 1, t)
            pair(t).start()
        z_r = [remote(zb.at[s, 1 - c], z_ref.at[:, :, 2 * s + c], s_zs.at[s], s_zr.at[s], c_dev) for s in range(2)]
        z_w = [remote(zb.at[s, 1 - c], z_ref.at[:, :, 2 * s + 1 - c], s_zs.at[s], s_zr.at[s], c_dev) for s in range(2)]
        for s in range(2):
            z_r[s].start()

        def own_part(k):
            t, rows = place(k)
            if k == N_A or (rows.start == 0 and (k > N_A or t < n_t)):
                pair(t).wait_recv()
            return acc[c, t, rows, :] + prx[t, rows, :]

        def send_b(i):
            if i < N_B:
                put(pb, N_A + i, own_part(N_A + i))
                part_up(N_A + i).start()

        def to_inner(k):
            return remote(cut(pb, k), cut(rb, k), s_os.at[k], s_or.at[k], inner_dev)

        def from_outer(k):
            return remote(cut(pb, k), cut(rb, k), s_os.at[k], s_or.at[k], outer_dev)

        def to_outer(k):
            return remote(cut(dw_ref, k), cut(dw_ref, k), s_ts.at[k], s_tr.at[k], outer_dev)

        def from_inner(k):
            return remote(cut(dw_ref, k), cut(dw_ref, k), s_ts.at[k], s_tr.at[k], inner_dev)

        @pl.when(jnp.logical_not(inner))
        def _():
            for k in range(max(N_A, N_B)):
                send_b(k)
                if k < N_A:
                    put(pb, k, own_part(k))
                    to_inner(k).start()
            for k in range(N_A):
                from_inner(k).wait_recv()
                to_inner(k).wait_send()

        @pl.when(inner)
        def _():
            send_b(0)
            for k in range(max(N_A + LAG, N_B)):
                send_b(k + 1)
                if k < N_A:
                    part = own_part(k)
                    from_outer(k).wait_recv()
                    put(pb, k, part + value(rb, k))
                    to_mate(k).start()
                m = k - LAG
                if 0 <= m < N_A:
                    to_mate(m).wait_recv()
                    put(dw_ref, m, value(pb, m) + value(mb, m))
                    to_outer(m).start()
            for k in range(N_A):
                to_mate(k).wait_send()
                to_outer(k).wait_send()

        for k in range(N_A, N_A + N_B):
            total_down(rb, k).wait_recv()
            part_up(k).wait_send()

        def drain(h, _):
            for p in range(len(x_cut)):
                x_fwd(h, p).wait_send()
            g_send(h).wait_send()
            return 0

        lax.fori_loop(0, H, drain, 0)

        def drain_w(t, _):
            pair(t).wait_send()
            return 0

        lax.fori_loop(0, 9, drain_w, 0)
        w_core.wait_send()
        for y in range(3):
            w_y[y].wait_send()
        for k in range(2):
            vecs_r[k].wait_send()
            dz_r[k].wait_send()
            z_r[k].wait_send()
            z_w[k].wait_recv()


def out_kernel(*refs):
    srcs, dsts, sem = refs[:3], refs[3:6], refs[6]
    copies = [pltpu.make_async_copy(a, b, sem.at[i]) for i, (a, b) in enumerate(zip(srcs, dsts))]
    for cp in copies:
        cp.start()
    for cp in copies:
        cp.wait()


def write_out(*arrays):
    return pl.pallas_call(
        out_kernel,
        out_shape=tuple(jax.ShapeDtypeStruct(a.shape, a.dtype) for a in arrays),
        in_specs=[pl.BlockSpec(memory_space=pltpu.VMEM)] * 3,
        out_specs=(pl.BlockSpec(memory_space=pl.ANY),) * 3,
        scratch_shapes=[pltpu.SemaphoreType.DMA((3,))],
        compiler_params=pltpu.CompilerParams(vmem_limit_bytes=16 * 1024 * 1024),
    )(*arrays)


def solution(mesh):
    act_spec = P('stage', ('dp', 'tp'))
    w_spec = P('stage', None, None, None, 'tp')
    vec_spec = P('stage', 'tp')
    chan_spec = P('stage', 'dp', None, None, 'tp')

    def device_step(act_in, w_conv, gamma_vec, beta_vec, z_grad):
        N, H, WD, CI = act_in.shape[1:]
        CO = w_conv.shape[-1]
        R = WD * N
        RP = 128 + 2 * PAD
        x = act_in[0].transpose(1, 2, 0, 3).reshape(H, R, CI)
        w = w_conv[0].reshape(9, CI, CO)
        dz = z_grad[0].transpose(1, 2, 0, 3).reshape(H, WD, 4, N, CO)
        dma = pltpu.SemaphoreType.DMA
        z, dx, dw = pl.pallas_call(
            functools.partial(block_kernel, H, WD, CI, CO),
            out_shape=(
                jax.ShapeDtypeStruct((H, WD, 4, N, CO), BF16),
                jax.ShapeDtypeStruct((H, R, CI), BF16),
                jax.ShapeDtypeStruct((9, CI, CO), F32),
            ),
            in_specs=[pl.BlockSpec(memory_space=pltpu.HBM)] * 5,
            out_specs=(pl.BlockSpec(memory_space=pltpu.VMEM),) * 3,
            scratch_shapes=[
                pltpu.VMEM((2, H + 2, RP, CI), BF16),
                pltpu.VMEM((2, H + 2, RP - 16, CI), BF16),
                pltpu.VMEM((2, H + 2, RP, 2 * CO), BF16),
                pltpu.VMEM((2, H + 2, RP - 16, 2 * CO), BF16),
                pltpu.VMEM((4, 9, CI, CO), BF16),
                pltpu.VMEM((2, 2, H, WD, N, CO), BF16),
                pltpu.VMEM((2, 2, H, WD, N, CO), BF16),
                pltpu.VMEM((2, 2, 1, CO), F32),
                pltpu.VMEM((2, 9, CI, CO), F32),
                pltpu.VMEM((9, CI, CO), F32),
                pltpu.VMEM((9, CI, CO), F32),
                pltpu.VMEM((9, CI, CO), F32),
                pltpu.VMEM((9, CI, CO), F32),
                pltpu.VMEM((CI, 256), BF16),
                pltpu.VMEM((2, H, R, 2 * CO), BF16),
                dma((2, H)), dma((2, 2, H)), dma((2, H)), dma((H,)), dma((2, H)), dma((H,)), dma((H,)),
                dma, dma((5, 4, 3)), dma((4, 4, 3)), dma((2,)), dma((3,)), dma((3,)), dma((2,)), dma((2,)), dma((2,)),
                dma((2,)), dma((2,)), dma((9,)), dma((9,)),
                *[dma((N_A + N_B,))] * 6,
            ],
            compiler_params=pltpu.CompilerParams(collective_id=0, has_side_effects=True, vmem_limit_bytes=46 * 1024 * 1024),
        )(*[pltpu.with_memory_space_constraint(a, pltpu.HBM) for a in (x, w, gamma_vec, beta_vec, dz)])
        z, dx, dw = write_out(z, dx, dw)
        z_full = z.reshape(H, WD, 4 * N, CO).transpose(2, 0, 1, 3)
        dx_full = dx.reshape(H, WD, N, CI).transpose(2, 0, 1, 3)
        dw_full = dw.reshape(3, 3, CI, CO)
        return z_full[None], dx_full[None], dw_full[None]

    return jax.shard_map(device_step, mesh=mesh, in_specs=(act_spec, w_spec, vec_spec, vec_spec, chan_spec), out_specs=(chan_spec, act_spec, w_spec), check_vma=False)
```

```python
import functools

import jax
import jax.numpy as jnp
from jax import lax
from jax.experimental import pallas as pl
from jax.experimental.pallas import tpu as pltpu
from jax.sharding import PartitionSpec as P

MESH = pl.DeviceIdType.MESH
F32 = jnp.float32
BF16 = jnp.bfloat16
PAD = 16
AHEAD = 2
LAG = 3
LAG_OUT = 8
N_B = 14
CHUNKS = tuple((t, q, 1) for t in range(9) for q in range(4))
N_A = len(CHUNKS) - N_B


def remote(src, dst, send_sem, recv_sem, dev):
    return pltpu.make_async_remote_copy(src_ref=src, dst_ref=dst, send_sem=send_sem, recv_sem=recv_sem, device_id=dev, device_id_type=MESH)


def block_kernel(H, WD, CI, CO, x_ref, w_ref, gam_ref, bet_ref, dz_ref, z_ref, dx_ref, dw_ref,
                 xe, xo, ge, go, wall, dzb, zb, vec, acc, prx, pb, rb, mb, xt, relay, *sems):
    (s_xs, s_xr, s_xf, s_gs, s_gr, s_gl, s_gf, s_wl, s_ws, s_wr, s_vl, s_vs, s_vr, s_dl, s_ds, s_dr,
     s_zs, s_zr, s_ps, s_pr, s_os, s_or, s_ms, s_mr, s_ts, s_tr) = sems
    R = WD * 8
    quarter = CI // 4
    n_blk = min(CI, 256)
    CW = 2 * CO
    zi = lax.axis_index("dp")
    st = lax.axis_index("stage")
    tp = lax.axis_index("tp")
    xi = tp // 2
    c = tp % 2
    y_dev = (zi, 1 - st, tp)
    x_dev = (zi, st, 2 * (1 - xi) + c)
    c_dev = (zi, st, 2 * xi + 1 - c)
    z_mate = jnp.where(zi == 1, 2, 1)
    z_out = jnp.where(zi < 2, 0, 3)
    z_in = jnp.where(zi < 2, 1, 2)
    inner = jnp.logical_or(zi == 1, zi == 2)
    mate_dev = (z_mate, st, tp)
    outer_dev = (z_out, st, tp)
    inner_dev = (z_in, st, tp)

    barrier = pltpu.get_barrier_semaphore()
    for dev in (y_dev, x_dev, c_dev):
        pl.semaphore_signal(barrier, inc=1, device_id=dev, device_id_type=MESH)

    @pl.when(inner)
    def _():
        for dev in (mate_dev, outer_dev):
            pl.semaphore_signal(barrier, inc=1, device_id=dev, device_id_type=MESH)
        pl.semaphore_wait(barrier, 5)

    @pl.when(jnp.logical_not(inner))
    def _():
        pl.semaphore_signal(barrier, inc=1, device_id=inner_dev, device_id_type=MESH)
        pl.semaphore_wait(barrier, 4)

    def zero_borders(buf):
        ch = buf.shape[-1]

        def rows(h, _):
            for s in range(2):
                buf[s, h, 0:PAD, :] = jnp.zeros((PAD, ch), BF16)
                buf[s, h, PAD + R:, :] = jnp.zeros((buf.shape[2] - PAD - R, ch), BF16)
            return 0

        lax.fori_loop(0, H + 2, rows, 0)

    def zero_planes(buf):
        for s in range(2):
            for h in (0, H + 1):
                buf[s, h] = jnp.zeros(buf.shape[2:], BF16)

    def odd_copy(even, odd, s, h):
        n = odd.shape[2]
        odd[s, h] = even[s, h, 8:8 + n, :]

    def tap_rows(even, odd, s, plane, shift, n):
        if shift == 0:
            return even[s, plane, PAD:PAD + n, :]
        start = PAD + 8 * shift - 8
        return odd[s, plane, start:start + n, :]

    x_cut = ((0, R),)

    def x_view(s, h, p):
        return xe.at[s, h + 1, pl.ds(PAD + x_cut[p][0], x_cut[p][1]), :]

    def place(k):
        t, q0, nq = CHUNKS[k]
        return t, slice(q0 * quarter, (q0 + nq) * quarter)

    def cut(buf, k):
        t, rows = place(k)
        return buf.at[t, rows, :]

    def value(buf, k):
        t, rows = place(k)
        return buf[t, rows, :]

    def put(buf, k, val):
        t, rows = place(k)
        buf[t, rows, :] = val

    def part_up(k):
        return remote(cut(pb, k), cut(pb, k), s_os.at[k], s_or.at[k], y_dev)

    def to_mate(k):
        return remote(cut(pb, k), cut(mb, k), s_ms.at[k], s_mr.at[k], mate_dev)

    def total_down(src, k):
        return remote(cut(src, k), cut(dw_ref, k), s_ts.at[k], s_tr.at[k], y_dev)

    @pl.when(st == 0)
    def _():
        def x_copy(h, p):
            return remote(x_ref.at[h, pl.ds(*x_cut[p]), :], x_view(xi, h, p), s_xs.at[p, h], s_xr.at[xi, p, h], y_dev)

        def x_send(h, _):
            for p in range(len(x_cut)):
                x_copy(h, p).start()
            return 0

        lax.fori_loop(0, H, x_send, 0)
        zero_borders(ge)
        zero_planes(ge)
        zero_planes(go)

        def zero_out(h, _):
            z_ref[h] = jnp.zeros(z_ref.shape[1:], BF16)
            return 0

        lax.fori_loop(0, H, zero_out, 0)

        def zero_dw(t, _):
            dw_ref[t] = jnp.zeros((CI, CO), F32)
            return 0

        lax.fori_loop(0, 9, zero_dw, 0)

        def g_in(j, b):
            return remote(ge.at[b, j + 1, pl.ds(PAD, R), :], ge.at[b, j + 1, pl.ds(PAD, R), :], s_gf.at[j], s_gr.at[b, j], x_dev)

        def relay_in(j):
            return remote(relay.at[:, j], relay.at[:, j], s_gf.at[j], s_gl.at[j], y_dev)

        def relay_out(j):
            return remote(relay.at[1 - xi, j], ge.at[xi, j + 1, pl.ds(PAD, R), :], s_gf.at[j], s_gr.at[xi, j], x_dev)

        def g_relay(j):
            relay_in(j).wait_recv()
            relay_out(j).start()
            ge[xi, j + 1, PAD:PAD + R, :] = relay[xi, j]

        def relay_rows(lo, hi):
            lax.fori_loop(lo, min(hi, H), lambda j, _: (g_relay(j), 0)[1], 0)

        tp_x = 2 * (1 - xi) + c
        left_dev = (jnp.maximum(zi - 1, 0), st, tp)
        right_dev = (jnp.minimum(zi + 1, 3), st, tp)

        def w_unit(b, q, y, kind, dev):
            view = wall.at[b, pl.ds(3 * y, 3), pl.ds(pl.multiple_of(q * quarter, quarter), quarter), :]
            return remote(view, view, s_ws.at[kind, q, y], s_wr.at[b, q, y], dev)

        def w_got(q, go_right, go_left):
            def take(y, _):
                w_unit(tp, q, y, 0, y_dev).wait_recv()
                if go_right:
                    @pl.when(zi < 3)
                    def _():
                        w_unit(tp, q, y, 2, right_dev).start()
                if go_left:
                    @pl.when(zi > 0)
                    def _():
                        w_unit(tp, q, y, 3, left_dev).start()
                w_unit(tp, q, y, 0, x_dev).start()
                w_unit(tp, q, y, 1, c_dev).start()
                return 0

            lax.fori_loop(0, 3, take, 0)

        w_got(zi, True, True)
        for d in range(1, 4):
            @pl.when(zi - d >= 0)
            def _():
                w_got(zi - d, True, False)

            @pl.when(zi + d <= 3)
            def _():
                w_got(zi + d, False, True)

            relay_rows(2 * (d - 1), 2 * d)

        def w_cross(q, _):
            for y in range(3):
                w_unit(tp_x, q, y, 4, x_dev).wait_recv()
                w_unit(tp_x, q, y, 4, c_dev).start()
            return 0

        relay_rows(6, 9)
        lax.fori_loop(0, 4, w_cross, 0)
        relay_rows(9, H)

        def w_all(q, _):
            for y in range(3):
                for b in (2 * xi + 1 - c, 2 * (1 - xi) + 1 - c):
                    w_unit(b, q, y, 1, c_dev).wait_recv()
            return 0

        lax.fori_loop(0, 4, w_all, 0)

        G = 4

        def g_take(j, _):
            g_in(j, 1 - xi).wait_recv()
            for b in range(2):
                odd_copy(ge, go, b, j + 1)
            return 0

        def dx_rows(h0):
            for n in range(CI // n_blk):
                tot = jnp.zeros((G * R, n_blk), F32)
                for b in range(2):
                    for t in range(9):
                        lhs = jnp.concatenate([tap_rows(ge, go, b, h0 + r + 2 - t // 3, 1 - t % 3, R) for r in range(G)], axis=0)
                        rhs = jnp.concatenate([wall[2 * b + i, t, n * n_blk:(n + 1) * n_blk, :] for i in range(2)], axis=1)
                        tot = tot + lax.dot_general(lhs, rhs, (((1,), (1,)), ((), ())), preferred_element_type=F32)
                for r in range(G):
                    dx_ref[h0 + r, :, n * n_blk:(n + 1) * n_blk] = tot[r * R:(r + 1) * R].astype(BF16)

        def dx_step(i):
            @pl.when(i >= 0)
            def _():
                lo = jnp.where(i == 0, 0, G * i + 1)
                lax.fori_loop(lo, jnp.minimum(G * i + G + 1, H), g_take, 0)
                dx_rows(jnp.minimum(G * i, H - G))

        def b_to_inner(k, dev):
            return remote(cut(pb, k), cut(rb, k), s_os.at[k], s_tr.at[k], dev)

        def b_to_outer(k, dev):
            return remote(cut(rb, k), cut(mb, k), s_os.at[k], s_mr.at[k], dev)

        def b_up(k):
            part_up(k).wait_recv()

            @pl.when(jnp.logical_not(inner))
            def _():
                b_to_inner(k, inner_dev).start()

            @pl.when(inner)
            def _():
                b_to_inner(k, outer_dev).wait_recv()
                put(pb, k, value(pb, k) + value(rb, k))
                to_mate(k).start()

        def b_total(k):
            to_mate(k).wait_recv()
            put(rb, k, value(pb, k) + value(mb, k))
            b_to_outer(k, outer_dev).start()
            total_down(rb, k).start()

        def b_down(k):
            b_to_outer(k, inner_dev).wait_recv()
            total_down(mb, k).start()

        n_g = -(-H // G)
        slots = N_A + N_B

        def dx_loop(lo, hi):
            lax.fori_loop(min(lo, n_g), min(hi, n_g), lambda i, _: (dx_step(i), 0)[1], 0)

        def b_some(lo, hi):
            for k in range(lo, hi):
                b_up(k)

                @pl.when(inner)
                def _():
                    if k - LAG >= N_A:
                        b_total(k - LAG)

                @pl.when(jnp.logical_not(inner))
                def _():
                    if k - LAG_OUT >= N_A:
                        b_down(k - LAG_OUT)

        b_some(N_A, N_A + 2)

        def dx_between(i, _):
            for m in range(n_g):
                @pl.when(i == m)
                def _():
                    b_some(N_A + 2 + 2 * m, N_A + 4 + 2 * m)

            dx_step(i)
            return 0

        lax.fori_loop(0, n_g, dx_between, 0)
        b_some(N_A + 2 + 2 * n_g, slots)

        @pl.when(inner)
        def _():
            for k in range(slots - LAG, slots):
                b_total(k)

        @pl.when(jnp.logical_not(inner))
        def _():
            for k in range(slots - LAG_OUT, slots):
                b_down(k)

        for k in range(N_A, slots):
            total_down(rb, k).wait_send()

            @pl.when(jnp.logical_not(inner))
            def _():
                b_to_inner(k, inner_dev).wait_send()

            @pl.when(inner)
            def _():
                to_mate(k).wait_send()
                b_to_outer(k, outer_dev).wait_send()

        def drain(h, _):
            for p in range(len(x_cut)):
                x_copy(h, p).wait_send()
            relay_out(h).wait_send()
            return 0

        lax.fori_loop(0, H, drain, 0)

        def drain_w(q, _):
            for y in range(3):
                w_unit(tp, q, y, 0, x_dev).wait_send()
                w_unit(tp, q, y, 1, c_dev).wait_send()
                w_unit(tp_x, q, y, 4, c_dev).wait_send()

                @pl.when(jnp.logical_and(zi < 3, q <= zi))
                def _():
                    w_unit(tp, q, y, 2, right_dev).wait_send()

                @pl.when(jnp.logical_and(zi > 0, q >= zi))
                def _():
                    w_unit(tp, q, y, 3, left_dev).wait_send()

            return 0

        lax.fori_loop(0, 4, drain_w, 0)

    @pl.when(st == 1)
    def _():
        w_loc = pltpu.make_async_copy(w_ref, wall.at[c], s_wl)
        w_core = remote(w_ref, wall.at[c], s_vs.at[2], s_vr.at[2], c_dev)
        vecs_l = [pltpu.make_async_copy(r, vec.at[k, c], s_vl.at[k]) for k, r in enumerate((gam_ref, bet_ref))]
        vecs_r = [remote(r, vec.at[k, c], s_vs.at[k], s_vr.at[k], c_dev) for k, r in enumerate((gam_ref, bet_ref))]
        dz_l = [pltpu.make_async_copy(dz_ref.at[:, :, 2 * s + c], dzb.at[s, c], s_dl.at[s]) for s in range(2)]
        dz_r = [remote(dz_ref.at[:, :, 2 * s + 1 - c], dzb.at[s, c], s_ds.at[s], s_dr.at[s], c_dev) for s in range(2)]

        part = pl.ds(pl.multiple_of(zi * quarter, quarter), quarter)
        w_y = [remote(w_ref.at[3 * y:3 * y + 3, part, :], wall.at[tp, 3 * y:3 * y + 3, part, :], s_ws.at[0, zi, y], s_wr.at[tp, zi, y], y_dev) for y in range(3)]

        for y in range(3):
            w_y[y].start()
        w_loc.start()
        w_core.start()
        for k in range(2):
            vecs_l[k].start()
            vecs_r[k].start()
            dz_l[k].start()
            dz_r[k].start()

        zero_borders(xe)
        zero_borders(ge)
        for buf in (xe, xo, ge, go):
            zero_planes(buf)

        def zero_acc(t, _):
            for k in range(2):
                acc[k, t] = jnp.zeros((CI, CO), F32)
            return 0

        lax.fori_loop(0, 9, zero_acc, 0)

        def zero_dx(h, _):
            dx_ref[h] = jnp.zeros((R, CI), BF16)
            return 0

        lax.fori_loop(0, H, zero_dx, 0)
        for k in range(2):
            vecs_l[k].wait()
            vecs_r[k].wait_recv()
            dz_l[k].wait()
            dz_r[k].wait_recv()
        w_loc.wait()
        w_core.wait_recv()

        def x_in(j, s, p):
            return remote(x_view(s, j, p), x_view(s, j, p), s_xf.at[p, j], s_xr.at[s, p, j], y_dev)

        def x_fwd(j, p):
            return remote(x_view(xi, j, p), x_view(xi, j, p), s_xf.at[p, j], s_xr.at[xi, p, j], x_dev)

        def g_send(h):
            return remote(ge.at[:, h + 1, pl.ds(PAD, R), :], relay.at[:, h], s_gs.at[h], s_gl.at[h], y_dev)

        def x_relay(j):
            for p in range(len(x_cut)):
                x_in(j, xi, p).wait_recv()
                x_fwd(j, p).start()

        lax.fori_loop(0, AHEAD, lambda j, _: (x_relay(j), 0)[1], 0)

        for plane in (0, H + 1):
            xt[plane] = jnp.zeros(xt.shape[1:], BF16)

        def turn_x(q):
            rows = jnp.concatenate([xe[s, q + 1, PAD:PAD + 128, :] for s in range(2)], axis=0)
            xt[q + 1] = rows.T

        def add_dw(h, t):
            rhs = jnp.concatenate([tap_rows(ge, go, s, h + 1, 1 - t % 3, 128) for s in range(2)], axis=0)
            prod = jnp.dot(xt[h + t // 3], rhs, preferred_element_type=F32)
            for k in range(2):
                acc[k, t] += prod[:, k * CO:(k + 1) * CO]

        def step(j, _):
            @pl.when(j + AHEAD < H)
            def _():
                x_relay(j + AHEAD)

            @pl.when(j < H)
            def _():
                for p in range(len(x_cut)):
                    x_in(j, 1 - xi, p).wait_recv()
                for s in range(2):
                    odd_copy(xe, xo, s, j + 1)
                turn_x(j)

            @pl.when(jnp.logical_and(j >= 1, j < H + 1))
            def _():
                h = j - 1
                pre = jnp.zeros((2 * R, CW), F32)
                for ky in range(3):
                    for kx in range(3):
                        t = 3 * ky + kx
                        lhs = jnp.concatenate([tap_rows(xe, xo, s, h + ky, kx - 1, R) for s in range(2)], axis=0)
                        rhs = jnp.concatenate([wall[0, t], wall[1, t]], axis=1)
                        pre = pre + jnp.dot(lhs, rhs, preferred_element_type=F32)
                for k in range(2):
                    gam = vec[0, k]
                    bet = vec[1, k]
                    for s in range(2):
                        y = pre[s * R:(s + 1) * R, k * CO:(k + 1) * CO] * gam + bet
                        zb[s, k, h] = jnp.maximum(y, 0.0).reshape(WD, 8, CO).astype(BF16)
                        dzr = dzb[s, k, h].astype(F32).reshape(R, CO)
                        ge[s, h + 1, PAD:PAD + R, k * CO:(k + 1) * CO] = jnp.where(y > 0, dzr * gam, 0.0).astype(BF16)
                g_send(h).start()
                for s in range(2):
                    odd_copy(ge, go, s, h + 1)
                    z_ref[h, :, 2 * s + c] = zb[s, c, h]

            @pl.when(jnp.logical_and(j >= 1, j < H))
            def _():
                for kx in range(3):
                    for ky in range(3):
                        add_dw(j - 1, 3 * ky + kx)

            return 0

        lax.fori_loop(0, H + 1, step, 0)

        def pair(t):
            return remote(acc.at[1 - c, t], prx.at[t], s_ps.at[t], s_pr.at[t], c_dev)

        n_t = CHUNKS[N_A][0]
        order = sorted(range(9), key=lambda t: 2 * (t - n_t) if t >= n_t else 2 * t + 1)
        for t in order:
            if t < 6:
                add_dw(H - 1, t)
            pair(t).start()
        z_r = [remote(zb.at[s, 1 - c], z_ref.at[:, :, 2 * s + c], s_zs.at[s], s_zr.at[s], c_dev) for s in range(2)]
        z_w = [remote(zb.at[s, 1 - c], z_ref.at[:, :, 2 * s + 1 - c], s_zs.at[s], s_zr.at[s], c_dev) for s in range(2)]
        for s in range(2):
            z_r[s].start()

        def own_part(k):
            t, rows = place(k)
            if k == N_A or (rows.start == 0 and (k > N_A or t < n_t)):
                pair(t).wait_recv()
            return acc[c, t, rows, :] + prx[t, rows, :]

        def send_b(i):
            if i < N_B:
                put(pb, N_A + i, own_part(N_A + i))
                part_up(N_A + i).start()

        def to_inner(k):
            return remote(cut(pb, k), cut(rb, k), s_os.at[k], s_or.at[k], inner_dev)

        def from_outer(k):
            return remote(cut(pb, k), cut(rb, k), s_os.at[k], s_or.at[k], outer_dev)

        def to_outer(k):
            return remote(cut(dw_ref, k), cut(dw_ref, k), s_ts.at[k], s_tr.at[k], outer_dev)

        def from_inner(k):
            return remote(cut(dw_ref, k), cut(dw_ref, k), s_ts.at[k], s_tr.at[k], inner_dev)

        @pl.when(jnp.logical_not(inner))
        def _():
            for k in range(max(N_A, N_B)):
                send_b(k)
                if k < N_A:
                    put(pb, k, own_part(k))
                    to_inner(k).start()
            for k in range(N_A):
                from_inner(k).wait_recv()
                to_inner(k).wait_send()

        @pl.when(inner)
        def _():
            send_b(0)
            for k in range(max(N_A + LAG, N_B)):
                send_b(k + 1)
                if k < N_A:
                    part = own_part(k)
                    from_outer(k).wait_recv()
                    put(pb, k, part + value(rb, k))
                    to_mate(k).start()
                m = k - LAG
                if 0 <= m < N_A:
                    to_mate(m).wait_recv()
                    put(dw_ref, m, value(pb, m) + value(mb, m))
                    to_outer(m).start()
            for k in range(N_A):
                to_mate(k).wait_send()
                to_outer(k).wait_send()

        for k in range(N_A, N_A + N_B):
            total_down(rb, k).wait_recv()
            part_up(k).wait_send()

        def drain(h, _):
            for p in range(len(x_cut)):
                x_fwd(h, p).wait_send()
            g_send(h).wait_send()
            return 0

        lax.fori_loop(0, H, drain, 0)

        def drain_w(t, _):
            pair(t).wait_send()
            return 0

        lax.fori_loop(0, 9, drain_w, 0)
        w_core.wait_send()
        for y in range(3):
            w_y[y].wait_send()
        for k in range(2):
            vecs_r[k].wait_send()
            dz_r[k].wait_send()
            z_r[k].wait_send()
            z_w[k].wait_recv()


def out_kernel(*refs):
    srcs, dsts, sem = refs[:3], refs[3:6], refs[6]
    copies = [pltpu.make_async_copy(a, b, sem.at[i]) for i, (a, b) in enumerate(zip(srcs, dsts))]
    for cp in copies:
        cp.start()
    for cp in copies:
        cp.wait()


def write_out(*arrays):
    return pl.pallas_call(
        out_kernel,
        out_shape=tuple(jax.ShapeDtypeStruct(a.shape, a.dtype) for a in arrays),
        in_specs=[pl.BlockSpec(memory_space=pltpu.VMEM)] * 3,
        out_specs=(pl.BlockSpec(memory_space=pl.ANY),) * 3,
        scratch_shapes=[pltpu.SemaphoreType.DMA((3,))],
        compiler_params=pltpu.CompilerParams(vmem_limit_bytes=16 * 1024 * 1024),
    )(*arrays)


def solution(mesh):
    act_spec = P('stage', ('dp', 'tp'))
    w_spec = P('stage', None, None, None, 'tp')
    vec_spec = P('stage', 'tp')
    chan_spec = P('stage', 'dp', None, None, 'tp')

    def device_step(act_in, w_conv, gamma_vec, beta_vec, z_grad):
        N, H, WD, CI = act_in.shape[1:]
        CO = w_conv.shape[-1]
        R = WD * N
        RP = 128 + 2 * PAD
        x = act_in[0].transpose(1, 2, 0, 3).reshape(H, R, CI)
        w = w_conv[0].reshape(9, CI, CO)
        dz = z_grad[0].transpose(1, 2, 0, 3).reshape(H, WD, 4, N, CO)
        dma = pltpu.SemaphoreType.DMA
        z, dx, dw = pl.pallas_call(
            functools.partial(block_kernel, H, WD, CI, CO),
            out_shape=(
                jax.ShapeDtypeStruct((H, WD, 4, N, CO), BF16),
                jax.ShapeDtypeStruct((H, R, CI), BF16),
                jax.ShapeDtypeStruct((9, CI, CO), F32),
            ),
            in_specs=[pl.BlockSpec(memory_space=pltpu.HBM)] * 5,
            out_specs=(pl.BlockSpec(memory_space=pltpu.VMEM),) * 3,
            scratch_shapes=[
                pltpu.VMEM((2, H + 2, RP, CI), BF16),
                pltpu.VMEM((2, H + 2, RP - 16, CI), BF16),
                pltpu.VMEM((2, H + 2, RP, 2 * CO), BF16),
                pltpu.VMEM((2, H + 2, RP - 16, 2 * CO), BF16),
                pltpu.VMEM((4, 9, CI, CO), BF16),
                pltpu.VMEM((2, 2, H, WD, N, CO), BF16),
                pltpu.VMEM((2, 2, H, WD, N, CO), BF16),
                pltpu.VMEM((2, 2, 1, CO), F32),
                pltpu.VMEM((2, 9, CI, CO), F32),
                pltpu.VMEM((9, CI, CO), F32),
                pltpu.VMEM((9, CI, CO), F32),
                pltpu.VMEM((9, CI, CO), F32),
                pltpu.VMEM((9, CI, CO), F32),
                pltpu.VMEM((H + 2, CI, 256), BF16),
                pltpu.VMEM((2, H, R, 2 * CO), BF16),
                dma((1, H)), dma((2, 1, H)), dma((1, H)), dma((H,)), dma((2, H)), dma((H,)), dma((H,)),
                dma, dma((5, 4, 3)), dma((4, 4, 3)), dma((2,)), dma((3,)), dma((3,)), dma((2,)), dma((2,)), dma((2,)),
                dma((2,)), dma((2,)), dma((9,)), dma((9,)),
                *[dma((N_A + N_B,))] * 6,
            ],
            compiler_params=pltpu.CompilerParams(collective_id=0, has_side_effects=True, vmem_limit_bytes=46 * 1024 * 1024),
        )(*[pltpu.with_memory_space_constraint(a, pltpu.HBM) for a in (x, w, gamma_vec, beta_vec, dz)])
        z, dx, dw = write_out(z, dx, dw)
        z_full = z.reshape(H, WD, 4 * N, CO).transpose(2, 0, 1, 3)
        dx_full = dx.reshape(H, WD, N, CI).transpose(2, 0, 1, 3)
        dw_full = dw.reshape(3, 3, CI, CO)
        return z_full[None], dx_full[None], dw_full[None]

    return jax.shard_map(device_step, mesh=mesh, in_specs=(act_spec, w_spec, vec_spec, vec_spec, chan_spec), out_specs=(chan_spec, act_spec, w_spec), check_vma=False)
```

```python
import functools

import jax
import jax.numpy as jnp
from jax import lax
from jax.experimental import pallas as pl
from jax.experimental.pallas import tpu as pltpu
from jax.sharding import PartitionSpec as P

MESH = pl.DeviceIdType.MESH
F32 = jnp.float32
BF16 = jnp.bfloat16
PAD = 16
AHEAD = 2
LAG = 3
LAG_OUT = 8
N_B = 14
CHUNKS = tuple((t, q, 1) for t in range(9) for q in range(4))
N_A = len(CHUNKS) - N_B


def remote(src, dst, send_sem, recv_sem, dev):
    return pltpu.make_async_remote_copy(src_ref=src, dst_ref=dst, send_sem=send_sem, recv_sem=recv_sem, device_id=dev, device_id_type=MESH)


def block_kernel(H, WD, CI, CO, x_ref, w_ref, gam_ref, bet_ref, dz_ref, z_ref, dx_ref, dw_ref,
                 xe, xo, ge, go, wall, dzb, zb, vec, acc, prx, pb, rb, mb, xt, relay, *sems):
    (s_xs, s_xr, s_xf, s_gs, s_gr, s_gl, s_gf, s_wl, s_ws, s_wr, s_vl, s_vs, s_vr, s_dl, s_ds, s_dr,
     s_zs, s_zr, s_ps, s_pr, s_os, s_or, s_ms, s_mr, s_ts, s_tr) = sems
    R = WD * 8
    quarter = CI // 4
    n_blk = min(CI, 256)
    CW = 2 * CO
    zi = lax.axis_index("dp")
    st = lax.axis_index("stage")
    tp = lax.axis_index("tp")
    xi = tp // 2
    c = tp % 2
    y_dev = (zi, 1 - st, tp)
    x_dev = (zi, st, 2 * (1 - xi) + c)
    c_dev = (zi, st, 2 * xi + 1 - c)
    z_mate = jnp.where(zi == 1, 2, 1)
    z_out = jnp.where(zi < 2, 0, 3)
    z_in = jnp.where(zi < 2, 1, 2)
    inner = jnp.logical_or(zi == 1, zi == 2)
    mate_dev = (z_mate, st, tp)
    outer_dev = (z_out, st, tp)
    inner_dev = (z_in, st, tp)

    barrier = pltpu.get_barrier_semaphore()
    for dev in (y_dev, x_dev, c_dev):
        pl.semaphore_signal(barrier, inc=1, device_id=dev, device_id_type=MESH)

    @pl.when(inner)
    def _():
        for dev in (mate_dev, outer_dev):
            pl.semaphore_signal(barrier, inc=1, device_id=dev, device_id_type=MESH)
        pl.semaphore_wait(barrier, 5)

    @pl.when(jnp.logical_not(inner))
    def _():
        pl.semaphore_signal(barrier, inc=1, device_id=inner_dev, device_id_type=MESH)
        pl.semaphore_wait(barrier, 4)

    def zero_borders(buf):
        ch = buf.shape[-1]

        def rows(h, _):
            for s in range(2):
                buf[s, h, 0:PAD, :] = jnp.zeros((PAD, ch), BF16)
                buf[s, h, PAD + R:, :] = jnp.zeros((buf.shape[2] - PAD - R, ch), BF16)
            return 0

        lax.fori_loop(0, H + 2, rows, 0)

    def zero_planes(buf):
        for s in range(2):
            for h in (0, H + 1):
                buf[s, h] = jnp.zeros(buf.shape[2:], BF16)

    def odd_copy(even, odd, s, h):
        n = odd.shape[2]
        odd[s, h] = even[s, h, 8:8 + n, :]

    def tap_rows(even, odd, s, plane, shift, n):
        if shift == 0:
            return even[s, plane, PAD:PAD + n, :]
        start = PAD + 8 * shift - 8
        return odd[s, plane, start:start + n, :]

    x_cut = ((0, 48), (48, R - 48))

    def x_view(s, h, p):
        return xe.at[s, h + 1, pl.ds(PAD + x_cut[p][0], x_cut[p][1]), :]

    def place(k):
        t, q0, nq = CHUNKS[k]
        return t, slice(q0 * quarter, (q0 + nq) * quarter)

    def cut(buf, k):
        t, rows = place(k)
        return buf.at[t, rows, :]

    def value(buf, k):
        t, rows = place(k)
        return buf[t, rows, :]

    def put(buf, k, val):
        t, rows = place(k)
        buf[t, rows, :] = val

    def part_up(k):
        return remote(cut(pb, k), cut(pb, k), s_os.at[k], s_or.at[k], y_dev)

    def to_mate(k):
        return remote(cut(pb, k), cut(mb, k), s_ms.at[k], s_mr.at[k], mate_dev)

    def total_down(src, k):
        return remote(cut(src, k), cut(dw_ref, k), s_ts.at[k], s_tr.at[k], y_dev)

    @pl.when(st == 0)
    def _():
        def x_copy(h, p):
            return remote(x_ref.at[h, pl.ds(*x_cut[p]), :], x_view(xi, h, p), s_xs.at[p, h], s_xr.at[xi, p, h], y_dev)

        def x_send(h, _):
            for p in range(len(x_cut)):
                x_copy(h, p).start()
            return 0

        lax.fori_loop(0, H, x_send, 0)
        zero_borders(ge)
        zero_planes(ge)
        zero_planes(go)

        def zero_out(h, _):
            z_ref[h] = jnp.zeros(z_ref.shape[1:], BF16)
            return 0

        lax.fori_loop(0, H, zero_out, 0)

        def zero_dw(t, _):
            dw_ref[t] = jnp.zeros((CI, CO), F32)
            return 0

        lax.fori_loop(0, 9, zero_dw, 0)

        def g_in(j, b):
            return remote(ge.at[b, j + 1, pl.ds(PAD, R), :], ge.at[b, j + 1, pl.ds(PAD, R), :], s_gf.at[j], s_gr.at[b, j], x_dev)

        def relay_in(j):
            return remote(relay.at[:, j], relay.at[:, j], s_gf.at[j], s_gl.at[j], y_dev)

        def relay_out(j):
            return remote(relay.at[1 - xi, j], ge.at[xi, j + 1, pl.ds(PAD, R), :], s_gf.at[j], s_gr.at[xi, j], x_dev)

        def g_relay(j):
            relay_in(j).wait_recv()
            relay_out(j).start()
            ge[xi, j + 1, PAD:PAD + R, :] = relay[xi, j]

        def relay_rows(lo, hi):
            lax.fori_loop(lo, min(hi, H), lambda j, _: (g_relay(j), 0)[1], 0)

        tp_x = 2 * (1 - xi) + c
        left_dev = (jnp.maximum(zi - 1, 0), st, tp)
        right_dev = (jnp.minimum(zi + 1, 3), st, tp)

        def w_unit(b, q, y, kind, dev):
            view = wall.at[b, pl.ds(3 * y, 3), pl.ds(pl.multiple_of(q * quarter, quarter), quarter), :]
            return remote(view, view, s_ws.at[kind, q, y], s_wr.at[b, q, y], dev)

        def w_got(q, go_right, go_left):
            def take(y, _):
                w_unit(tp, q, y, 0, y_dev).wait_recv()
                if go_right:
                    @pl.when(zi < 3)
                    def _():
                        w_unit(tp, q, y, 2, right_dev).start()
                if go_left:
                    @pl.when(zi > 0)
                    def _():
                        w_unit(tp, q, y, 3, left_dev).start()
                w_unit(tp, q, y, 0, x_dev).start()
                w_unit(tp, q, y, 1, c_dev).start()
                return 0

            lax.fori_loop(0, 3, take, 0)

        w_got(zi, True, True)
        for d in range(1, 4):
            @pl.when(zi - d >= 0)
            def _():
                w_got(zi - d, True, False)

            @pl.when(zi + d <= 3)
            def _():
                w_got(zi + d, False, True)

            relay_rows(2 * (d - 1), 2 * d)

        def w_cross(q, _):
            for y in range(3):
                w_unit(tp_x, q, y, 4, x_dev).wait_recv()
                w_unit(tp_x, q, y, 4, c_dev).start()
            return 0

        relay_rows(6, 9)
        lax.fori_loop(0, 4, w_cross, 0)
        relay_rows(9, H)

        def w_all(q, _):
            for y in range(3):
                for b in (2 * xi + 1 - c, 2 * (1 - xi) + 1 - c):
                    w_unit(b, q, y, 1, c_dev).wait_recv()
            return 0

        lax.fori_loop(0, 4, w_all, 0)

        G = 4

        def g_take(j, _):
            g_in(j, 1 - xi).wait_recv()
            for b in range(2):
                odd_copy(ge, go, b, j + 1)
            return 0

        def dx_rows(h0):
            for n in range(CI // n_blk):
                tot = jnp.zeros((G * R, n_blk), F32)
                for b in range(2):
                    for t in range(9):
                        lhs = jnp.concatenate([tap_rows(ge, go, b, h0 + r + 2 - t // 3, 1 - t % 3, R) for r in range(G)], axis=0)
                        rhs = jnp.concatenate([wall[2 * b + i, t, n * n_blk:(n + 1) * n_blk, :] for i in range(2)], axis=1)
                        tot = tot + lax.dot_general(lhs, rhs, (((1,), (1,)), ((), ())), preferred_element_type=F32)
                for r in range(G):
                    dx_ref[h0 + r, :, n * n_blk:(n + 1) * n_blk] = tot[r * R:(r + 1) * R].astype(BF16)

        def dx_step(i):
            @pl.when(i >= 0)
            def _():
                lo = jnp.where(i == 0, 0, G * i + 1)
                lax.fori_loop(lo, jnp.minimum(G * i + G + 1, H), g_take, 0)
                dx_rows(jnp.minimum(G * i, H - G))

        def b_to_inner(k, dev):
            return remote(cut(pb, k), cut(rb, k), s_os.at[k], s_tr.at[k], dev)

        def b_to_outer(k, dev):
            return remote(cut(rb, k), cut(mb, k), s_os.at[k], s_mr.at[k], dev)

        def b_up(k):
            part_up(k).wait_recv()

            @pl.when(jnp.logical_not(inner))
            def _():
                b_to_inner(k, inner_dev).start()

            @pl.when(inner)
            def _():
                b_to_inner(k, outer_dev).wait_recv()
                put(pb, k, value(pb, k) + value(rb, k))
                to_mate(k).start()

        def b_total(k):
            to_mate(k).wait_recv()
            put(rb, k, value(pb, k) + value(mb, k))
            b_to_outer(k, outer_dev).start()
            total_down(rb, k).start()

        def b_down(k):
            b_to_outer(k, inner_dev).wait_recv()
            total_down(mb, k).start()

        n_g = -(-H // G)
        slots = N_A + N_B

        def dx_loop(lo, hi):
            lax.fori_loop(min(lo, n_g), min(hi, n_g), lambda i, _: (dx_step(i), 0)[1], 0)

        def b_some(lo, hi):
            for k in range(lo, hi):
                b_up(k)

                @pl.when(inner)
                def _():
                    if k - LAG >= N_A:
                        b_total(k - LAG)

                @pl.when(jnp.logical_not(inner))
                def _():
                    if k - LAG_OUT >= N_A:
                        b_down(k - LAG_OUT)

        b_some(N_A, N_A + 2)

        def dx_between(i, _):
            for m in range(n_g):
                @pl.when(i == m)
                def _():
                    b_some(N_A + 2 + 2 * m, N_A + 4 + 2 * m)

            dx_step(i)
            return 0

        lax.fori_loop(0, n_g, dx_between, 0)
        b_some(N_A + 2 + 2 * n_g, slots)

        @pl.when(inner)
        def _():
            for k in range(slots - LAG, slots):
                b_total(k)

        @pl.when(jnp.logical_not(inner))
        def _():
            for k in range(slots - LAG_OUT, slots):
                b_down(k)

        for k in range(N_A, slots):
            total_down(rb, k).wait_send()

            @pl.when(jnp.logical_not(inner))
            def _():
                b_to_inner(k, inner_dev).wait_send()

            @pl.when(inner)
            def _():
                to_mate(k).wait_send()
                b_to_outer(k, outer_dev).wait_send()

        def drain(h, _):
            for p in range(len(x_cut)):
                x_copy(h, p).wait_send()
            relay_out(h).wait_send()
            return 0

        lax.fori_loop(0, H, drain, 0)

        def drain_w(q, _):
            for y in range(3):
                w_unit(tp, q, y, 0, x_dev).wait_send()
                w_unit(tp, q, y, 1, c_dev).wait_send()
                w_unit(tp_x, q, y, 4, c_dev).wait_send()

                @pl.when(jnp.logical_and(zi < 3, q <= zi))
                def _():
                    w_unit(tp, q, y, 2, right_dev).wait_send()

                @pl.when(jnp.logical_and(zi > 0, q >= zi))
                def _():
                    w_unit(tp, q, y, 3, left_dev).wait_send()

            return 0

        lax.fori_loop(0, 4, drain_w, 0)

    @pl.when(st == 1)
    def _():
        w_loc = pltpu.make_async_copy(w_ref, wall.at[c], s_wl)
        w_core = remote(w_ref, wall.at[c], s_vs.at[2], s_vr.at[2], c_dev)
        vecs_l = [pltpu.make_async_copy(r, vec.at[k, c], s_vl.at[k]) for k, r in enumerate((gam_ref, bet_ref))]
        vecs_r = [remote(r, vec.at[k, c], s_vs.at[k], s_vr.at[k], c_dev) for k, r in enumerate((gam_ref, bet_ref))]
        dz_l = [pltpu.make_async_copy(dz_ref.at[:, :, 2 * s + c], dzb.at[s, c], s_dl.at[s]) for s in range(2)]
        dz_r = [remote(dz_ref.at[:, :, 2 * s + 1 - c], dzb.at[s, c], s_ds.at[s], s_dr.at[s], c_dev) for s in range(2)]

        part = pl.ds(pl.multiple_of(zi * quarter, quarter), quarter)
        w_y = [remote(w_ref.at[3 * y:3 * y + 3, part, :], wall.at[tp, 3 * y:3 * y + 3, part, :], s_ws.at[0, zi, y], s_wr.at[tp, zi, y], y_dev) for y in range(3)]

        for y in range(3):
            w_y[y].start()
        w_loc.start()
        w_core.start()
        for k in range(2):
            vecs_l[k].start()
            vecs_r[k].start()
            dz_l[k].start()
            dz_r[k].start()

        zero_borders(xe)
        zero_borders(ge)
        for buf in (xe, xo, ge, go):
            zero_planes(buf)

        def zero_acc(t, _):
            for k in range(2):
                acc[k, t] = jnp.zeros((CI, CO), F32)
            return 0

        lax.fori_loop(0, 9, zero_acc, 0)

        def zero_dx(h, _):
            dx_ref[h] = jnp.zeros((R, CI), BF16)
            return 0

        lax.fori_loop(0, H, zero_dx, 0)
        for k in range(2):
            vecs_l[k].wait()
            vecs_r[k].wait_recv()
            dz_l[k].wait()
            dz_r[k].wait_recv()
        w_loc.wait()
        w_core.wait_recv()

        def x_in(j, s, p):
            return remote(x_view(s, j, p), x_view(s, j, p), s_xf.at[p, j], s_xr.at[s, p, j], y_dev)

        def x_fwd(j, p):
            return remote(x_view(xi, j, p), x_view(xi, j, p), s_xf.at[p, j], s_xr.at[xi, p, j], x_dev)

        def g_send(h):
            return remote(ge.at[:, h + 1, pl.ds(PAD, R), :], relay.at[:, h], s_gs.at[h], s_gl.at[h], y_dev)

        def x_relay(j):
            for p in range(len(x_cut)):
                x_in(j, xi, p).wait_recv()
                x_fwd(j, p).start()

        lax.fori_loop(0, AHEAD, lambda j, _: (x_relay(j), 0)[1], 0)

        for plane in (0, H + 1):
            xt[plane] = jnp.zeros(xt.shape[1:], BF16)

        def turn_x(q):
            rows = jnp.concatenate([xe[s, q + 1, PAD:PAD + 128, :] for s in range(2)], axis=0)
            xt[q + 1] = rows.T

        def add_dw(h, t):
            rhs = jnp.concatenate([tap_rows(ge, go, s, h + 1, 1 - t % 3, 128) for s in range(2)], axis=0)
            prod = jnp.dot(xt[h + t // 3], rhs, preferred_element_type=F32)
            for k in range(2):
                acc[k, t] += prod[:, k * CO:(k + 1) * CO]

        def step(j, _):
            @pl.when(j + AHEAD < H)
            def _():
                x_relay(j + AHEAD)

            @pl.when(j < H)
            def _():
                for p in range(len(x_cut)):
                    x_in(j, 1 - xi, p).wait_recv()
                for s in range(2):
                    odd_copy(xe, xo, s, j + 1)
                turn_x(j)

            @pl.when(jnp.logical_and(j >= 1, j < H + 1))
            def _():
                h = j - 1
                pre = jnp.zeros((2 * R, CW), F32)
                for ky in range(3):
                    for kx in range(3):
                        t = 3 * ky + kx
                        lhs = jnp.concatenate([tap_rows(xe, xo, s, h + ky, kx - 1, R) for s in range(2)], axis=0)
                        rhs = jnp.concatenate([wall[0, t], wall[1, t]], axis=1)
                        pre = pre + jnp.dot(lhs, rhs, preferred_element_type=F32)
                for k in range(2):
                    gam = vec[0, k]
                    bet = vec[1, k]
                    for s in range(2):
                        y = pre[s * R:(s + 1) * R, k * CO:(k + 1) * CO] * gam + bet
                        zb[s, k, h] = jnp.maximum(y, 0.0).reshape(WD, 8, CO).astype(BF16)
                        dzr = dzb[s, k, h].astype(F32).reshape(R, CO)
                        ge[s, h + 1, PAD:PAD + R, k * CO:(k + 1) * CO] = jnp.where(y > 0, dzr * gam, 0.0).astype(BF16)
                g_send(h).start()
                for s in range(2):
                    odd_copy(ge, go, s, h + 1)
                    z_ref[h, :, 2 * s + c] = zb[s, c, h]

            @pl.when(jnp.logical_and(j >= 1, j < H))
            def _():
                for kx in range(3):
                    for ky in range(3):
                        add_dw(j - 1, 3 * ky + kx)

            return 0

        lax.fori_loop(0, H + 1, step, 0)

        def pair(t):
            return remote(acc.at[1 - c, t], prx.at[t], s_ps.at[t], s_pr.at[t], c_dev)

        n_t = CHUNKS[N_A][0]
        order = sorted(range(9), key=lambda t: 2 * (t - n_t) if t >= n_t else 2 * t + 1)
        for t in order:
            if t < 6:
                add_dw(H - 1, t)
            pair(t).start()
        z_r = [remote(zb.at[s, 1 - c], z_ref.at[:, :, 2 * s + c], s_zs.at[s], s_zr.at[s], c_dev) for s in range(2)]
        z_w = [remote(zb.at[s, 1 - c], z_ref.at[:, :, 2 * s + 1 - c], s_zs.at[s], s_zr.at[s], c_dev) for s in range(2)]
        for s in range(2):
            z_r[s].start()

        def own_part(k):
            t, rows = place(k)
            if k == N_A or (rows.start == 0 and (k > N_A or t < n_t)):
                pair(t).wait_recv()
            return acc[c, t, rows, :] + prx[t, rows, :]

        def send_b(i):
            if i < N_B:
                put(pb, N_A + i, own_part(N_A + i))
                part_up(N_A + i).start()

        def to_inner(k):
            return remote(cut(pb, k), cut(rb, k), s_os.at[k], s_or.at[k], inner_dev)

        def from_outer(k):
            return remote(cut(pb, k), cut(rb, k), s_os.at[k], s_or.at[k], outer_dev)

        def to_outer(k):
            return remote(cut(dw_ref, k), cut(dw_ref, k), s_ts.at[k], s_tr.at[k], outer_dev)

        def from_inner(k):
            return remote(cut(dw_ref, k), cut(dw_ref, k), s_ts.at[k], s_tr.at[k], inner_dev)

        @pl.when(jnp.logical_not(inner))
        def _():
            for k in range(max(N_A, N_B)):
                send_b(k)
                if k < N_A:
                    put(pb, k, own_part(k))
                    to_inner(k).start()
            for k in range(N_A):
                from_inner(k).wait_recv()
                to_inner(k).wait_send()

        @pl.when(inner)
        def _():
            send_b(0)
            for k in range(max(N_A + LAG, N_B)):
                send_b(k + 1)
                if k < N_A:
                    part = own_part(k)
                    from_outer(k).wait_recv()
                    put(pb, k, part + value(rb, k))
                    to_mate(k).start()
                m = k - LAG
                if 0 <= m < N_A:
                    to_mate(m).wait_recv()
                    put(dw_ref, m, value(pb, m) + value(mb, m))
                    to_outer(m).start()
            for k in range(N_A):
                to_mate(k).wait_send()
                to_outer(k).wait_send()

        for k in range(N_A, N_A + N_B):
            total_down(rb, k).wait_recv()
            part_up(k).wait_send()

        def drain(h, _):
            for p in range(len(x_cut)):
                x_fwd(h, p).wait_send()
            g_send(h).wait_send()
            return 0

        lax.fori_loop(0, H, drain, 0)

        def drain_w(t, _):
            pair(t).wait_send()
            return 0

        lax.fori_loop(0, 9, drain_w, 0)
        w_core.wait_send()
        for y in range(3):
            w_y[y].wait_send()
        for k in range(2):
            vecs_r[k].wait_send()
            dz_r[k].wait_send()
            z_r[k].wait_send()
            z_w[k].wait_recv()


def out_kernel(*refs):
    srcs, dsts, sem = refs[:3], refs[3:6], refs[6]
    copies = [pltpu.make_async_copy(a, b, sem.at[i]) for i, (a, b) in enumerate(zip(srcs, dsts))]
    for cp in copies:
        cp.start()
    for cp in copies:
        cp.wait()


def write_out(*arrays):
    return pl.pallas_call(
        out_kernel,
        out_shape=tuple(jax.ShapeDtypeStruct(a.shape, a.dtype) for a in arrays),
        in_specs=[pl.BlockSpec(memory_space=pltpu.VMEM)] * 3,
        out_specs=(pl.BlockSpec(memory_space=pl.ANY),) * 3,
        scratch_shapes=[pltpu.SemaphoreType.DMA((3,))],
        compiler_params=pltpu.CompilerParams(vmem_limit_bytes=16 * 1024 * 1024),
    )(*arrays)


def solution(mesh):
    act_spec = P('stage', ('dp', 'tp'))
    w_spec = P('stage', None, None, None, 'tp')
    vec_spec = P('stage', 'tp')
    chan_spec = P('stage', 'dp', None, None, 'tp')

    def device_step(act_in, w_conv, gamma_vec, beta_vec, z_grad):
        N, H, WD, CI = act_in.shape[1:]
        CO = w_conv.shape[-1]
        R = WD * N
        RP = 128 + 2 * PAD
        x = act_in[0].transpose(1, 2, 0, 3).reshape(H, R, CI)
        w = w_conv[0].reshape(9, CI, CO)
        dz = z_grad[0].transpose(1, 2, 0, 3).reshape(H, WD, 4, N, CO)
        dma = pltpu.SemaphoreType.DMA
        z, dx, dw = pl.pallas_call(
            functools.partial(block_kernel, H, WD, CI, CO),
            out_shape=(
                jax.ShapeDtypeStruct((H, WD, 4, N, CO), BF16),
                jax.ShapeDtypeStruct((H, R, CI), BF16),
                jax.ShapeDtypeStruct((9, CI, CO), F32),
            ),
            in_specs=[pl.BlockSpec(memory_space=pltpu.HBM)] * 5,
            out_specs=(pl.BlockSpec(memory_space=pltpu.VMEM),) * 3,
            scratch_shapes=[
                pltpu.VMEM((2, H + 2, RP, CI), BF16),
                pltpu.VMEM((2, H + 2, RP - 16, CI), BF16),
                pltpu.VMEM((2, H + 2, RP, 2 * CO), BF16),
                pltpu.VMEM((2, H + 2, RP - 16, 2 * CO), BF16),
                pltpu.VMEM((4, 9, CI, CO), BF16),
                pltpu.VMEM((2, 2, H, WD, N, CO), BF16),
                pltpu.VMEM((2, 2, H, WD, N, CO), BF16),
                pltpu.VMEM((2, 2, 1, CO), F32),
                pltpu.VMEM((2, 9, CI, CO), F32),
                pltpu.VMEM((9, CI, CO), F32),
                pltpu.VMEM((9, CI, CO), F32),
                pltpu.VMEM((9, CI, CO), F32),
                pltpu.VMEM((9, CI, CO), F32),
                pltpu.VMEM((H + 2, CI, 256), BF16),
                pltpu.VMEM((2, H, R, 2 * CO), BF16),
                dma((2, H)), dma((2, 2, H)), dma((2, H)), dma((H,)), dma((2, H)), dma((H,)), dma((H,)),
                dma, dma((5, 4, 3)), dma((4, 4, 3)), dma((2,)), dma((3,)), dma((3,)), dma((2,)), dma((2,)), dma((2,)),
                dma((2,)), dma((2,)), dma((9,)), dma((9,)),
                *[dma((N_A + N_B,))] * 6,
            ],
            compiler_params=pltpu.CompilerParams(collective_id=0, has_side_effects=True, vmem_limit_bytes=46 * 1024 * 1024),
        )(*[pltpu.with_memory_space_constraint(a, pltpu.HBM) for a in (x, w, gamma_vec, beta_vec, dz)])
        z, dx, dw = write_out(z, dx, dw)
        z_full = z.reshape(H, WD, 4 * N, CO).transpose(2, 0, 1, 3)
        dx_full = dx.reshape(H, WD, N, CI).transpose(2, 0, 1, 3)
        dw_full = dw.reshape(3, 3, CI, CO)
        return z_full[None], dx_full[None], dw_full[None]

    return jax.shard_map(device_step, mesh=mesh, in_specs=(act_spec, w_spec, vec_spec, vec_spec, chan_spec), out_specs=(chan_spec, act_spec, w_spec), check_vma=False)
```
